128 devices in a mesh: batch: 1, time: 2 (over core), region: 64 (over z, y, x).
Axes of the slice: x: 4, y: 4, z: 4, core: 2. Of those that a mesh axis runs over, the one named last changes fastest.
Arguments:
- patches: bfloat16 [24576, 1536], P(('batch', 'time', 'region'))
- enc_pos: bfloat16 [24576, 768], P(('batch', 'time', 'region'))
- vis_mask: int32 [24576], P(('batch', 'time', 'region'))
- dec_pos: bfloat16 [24576, 384], P(('batch', 'time', 'region'))
- w_embed: bfloat16 [1536, 768], replicated
- b_embed: float32 [768], replicated
- enc_vec: float32 [2, 12, 768], replicated
- enc_wqkv: bfloat16 [2, 768, 3, 12, 64], replicated
- enc_wo: bfloat16 [2, 12, 64, 768], replicated
- enc_w1: bfloat16 [2, 768, 3072], replicated
- enc_w2: bfloat16 [2, 3072, 768], replicated
- enc_final: float32 [2, 768], replicated
- w_dec_in: bfloat16 [768, 384], replicated
- mask_token: bfloat16 [384], replicated
- dec_vec: float32 [2, 12, 384], replicated
- dec_wqkv: bfloat16 [2, 384, 3, 6, 64], replicated
- dec_wo: bfloat16 [2, 6, 64, 384], replicated
- dec_w1: bfloat16 [2, 384, 1536], replicated
- dec_w2: bfloat16 [2, 1536, 384], replicated
- dec_final: float32 [2, 384], replicated
- w_out: bfloat16 [384, 1536], replicated
Outputs:
- output: float32 [24576, 1536], P(('batch', 'time', 'region'))
All inputs are finite; a program needn't handle non-finite values.
Results may differ from the reference program's by a relative error of at most 0.0143243.
Values are sent between devices in bfloat16 or wider.
A program may use at most 1 GiB of HBM per device.

```python
import jax
import jax.numpy as jnp
from jax import lax

PATCH_DIM = 1536
ENC_WIDTH = 768
ENC_HEADS = 12
DEC_WIDTH = 384
DEC_HEADS = 6
TOKENS_DEV = 192
TIME_BLOCKS = 2
REGIONS = 64
KEEP_DIV = 8
ENC_LAYERS = 2
DEC_LAYERS = 2

SHARDS = TIME_BLOCKS * REGIONS
TOKENS = TOKENS_DEV * SHARDS
VIS_DEV = TOKENS_DEV // KEEP_DIV
VISIBLE = VIS_DEV * SHARDS
SKEW = min(4, REGIONS)
ENC_HEAD = ENC_WIDTH // ENC_HEADS
DEC_HEAD = DEC_WIDTH // DEC_HEADS
LN_EPS = 1e-6


def draw_mask(mask_key):
    key_rank, key_shift, key_place = jax.random.split(mask_key, 3)
    pair_count = (REGIONS - SKEW) // 2
    shifts = jax.random.randint(key_shift, (TIME_BLOCKS, pair_count), 0, VIS_DEV + 1)
    paired = jnp.stack([VIS_DEV + shifts, VIS_DEV - shifts], axis=-1).reshape(TIME_BLOCKS, REGIONS - SKEW)
    profile = jnp.concatenate([jnp.full((TIME_BLOCKS, 1), SKEW * VIS_DEV, jnp.int32), jnp.zeros((TIME_BLOCKS, SKEW - 1), jnp.int32), paired.astype(jnp.int32)], axis=1)
    region_rank = jax.vmap(lambda one_key: jax.random.permutation(one_key, REGIONS))(jax.random.split(key_rank, TIME_BLOCKS))
    counts = jnp.take_along_axis(profile, region_rank, axis=1).reshape(SHARDS, 1)
    token_rank = jax.vmap(lambda one_key: jax.random.permutation(one_key, TOKENS_DEV))(jax.random.split(key_place, SHARDS))
    return (token_rank < counts).astype(jnp.int32).reshape(TOKENS)


def normal_draw(draw_key, out_shape, spread):
    return jax.random.normal(draw_key, out_shape, jnp.float32) * spread


def qkv_gain():
    return jnp.array([1.6, 1.6, 1.0], jnp.float32)[:, None, None]


def block_vectors(draw_key, layer_count, model_width):
    gain_rows = jnp.array([1.0, 0.0, 1.0, 0.0, 0.0, 0.0, 0.0, 0.0, 0.0, 0.0, 0.0, 0.0], jnp.float32)[:, None]
    return jax.random.normal(draw_key, (layer_count, 12, model_width), jnp.float32) * 0.2 + gain_rows


def final_vectors(draw_key, model_width):
    return jax.random.normal(draw_key, (2, model_width), jnp.float32) * 0.2 + jnp.array([1.0, 0.0], jnp.float32)[:, None]


def setup_inputs(seed: int = 0, part: int = 0) -> dict:
    part_key = jax.random.fold_in(jax.random.key(seed), part)
    key_patch, key_epos, key_mask, key_dpos = jax.random.split(part_key, 4)
    weight_keys = jax.random.split(jax.random.key(seed + 1), 17)
    return {
        "patches": normal_draw(key_patch, (TOKENS, PATCH_DIM), 1.0).astype(jnp.bfloat16),
        "enc_pos": normal_draw(key_epos, (TOKENS, ENC_WIDTH), 0.5).astype(jnp.bfloat16),
        "vis_mask": draw_mask(key_mask),
        "dec_pos": normal_draw(key_dpos, (TOKENS, DEC_WIDTH), 0.5).astype(jnp.bfloat16),
        "w_embed": normal_draw(weight_keys[0], (PATCH_DIM, ENC_WIDTH), PATCH_DIM ** -0.5).astype(jnp.bfloat16),
        "b_embed": normal_draw(weight_keys[1], (ENC_WIDTH,), 0.5),
        "enc_vec": block_vectors(weight_keys[2], ENC_LAYERS, ENC_WIDTH),
        "enc_wqkv": (normal_draw(weight_keys[3], (ENC_LAYERS, ENC_WIDTH, 3, ENC_HEADS, ENC_HEAD), ENC_WIDTH ** -0.5) * qkv_gain()).astype(jnp.bfloat16),
        "enc_wo": normal_draw(weight_keys[4], (ENC_LAYERS, ENC_HEADS, ENC_HEAD, ENC_WIDTH), 1.5 * ENC_WIDTH ** -0.5).astype(jnp.bfloat16),
        "enc_w1": normal_draw(weight_keys[5], (ENC_LAYERS, ENC_WIDTH, 4 * ENC_WIDTH), ENC_WIDTH ** -0.5).astype(jnp.bfloat16),
        "enc_w2": normal_draw(weight_keys[6], (ENC_LAYERS, 4 * ENC_WIDTH, ENC_WIDTH), (4 * ENC_WIDTH) ** -0.5).astype(jnp.bfloat16),
        "enc_final": final_vectors(weight_keys[7], ENC_WIDTH),
        "w_dec_in": normal_draw(weight_keys[8], (ENC_WIDTH, DEC_WIDTH), 1.5 * ENC_WIDTH ** -0.5).astype(jnp.bfloat16),
        "mask_token": normal_draw(weight_keys[9], (DEC_WIDTH,), 1.0).astype(jnp.bfloat16),
        "dec_vec": block_vectors(weight_keys[10], DEC_LAYERS, DEC_WIDTH),
        "dec_wqkv": (normal_draw(weight_keys[11], (DEC_LAYERS, DEC_WIDTH, 3, DEC_HEADS, DEC_HEAD), DEC_WIDTH ** -0.5) * qkv_gain()).astype(jnp.bfloat16),
        "dec_wo": normal_draw(weight_keys[12], (DEC_LAYERS, DEC_HEADS, DEC_HEAD, DEC_WIDTH), 1.5 * DEC_WIDTH ** -0.5).astype(jnp.bfloat16),
        "dec_w1": normal_draw(weight_keys[13], (DEC_LAYERS, DEC_WIDTH, 4 * DEC_WIDTH), DEC_WIDTH ** -0.5).astype(jnp.bfloat16),
        "dec_w2": normal_draw(weight_keys[14], (DEC_LAYERS, 4 * DEC_WIDTH, DEC_WIDTH), (4 * DEC_WIDTH) ** -0.5).astype(jnp.bfloat16),
        "dec_final": final_vectors(weight_keys[15], DEC_WIDTH),
        "w_out": normal_draw(weight_keys[16], (DEC_WIDTH, PATCH_DIM), DEC_WIDTH ** -0.5).astype(jnp.bfloat16),
    }


def layer_norm(hidden, ln_gain, ln_shift):
    hid_f32 = hidden.astype(jnp.float32)
    mean_val = jnp.mean(hid_f32, axis=-1, keepdims=True)
    centered = hid_f32 - mean_val
    variance = jnp.mean(centered * centered, axis=-1, keepdims=True)
    return centered * lax.rsqrt(variance + LN_EPS) * ln_gain + ln_shift


def attention(query_rows, key_rows, value_rows, blocks):
    query_count, head_count, head_dim = query_rows.shape
    q_blocks = query_rows.reshape(blocks, query_count // blocks, head_count, head_dim)
    key_f32 = key_rows.astype(jnp.float32)
    value_f32 = value_rows.astype(jnp.float32)

    def one_block(q_block):
        scores = jnp.einsum("qhd,khd->hqk", q_block.astype(jnp.float32), key_f32) * (head_dim ** -0.5)
        attn_probs = jax.nn.softmax(scores, axis=-1).astype(jnp.bfloat16)
        return jnp.einsum("hqk,khd->qhd", attn_probs.astype(jnp.float32), value_f32).astype(jnp.bfloat16)

    return lax.map(one_block, q_blocks).reshape(query_count, head_count, head_dim)


def transformer_block(hidden, vec_rows, w_qkv, w_o, w_one, w_two, blocks):
    head_count, head_dim = w_qkv.shape[2], w_qkv.shape[3]
    normed = layer_norm(hidden, vec_rows[0], vec_rows[1]).astype(jnp.bfloat16)
    qkv_bias = jnp.stack([vec_rows[4], jnp.zeros_like(vec_rows[4]), vec_rows[5]]).reshape(1, 3, head_count, head_dim)
    qkv_rows = (jnp.einsum("nd,dche->nche", normed.astype(jnp.float32), w_qkv.astype(jnp.float32)) + qkv_bias).astype(jnp.bfloat16)
    attended = attention(qkv_rows[:, 0], qkv_rows[:, 1], qkv_rows[:, 2], blocks)
    residual = (hidden.astype(jnp.float32) + jnp.einsum("nhe,hed->nd", attended.astype(jnp.float32), w_o.astype(jnp.float32)) + vec_rows[6]).astype(jnp.bfloat16)
    normed_mlp = layer_norm(residual, vec_rows[2], vec_rows[3]).astype(jnp.bfloat16)
    mlp_hidden = jax.nn.gelu(jnp.dot(normed_mlp, w_one, preferred_element_type=jnp.float32) + vec_rows[8:12].reshape(-1), approximate=False).astype(jnp.bfloat16)
    return (residual.astype(jnp.float32) + jnp.dot(mlp_hidden, w_two, preferred_element_type=jnp.float32) + vec_rows[7]).astype(jnp.bfloat16)


def run_stack(hidden, vec_stack, wqkv_stack, wo_stack, w1_stack, w2_stack, blocks):
    def layer_step(hidden_state, layer_params):
        vec_rows, w_qkv, w_o, w_one, w_two = layer_params
        return transformer_block(hidden_state, vec_rows, w_qkv, w_o, w_one, w_two, blocks), None

    final_state, _ = lax.scan(layer_step, hidden, (vec_stack, wqkv_stack, wo_stack, w1_stack, w2_stack))
    return final_state


def reference(patches, enc_pos, vis_mask, dec_pos, w_embed, b_embed, enc_vec, enc_wqkv, enc_wo, enc_w1, enc_w2, enc_final, w_dec_in, mask_token, dec_vec, dec_wqkv, dec_wo, dec_w1, dec_w2, dec_final, w_out):
    vis_idx = jnp.nonzero(vis_mask, size=VISIBLE)[0]
    embedded = (jnp.dot(patches[vis_idx], w_embed, preferred_element_type=jnp.float32) + b_embed + enc_pos[vis_idx].astype(jnp.float32)).astype(jnp.bfloat16)
    encoded = run_stack(embedded, enc_vec, enc_wqkv, enc_wo, enc_w1, enc_w2, SHARDS)
    latent = jnp.dot(layer_norm(encoded, enc_final[0], enc_final[1]).astype(jnp.bfloat16), w_dec_in, preferred_element_type=jnp.float32).astype(jnp.bfloat16)
    scattered = jnp.zeros((TOKENS, DEC_WIDTH), jnp.float32).at[vis_idx].set(latent.astype(jnp.float32))
    dec_in = (jnp.where(vis_mask[:, None] == 1, scattered, mask_token.astype(jnp.float32)) + dec_pos.astype(jnp.float32)).astype(jnp.bfloat16)
    decoded = run_stack(dec_in, dec_vec, dec_wqkv, dec_wo, dec_w1, dec_w2, SHARDS)
    return jnp.dot(layer_norm(decoded, dec_final[0], dec_final[1]).astype(jnp.bfloat16), w_out, preferred_element_type=jnp.float32)
```

```python
import functools
import jax
import jax.numpy as jnp
from jax import lax
from jax.experimental import pallas as pl
from jax.experimental.pallas import tpu as pltpu
from jax.sharding import PartitionSpec as P

LN_EPS = 1e-6
TOKEN_AXES = ("batch", "time", "region")
SIDE = 4
REGIONS = SIDE ** 3
PLANE = SIDE * SIDE * 2
ROW = SIDE * 2
HEAD = 64
MESH = pl.DeviceIdType.MESH
RING = (1, 3, 2)
VMEM_LIMIT = 60 * 1024 * 1024


def position():
    t, r = lax.axis_index("time"), lax.axis_index("region")
    return t, r // 16, lax.rem(r // 4, 4), lax.rem(r, 4)


def device(t, z, y, x):
    return {"time": t, "region": z * 16 + y * 4 + x}


def turn(a, d):
    return lax.rem(a + d, SIDE)


def gather_kernel(a_ref, b_ref, q_ref, kv_ref, qall_ref, a_send, a_recv, b_send, b_recv, q_send, q_recv):
    t, z, y, x = position()
    other = 1 - t
    barrier = pltpu.get_barrier_semaphore()
    peers = [(other, z, y, x)]
    for d in RING:
        for c in range(2):
            peers += [(c, turn(z, d), y, x), (c, z, turn(y, d), x), (c, z, y, turn(x, d))]
    for peer in peers:
        pl.semaphore_signal(barrier, inc=1, device_id=device(*peer), device_id_type=MESH)
    pl.semaphore_wait(barrier, len(peers))

    def slot(z_, y_, t_):
        return (z_ * SIDE + y_) * 2 + t_

    mine = slot(z, y, t)
    row_mine = x * 2 + t
    sends = []
    counts = {"a": 0, "b": 0, "q": 0}
    send_sems = {"a": a_send, "b": b_send, "q": q_send}
    recv_sems = {"a": a_recv, "b": b_recv, "q": q_recv}
    dests = {"a": kv_ref.at[0], "b": kv_ref.at[1], "q": qall_ref}
    sources = {"a": a_ref, "b": b_ref, "q": q_ref}

    def send(kind, src, to_slot, peer):
        copy = pltpu.make_async_remote_copy(
            src_ref=src,
            dst_ref=dests[kind].at[to_slot],
            send_sem=send_sems[kind].at[counts[kind]],
            recv_sem=recv_sems[kind].at[to_slot],
            device_id=device(*peer),
            device_id_type=MESH,
        )
        counts[kind] += 1
        copy.start()
        sends.append(copy)

    def arrived(kind, at):
        pltpu.make_async_remote_copy(
            src_ref=dests[kind].at[at],
            dst_ref=dests[kind].at[at],
            send_sem=send_sems[kind].at[0],
            recv_sem=recv_sems[kind].at[at],
            device_id=device(t, z, y, x),
            device_id_type=MESH,
        ).wait_recv()

    send("q", q_ref.at[other], row_mine, (other, z, y, x))
    send("a", a_ref.at[other], mine, (other, z, y, x))
    send("b", b_ref.at[other], mine, (other, z, y, x))
    for d in RING:
        for c in range(2):
            send("q", q_ref.at[c], row_mine, (c, z, y, turn(x, d)))
            send("a", a_ref.at[c], mine, (c, z, turn(y, d), x))
            send("b", b_ref.at[c], mine, (c, turn(z, d), y, x))
    for d in RING:
        send("a", a_ref.at[t], mine, (t, turn(z, d), y, x))
        send("b", b_ref.at[t], mine, (t, z, turn(y, d), x))
    kv_ref[0, mine] = a_ref[t]
    kv_ref[1, mine] = b_ref[t]
    qall_ref[row_mine] = q_ref[t]

    arrivals = [(0, other)] + [(4 - d, c) for d in RING for c in range(2)]
    for d0, c in arrivals:
        at = slot(z, turn(y, d0), c)
        arrived("a", at)
        for d in RING:
            send("a", dests["a"].at[at], at, (t, turn(z, d), y, x))
        at = slot(turn(z, d0), y, c)
        arrived("b", at)
        for d in RING:
            send("b", dests["b"].at[at], at, (t, z, turn(y, d), x))
    for dz in RING:
        for dy in range(SIDE):
            for c in range(2):
                arrived("a", slot(turn(z, dz), turn(y, dy), c))
                arrived("b", slot(turn(z, dy), turn(y, dz), c))
    for d0, c in arrivals:
        arrived("q", turn(x, d0) * 2 + c)
    for copy in sends:
        copy.wait_send()


def gather(a, b, q, collective_id):
    halves, rows, lanes = a.shape
    n = 31
    vmem = pl.BlockSpec(memory_space=pltpu.VMEM)
    return pl.pallas_call(
        gather_kernel,
        out_shape=(
            jax.ShapeDtypeStruct((2, PLANE, rows, lanes), a.dtype),
            jax.ShapeDtypeStruct((ROW,) + q.shape[1:], q.dtype),
        ),
        in_specs=[vmem] * 3,
        out_specs=(vmem, vmem),
        scratch_shapes=[
            pltpu.SemaphoreType.DMA((n,)),
            pltpu.SemaphoreType.DMA((PLANE,)),
            pltpu.SemaphoreType.DMA((n,)),
            pltpu.SemaphoreType.DMA((PLANE,)),
            pltpu.SemaphoreType.DMA((ROW,)),
            pltpu.SemaphoreType.DMA((ROW,)),
        ],
        compiler_params=pltpu.CompilerParams(collective_id=collective_id, has_side_effects=True, vmem_limit_bytes=VMEM_LIMIT),
        name="gather_kv",
    )(a, b, q)


def flash_kernel(heads, key_block, steps, q_ref, k_ref, vt_ref, out_ref, acc_ref, stat_ref):
    width = heads * HEAD
    acc_ref[...] = jnp.zeros_like(acc_ref)
    lanes = q_ref.shape[-1]
    for h in range(heads):
        stat_ref[h] = jnp.full((8, lanes), -jnp.inf, jnp.float32)
        stat_ref[heads + h] = jnp.zeros((8, lanes), jnp.float32)

    def step(i, _):
        at = pl.multiple_of(i * key_block, key_block)
        for h in range(heads):
            k_rows = k_ref[pl.ds(at, key_block), (h // 2) * 128:(h // 2 + 1) * 128]
            scores = jnp.dot(k_rows, q_ref[h], preferred_element_type=jnp.float32)
            old = stat_ref[h, 0:1]
            new = jnp.maximum(old, jnp.max(scores, axis=0, keepdims=True))
            weights = jnp.exp(scores - new)
            fade = jnp.exp(old - new)
            stat_ref[h, 0:1] = new
            stat_ref[heads + h, 0:1] = stat_ref[heads + h, 0:1] * fade + jnp.sum(weights, axis=0, keepdims=True)
            part = jnp.dot(vt_ref[h * HEAD:(h + 1) * HEAD, pl.ds(at, key_block)], weights.astype(jnp.bfloat16), preferred_element_type=jnp.float32)
            acc_ref[h * HEAD:(h + 1) * HEAD] = acc_ref[h * HEAD:(h + 1) * HEAD] * fade + part
        return 0

    lax.fori_loop(0, steps, step, 0)
    for h in range(heads):
        acc_ref[width + h:width + h + 1] = stat_ref[h, 0:1]
        acc_ref[width + heads + h:width + heads + h + 1] = stat_ref[heads + h, 0:1]
    out_ref[...] = acc_ref[...].T


def flash(q, k, vt, key_block):
    heads, _, queries = q.shape
    keys, lanes = k.shape
    out_lanes = -(-(heads * HEAD + 2 * heads) // 128) * 128
    block = 256
    return pl.pallas_call(
        functools.partial(flash_kernel, heads, key_block, keys // key_block),
        grid=(queries // block,),
        out_shape=jax.ShapeDtypeStruct((queries, out_lanes), jnp.float32),
        in_specs=[
            pl.BlockSpec((heads, 128, block), lambda i: (0, 0, i)),
            pl.BlockSpec((keys, lanes), lambda i: (0, 0)),
            pl.BlockSpec((heads * HEAD, keys), lambda i: (0, 0)),
        ],
        out_specs=pl.BlockSpec((block, out_lanes), lambda i: (i, 0)),
        scratch_shapes=[pltpu.VMEM((out_lanes, block), jnp.float32), pltpu.VMEM((2 * heads, 8, block), jnp.float32)],
        compiler_params=pltpu.CompilerParams(vmem_limit_bytes=VMEM_LIMIT),
        name="flash",
    )(q, k, vt)


def combine_kernel(heads, part_ref, out_ref, got_ref, send_sem, recv_sem):
    t, z, y, x = position()
    barrier = pltpu.get_barrier_semaphore()
    peers = [(1 - t, z, y, x)] + [(c, z, y, turn(x, d)) for d in RING for c in range(2)]
    for peer in peers:
        pl.semaphore_signal(barrier, inc=1, device_id=device(*peer), device_id_type=MESH)
    pl.semaphore_wait(barrier, len(peers))
    mine = x * 2 + t
    sends = []
    for i, peer in enumerate(peers):
        copy = pltpu.make_async_remote_copy(
            src_ref=part_ref.at[peer[3] * 2 + peer[0]],
            dst_ref=got_ref.at[mine],
            send_sem=send_sem.at[i],
            recv_sem=recv_sem.at[mine],
            device_id=device(*peer),
            device_id_type=MESH,
        )
        copy.start()
        sends.append(copy)
    got_ref[mine] = part_ref[mine]
    for peer in peers:
        at = peer[3] * 2 + peer[0]
        pltpu.make_async_remote_copy(
            src_ref=got_ref.at[at],
            dst_ref=got_ref.at[at],
            send_sem=send_sem.at[0],
            recv_sem=recv_sem.at[at],
            device_id=device(t, z, y, x),
            device_id_type=MESH,
        ).wait_recv()
    width = heads * HEAD
    tokens = part_ref.shape[1]
    out_width = out_ref.shape[-1]
    head_of = lax.broadcasted_iota(jnp.int32, (tokens, out_width), 1) // HEAD

    def spread(columns):
        full = jnp.broadcast_to(columns[:, 0:1], (tokens, out_width))
        for h in range(1, heads):
            full = jnp.where(head_of == h, columns[:, h:h + 1], full)
        return full

    for c in range(2):
        blocks = [got_ref[2 * i + c] for i in range(SIDE)]
        tops = [b[:, width:width + heads] for b in blocks]
        top = functools.reduce(jnp.maximum, tops)
        fades = [jnp.exp(m - top) for m in tops]
        total = sum(f * b[:, width + heads:width + 2 * heads] for f, b in zip(fades, blocks))
        merged = sum(spread(f / total) * b[:, :out_width] for f, b in zip(fades, blocks))
        out_ref[c] = jnp.where(head_of < heads, merged, 0.0).astype(jnp.bfloat16)
    for copy in sends:
        copy.wait_send()


def combine(parts, heads, collective_id):
    _, tokens, lanes = parts.shape
    out_width = -(-heads * HEAD // 128) * 128
    vmem = pl.BlockSpec(memory_space=pltpu.VMEM)
    out = pl.pallas_call(
        functools.partial(combine_kernel, heads),
        out_shape=jax.ShapeDtypeStruct((2, tokens, out_width), jnp.bfloat16),
        in_specs=[vmem],
        out_specs=vmem,
        scratch_shapes=[
            pltpu.VMEM(parts.shape, jnp.float32),
            pltpu.SemaphoreType.DMA((ROW,)),
            pltpu.SemaphoreType.DMA((ROW,)),
        ],
        compiler_params=pltpu.CompilerParams(collective_id=collective_id, has_side_effects=True, vmem_limit_bytes=VMEM_LIMIT),
        name="combine",
    )(parts)
    return out[:, :, :heads * HEAD]


def exchange_kernel(spread, src_ref, dst_ref, send_sem, recv_sem):
    t, me = lax.axis_index("time"), lax.axis_index("region")
    barrier = pltpu.get_barrier_semaphore()

    def signal(d, _):
        pl.semaphore_signal(barrier, inc=1, device_id={"time": t, "region": lax.rem(me + d, REGIONS)}, device_id_type=MESH)
        return 0

    lax.fori_loop(1, REGIONS, signal, 0)
    pl.semaphore_wait(barrier, REGIONS - 1)

    def copy_to(peer, slot):
        return pltpu.make_async_remote_copy(
            src_ref=src_ref if spread else src_ref.at[peer],
            dst_ref=dst_ref.at[slot],
            send_sem=send_sem.at[peer],
            recv_sem=recv_sem.at[slot],
            device_id={"time": t, "region": peer},
            device_id_type=MESH,
        )

    def start(d, _):
        copy_to(lax.rem(me + d, REGIONS), me).start()
        return 0

    lax.fori_loop(1, REGIONS, start, 0)
    dst_ref[me] = src_ref[...] if spread else src_ref[me]

    def finish(d, _):
        peer = lax.rem(me + d, REGIONS)
        copy_to(peer, peer).wait_recv()
        return 0

    lax.fori_loop(1, REGIONS, finish, 0)

    def drain(d, _):
        copy_to(lax.rem(me + d, REGIONS), me).wait_send()
        return 0

    lax.fori_loop(1, REGIONS, drain, 0)


def exchange(rows, spread, collective_id):
    block = rows.shape if spread else rows.shape[1:]
    vmem = pl.BlockSpec(memory_space=pltpu.VMEM)
    return pl.pallas_call(
        functools.partial(exchange_kernel, spread),
        out_shape=jax.ShapeDtypeStruct((REGIONS,) + block, rows.dtype),
        in_specs=[vmem],
        out_specs=vmem,
        scratch_shapes=[pltpu.SemaphoreType.DMA((REGIONS,)), pltpu.SemaphoreType.DMA((REGIONS,))],
        compiler_params=pltpu.CompilerParams(collective_id=collective_id, has_side_effects=True),
        name="exchange",
    )(rows)


def layer_norm(hidden, ln_gain, ln_shift):
    hid_f32 = hidden.astype(jnp.float32)
    mean_val = jnp.mean(hid_f32, axis=-1, keepdims=True)
    centered = hid_f32 - mean_val
    variance = jnp.mean(centered * centered, axis=-1, keepdims=True)
    return centered * lax.rsqrt(variance + LN_EPS) * ln_gain + ln_shift


def run_block(hidden, vec_rows, w_qkv, w_o, w_one, w_two, key_block, collective_id):
    tokens, width = hidden.shape
    heads = w_qkv.shape[2] // 2
    half = heads * HEAD
    normed = layer_norm(hidden, vec_rows[0], vec_rows[1]).astype(jnp.bfloat16)
    w_rows = w_qkv.transpose(1, 2, 3, 0).reshape(3 * width, width)
    projected = lax.dot_general(normed, w_rows, (((1,), (1,)), ((), ())), preferred_element_type=jnp.float32)
    bias = jnp.concatenate([vec_rows[4], jnp.zeros_like(vec_rows[4]), vec_rows[5]])
    projected = (projected + bias).astype(jnp.bfloat16)

    def halves(part):
        return jnp.stack([projected[:, part * width + c * half:part * width + (c + 1) * half] for c in range(2)])

    q, k, v = halves(0) * jnp.bfloat16(HEAD ** -0.5), halves(1), halves(2)
    if half % 128 == 0:
        a, b = k, v
    else:
        both = jnp.concatenate([k, v], axis=-1)
        a, b = both[:, :tokens // 2], both[:, tokens // 2:]
    kv_all, q_all = gather(a, b, q, collective_id)
    if half % 128 == 0:
        keys = kv_all[0].reshape(-1, half)
        values_t = kv_all[1].reshape(-1, half).T
    else:
        keys = kv_all.reshape(-1, 2 * half)
        values_t = keys[:, half:].T
    count = ROW * tokens
    queries = q_all.reshape(count, heads, HEAD).transpose(1, 2, 0)
    padded = -(-count // 256) * 256
    rows = jnp.arange(heads) % 2
    zeros = jnp.zeros_like(queries)
    even = jnp.concatenate([queries, zeros], axis=1)
    odd = jnp.concatenate([zeros, queries], axis=1)
    queries = jnp.where((rows == 0)[:, None, None], even, odd)
    queries = jnp.pad(queries, ((0, 0), (0, 0), (0, padded - count)))
    parts = flash(queries, keys, values_t, key_block)[:count].reshape(ROW, tokens, -1)
    attended = combine(parts, heads, collective_id + 1)
    w_o = w_o.reshape(2, half, width)
    mixed = sum(jnp.dot(attended[c], w_o[c], preferred_element_type=jnp.float32) for c in range(2))
    residual = (hidden.astype(jnp.float32) + mixed + vec_rows[6]).astype(jnp.bfloat16)
    normed_mlp = layer_norm(residual, vec_rows[2], vec_rows[3]).astype(jnp.bfloat16)
    mlp_hidden = jax.nn.gelu(jnp.dot(normed_mlp, w_one, preferred_element_type=jnp.float32) + vec_rows[8:12].reshape(-1), approximate=False).astype(jnp.bfloat16)
    return (residual.astype(jnp.float32) + jnp.dot(mlp_hidden, w_two, preferred_element_type=jnp.float32) + vec_rows[7]).astype(jnp.bfloat16)


def one_hot_rows(selector, rows):
    return jnp.dot(selector.astype(jnp.bfloat16), rows, preferred_element_type=jnp.float32).astype(jnp.bfloat16)


def solution(mesh):
    def local_step(patches, enc_pos, vis_mask, dec_pos, w_embed, b_embed, enc_vec, enc_wqkv, enc_wo, enc_w1, enc_w2, enc_final, w_dec_in, mask_token, dec_vec, dec_wqkv, dec_wo, dec_w1, dec_w2, dec_final, w_out):
        tokens = patches.shape[0]
        per_dev = tokens // 8
        me = lax.axis_index("region")
        own_count = jnp.sum(vis_mask)
        counts = exchange(jnp.full((8, 128), own_count, jnp.int32), True, 1)[:, 0, 0]
        embedded = (jnp.dot(patches, w_embed, preferred_element_type=jnp.float32) + b_embed + enc_pos.astype(jnp.float32)).astype(jnp.bfloat16)

        region_ids = jnp.arange(REGIONS, dtype=jnp.int32)
        starts = jnp.sum(jnp.where(region_ids[None, :] < region_ids[:, None], counts[None, :], 0), axis=1)
        start = jnp.sum(jnp.where(region_ids < me, counts, 0))
        token_ids = jnp.arange(tokens, dtype=jnp.int32)
        local_rank = jnp.sum(jnp.where(token_ids[None, :] < token_ids[:, None], vis_mask[None, :], 0), axis=1)
        send_row = jnp.where(vis_mask == 1, lax.rem(start + local_rank, REGIONS) * 2 + local_rank // REGIONS, -1)
        row_ids = jnp.arange(2 * REGIONS, dtype=jnp.int32)
        deal = row_ids[:, None] == send_row[None, :]
        source_starts, source_counts = jnp.repeat(starts, 2), jnp.repeat(counts, 2)
        rank = lax.rem(me - lax.rem(source_starts, REGIONS) + REGIONS, REGIONS) + REGIONS * lax.rem(row_ids, 2)
        place = jnp.where(rank < source_counts, (source_starts + rank) // REGIONS, -1)
        pack = jnp.arange(per_dev, dtype=jnp.int32)[:, None] == place[None, :]

        sent = one_hot_rows(deal, embedded).reshape(REGIONS, 2, -1)
        hidden = one_hot_rows(pack, exchange(sent, False, 2).reshape(2 * REGIONS, -1))
        for layer in range(enc_vec.shape[0]):
            hidden = run_block(hidden, enc_vec[layer], enc_wqkv[layer], enc_wo[layer], enc_w1[layer], enc_w2[layer], 768, 4 + 2 * layer)
        latent = jnp.dot(layer_norm(hidden, enc_final[0], enc_final[1]).astype(jnp.bfloat16), w_dec_in, preferred_element_type=jnp.float32).astype(jnp.bfloat16)
        back = one_hot_rows(pack.T, latent).reshape(REGIONS, 2, -1)
        returned = exchange(back, False, 3).reshape(2 * REGIONS, -1)
        placed = jnp.dot(deal.T.astype(jnp.bfloat16), returned, preferred_element_type=jnp.float32)
        hidden = (jnp.where(vis_mask[:, None] == 1, placed, mask_token.astype(jnp.float32)) + dec_pos.astype(jnp.float32)).astype(jnp.bfloat16)
        for layer in range(dec_vec.shape[0]):
            hidden = run_block(hidden, dec_vec[layer], dec_wqkv[layer], dec_wo[layer], dec_w1[layer], dec_w2[layer], 512, 8 + 2 * layer)
        return jnp.dot(layer_norm(hidden, dec_final[0], dec_final[1]).astype(jnp.bfloat16), w_out, preferred_element_type=jnp.float32)

    token_rows = P(TOKEN_AXES, None)
    token_flags = P(TOKEN_AXES)
    replicated = P()
    in_specs = (token_rows, token_rows, token_flags, token_rows) + (replicated,) * 17
    return jax.shard_map(local_step, mesh=mesh, in_specs=in_specs, out_specs=token_rows, check_vma=False)
```

```python
import functools
import jax
import jax.numpy as jnp
from jax import lax
from jax.experimental import pallas as pl
from jax.experimental.pallas import tpu as pltpu
from jax.sharding import PartitionSpec as P

LN_EPS = 1e-6
TOKEN_AXES = ("batch", "time", "region")
SIDE = 4
REGIONS = SIDE ** 3
PLANE = SIDE * SIDE * 2
ROW = SIDE * 2
HEAD = 64
MESH = pl.DeviceIdType.MESH
RING = (1, 3, 2)
VMEM_LIMIT = 60 * 1024 * 1024
LOG2E = 1.4426950408889634
SAFE_SCORE = 60.0
SAFE_VALUE = 1e7


def position():
    t, r = lax.axis_index("time"), lax.axis_index("region")
    return t, r // 16, lax.rem(r // 4, 4), lax.rem(r, 4)


def device(t, z, y, x):
    return {"time": t, "region": z * 16 + y * 4 + x}


def turn(a, d):
    return lax.rem(a + d, SIDE)


def gather_kernel(a_ref, b_ref, q_ref, kv_ref, qall_ref, a_send, a_recv, b_send, b_recv, q_send, q_recv):
    t, z, y, x = position()
    other = 1 - t
    barrier = pltpu.get_barrier_semaphore()
    peers = [(other, z, y, x)]
    for d in RING:
        for c in range(2):
            peers += [(c, turn(z, d), y, x), (c, z, turn(y, d), x), (c, z, y, turn(x, d))]
    for peer in peers:
        pl.semaphore_signal(barrier, inc=1, device_id=device(*peer), device_id_type=MESH)
    pl.semaphore_wait(barrier, len(peers))

    def slot(z_, y_, t_):
        return (z_ * SIDE + y_) * 2 + t_

    mine = slot(z, y, t)
    row_mine = x * 2 + t
    sends = []
    counts = {"a": 0, "b": 0, "q": 0}
    send_sems = {"a": a_send, "b": b_send, "q": q_send}
    recv_sems = {"a": a_recv, "b": b_recv, "q": q_recv}
    dests = {"a": kv_ref.at[0], "b": kv_ref.at[1], "q": qall_ref}
    sources = {"a": a_ref, "b": b_ref, "q": q_ref}

    def send(kind, src, to_slot, peer):
        copy = pltpu.make_async_remote_copy(
            src_ref=src,
            dst_ref=dests[kind].at[to_slot],
            send_sem=send_sems[kind].at[counts[kind]],
            recv_sem=recv_sems[kind].at[to_slot],
            device_id=device(*peer),
            device_id_type=MESH,
        )
        counts[kind] += 1
        copy.start()
        sends.append(copy)

    def arrived(kind, at):
        pltpu.make_async_remote_copy(
            src_ref=dests[kind].at[at],
            dst_ref=dests[kind].at[at],
            send_sem=send_sems[kind].at[0],
            recv_sem=recv_sems[kind].at[at],
            device_id=device(t, z, y, x),
            device_id_type=MESH,
        ).wait_recv()

    send("q", q_ref.at[other], row_mine, (other, z, y, x))
    send("a", a_ref.at[other], mine, (other, z, y, x))
    send("b", b_ref.at[other], mine, (other, z, y, x))
    for d in RING:
        for c in range(2):
            send("q", q_ref.at[c], row_mine, (c, z, y, turn(x, d)))
            send("a", a_ref.at[c], mine, (c, z, turn(y, d), x))
            send("b", b_ref.at[c], mine, (c, turn(z, d), y, x))
    for d in RING:
        send("a", a_ref.at[t], mine, (t, turn(z, d), y, x))
        send("b", b_ref.at[t], mine, (t, z, turn(y, d), x))
    kv_ref[0, mine] = a_ref[t]
    kv_ref[1, mine] = b_ref[t]
    qall_ref[row_mine] = q_ref[t]

    arrivals = [(0, other)] + [(4 - d, c) for d in RING for c in range(2)]
    for d0, c in arrivals:
        at = slot(z, turn(y, d0), c)
        arrived("a", at)
        for d in RING:
            send("a", dests["a"].at[at], at, (t, turn(z, d), y, x))
        at = slot(turn(z, d0), y, c)
        arrived("b", at)
        for d in RING:
            send("b", dests["b"].at[at], at, (t, z, turn(y, d), x))
    for dz in RING:
        for dy in range(SIDE):
            for c in range(2):
                arrived("a", slot(turn(z, dz), turn(y, dy), c))
                arrived("b", slot(turn(z, dy), turn(y, dz), c))
    for d0, c in arrivals:
        arrived("q", turn(x, d0) * 2 + c)
    for copy in sends:
        copy.wait_send()


def gather(a, b, q, collective_id):
    halves, rows, lanes = a.shape
    n = 31
    vmem = pl.BlockSpec(memory_space=pltpu.VMEM)
    return pl.pallas_call(
        gather_kernel,
        out_shape=(
            jax.ShapeDtypeStruct((2, PLANE, rows, lanes), a.dtype),
            jax.ShapeDtypeStruct((ROW,) + q.shape[1:], q.dtype),
        ),
        in_specs=[vmem] * 3,
        out_specs=(vmem, vmem),
        scratch_shapes=[
            pltpu.SemaphoreType.DMA((n,)),
            pltpu.SemaphoreType.DMA((PLANE,)),
            pltpu.SemaphoreType.DMA((n,)),
            pltpu.SemaphoreType.DMA((PLANE,)),
            pltpu.SemaphoreType.DMA((ROW,)),
            pltpu.SemaphoreType.DMA((ROW,)),
        ],
        compiler_params=pltpu.CompilerParams(collective_id=collective_id, has_side_effects=True, vmem_limit_bytes=VMEM_LIMIT),
        name="gather_kv",
    )(a, b, q)


def flash_kernel(heads, key_block, steps, v_lane, q_ref, k_ref, v_ref, out_ref, acc_ref, stat_ref, vt_ref, norm_ref):
    width = heads * HEAD
    lanes = q_ref.shape[-1]
    pairs = -(-heads // 2) * 128
    scale = HEAD ** -0.5
    v_base = v_lane % 128
    v_first = v_lane - v_base

    @pl.when(pl.program_id(0) == 0)
    def prepare():
        rows = lax.broadcasted_iota(jnp.int32, (pairs, 128), 0)
        cols = lax.broadcasted_iota(jnp.int32, (pairs, 128), 1)
        picks = ((rows // HEAD == cols) & (cols < heads)).astype(jnp.bfloat16)
        norm_ref[...] = jnp.zeros_like(norm_ref)

        def turn_block(i, _):
            at = pl.multiple_of(i * key_block, key_block)
            values = v_ref[pl.ds(at, key_block), v_first:v_first + vt_ref.shape[0]]
            vt_ref[:, pl.ds(at, key_block)] = values.T
            k_rows = k_ref[pl.ds(at, key_block), :pairs].astype(jnp.float32)
            sums = jnp.dot((k_rows * k_rows).astype(jnp.bfloat16), picks, preferred_element_type=jnp.float32)
            norm_ref[0] = jnp.maximum(norm_ref[0], jnp.max(sums.reshape(key_block // 8, 8, 128), axis=0))
            sizes = jnp.abs(values.astype(jnp.float32))
            for j in range(vt_ref.shape[0] // 128):
                part = sizes[:, j * 128:(j + 1) * 128].reshape(key_block // 8, 8, 128)
                norm_ref[1] = jnp.maximum(norm_ref[1], jnp.max(part, axis=0))
            return 0

        lax.fori_loop(0, steps, turn_block, 0)

    acc_ref[...] = jnp.zeros_like(acc_ref)
    stat_ref[...] = jnp.zeros_like(stat_ref)
    k_norm = jnp.max(norm_ref[0], axis=0, keepdims=True)
    lane = lax.broadcasted_iota(jnp.int32, (1, 128), 1)
    bound = jnp.zeros((1, 128), jnp.float32)
    for h in range(heads):
        q_rows = q_ref[h].astype(jnp.float32)
        q_norm = jnp.max(jnp.sum(q_rows * q_rows, axis=0, keepdims=True), axis=1, keepdims=True)
        bound = jnp.where(lane == h, q_norm * k_norm, bound)
    limit = (SAFE_SCORE / scale) ** 2 / 1.05
    safe = (jnp.max(bound) <= limit) & (jnp.max(norm_ref[1]) <= SAFE_VALUE)

    def scores_of(at, size, h):
        k_rows = k_ref[pl.ds(at, size), (h // 2) * 128:(h // 2 + 1) * 128]
        return jnp.dot(k_rows, q_ref[h], preferred_element_type=jnp.float32)

    def weighted(at, size, h, weights):
        values = vt_ref[v_base + h * HEAD:v_base + (h + 1) * HEAD, pl.ds(at, size)]
        return jnp.dot(values, weights.astype(jnp.bfloat16), preferred_element_type=jnp.float32)

    @pl.when(safe)
    def plain():
        def step(i, _):
            at = pl.multiple_of(i * key_block, key_block)
            for h in range(heads):
                weights = jnp.exp2(scores_of(at, key_block, h) * (scale * LOG2E))
                stat_ref[heads + h] += jnp.sum(weights.reshape(key_block // 8, 8, lanes), axis=0)
                acc_ref[h * HEAD:(h + 1) * HEAD] += weighted(at, key_block, h, weights)
            return 0

        lax.fori_loop(0, steps, step, 0)
        for h in range(heads):
            acc_ref[width + heads + h:width + heads + h + 1] = jnp.sum(stat_ref[heads + h], axis=0, keepdims=True)

    @pl.when(jnp.logical_not(safe))
    def shifted():
        size = 256
        for h in range(heads):
            stat_ref[h] = jnp.full((8, lanes), -jnp.inf, jnp.float32)

        def step(i, _):
            at = pl.multiple_of(i * size, size)
            for h in range(heads):
                scores = scores_of(at, size, h) * scale
                old = stat_ref[h, 0:1]
                new = jnp.maximum(old, jnp.max(scores, axis=0, keepdims=True))
                weights = jnp.exp(scores - new)
                fade = jnp.exp(old - new)
                stat_ref[h, 0:1] = new
                stat_ref[heads + h, 0:1] = stat_ref[heads + h, 0:1] * fade + jnp.sum(weights, axis=0, keepdims=True)
                acc_ref[h * HEAD:(h + 1) * HEAD] = acc_ref[h * HEAD:(h + 1) * HEAD] * fade + weighted(at, size, h, weights)
            return 0

        lax.fori_loop(0, steps * key_block // size, step, 0)
        for h in range(heads):
            acc_ref[width + h:width + h + 1] = stat_ref[h, 0:1]
            acc_ref[width + heads + h:width + heads + h + 1] = stat_ref[heads + h, 0:1]

    out_ref[...] = acc_ref[...].T


def flash(q, k, v, v_lane, key_block, block):
    heads, _, queries = q.shape
    keys, lanes = k.shape
    out_lanes = -(-(heads * HEAD + 2 * heads) // 128) * 128
    v_rows = v.shape[1] - v_lane // 128 * 128
    whole = pl.BlockSpec((keys, lanes), lambda i: (0, 0))
    return pl.pallas_call(
        functools.partial(flash_kernel, heads, key_block, keys // key_block, v_lane),
        grid=(queries // block,),
        out_shape=jax.ShapeDtypeStruct((queries, out_lanes), jnp.float32),
        in_specs=[pl.BlockSpec((heads, 128, block), lambda i: (0, 0, i)), whole, whole],
        out_specs=pl.BlockSpec((block, out_lanes), lambda i: (i, 0)),
        scratch_shapes=[
            pltpu.VMEM((out_lanes, block), jnp.float32),
            pltpu.VMEM((2 * heads, 8, block), jnp.float32),
            pltpu.VMEM((v_rows, keys), jnp.bfloat16),
            pltpu.VMEM((2, 8, 128), jnp.float32),
        ],
        compiler_params=pltpu.CompilerParams(vmem_limit_bytes=VMEM_LIMIT),
        name="flash",
    )(q, k, v)


def combine_kernel(heads, part_ref, out_ref, got_ref, send_sem, recv_sem):
    t, z, y, x = position()
    barrier = pltpu.get_barrier_semaphore()
    peers = [(1 - t, z, y, x)] + [(c, z, y, turn(x, d)) for d in RING for c in range(2)]
    for peer in peers:
        pl.semaphore_signal(barrier, inc=1, device_id=device(*peer), device_id_type=MESH)
    pl.semaphore_wait(barrier, len(peers))
    mine = x * 2 + t
    sends = []
    for i, peer in enumerate(peers):
        copy = pltpu.make_async_remote_copy(
            src_ref=part_ref.at[peer[3] * 2 + peer[0]],
            dst_ref=got_ref.at[mine],
            send_sem=send_sem.at[i],
            recv_sem=recv_sem.at[mine],
            device_id=device(*peer),
            device_id_type=MESH,
        )
        copy.start()
        sends.append(copy)
    got_ref[mine] = part_ref[mine]
    for peer in peers:
        at = peer[3] * 2 + peer[0]
        pltpu.make_async_remote_copy(
            src_ref=got_ref.at[at],
            dst_ref=got_ref.at[at],
            send_sem=send_sem.at[0],
            recv_sem=recv_sem.at[at],
            device_id=device(t, z, y, x),
            device_id_type=MESH,
        ).wait_recv()
    width = heads * HEAD
    tokens = part_ref.shape[1]
    out_width = out_ref.shape[-1]
    head_of = lax.broadcasted_iota(jnp.int32, (tokens, out_width), 1) // HEAD

    def spread(columns):
        full = jnp.broadcast_to(columns[:, 0:1], (tokens, out_width))
        for h in range(1, heads):
            full = jnp.where(head_of == h, columns[:, h:h + 1], full)
        return full

    for c in range(2):
        blocks = [got_ref[2 * i + c] for i in range(SIDE)]
        tops = [b[:, width:width + heads] for b in blocks]
        top = functools.reduce(jnp.maximum, tops)
        fades = [jnp.exp(m - top) for m in tops]
        total = sum(f * b[:, width + heads:width + 2 * heads] for f, b in zip(fades, blocks))
        merged = sum(spread(f / total) * b[:, :out_width] for f, b in zip(fades, blocks))
        out_ref[c] = jnp.where(head_of < heads, merged, 0.0).astype(jnp.bfloat16)
    for copy in sends:
        copy.wait_send()


def combine(parts, heads, collective_id):
    _, tokens, lanes = parts.shape
    out_width = -(-heads * HEAD // 128) * 128
    vmem = pl.BlockSpec(memory_space=pltpu.VMEM)
    out = pl.pallas_call(
        functools.partial(combine_kernel, heads),
        out_shape=jax.ShapeDtypeStruct((2, tokens, out_width), jnp.bfloat16),
        in_specs=[vmem],
        out_specs=vmem,
        scratch_shapes=[
            pltpu.VMEM(parts.shape, jnp.float32),
            pltpu.SemaphoreType.DMA((ROW,)),
            pltpu.SemaphoreType.DMA((ROW,)),
        ],
        compiler_params=pltpu.CompilerParams(collective_id=collective_id, has_side_effects=True, vmem_limit_bytes=VMEM_LIMIT),
        name="combine",
    )(parts)
    return out[:, :, :heads * HEAD]


def exchange_kernel(spread, src_ref, dst_ref, send_sem, recv_sem):
    t, me = lax.axis_index("time"), lax.axis_index("region")
    barrier = pltpu.get_barrier_semaphore()

    def signal(d, _):
        pl.semaphore_signal(barrier, inc=1, device_id={"time": t, "region": lax.rem(me + d, REGIONS)}, device_id_type=MESH)
        return 0

    lax.fori_loop(1, REGIONS, signal, 0)
    pl.semaphore_wait(barrier, REGIONS - 1)

    def start(d, _):
        peer = lax.rem(me + d, REGIONS)
        pltpu.make_async_remote_copy(
            src_ref=src_ref if spread else src_ref.at[peer],
            dst_ref=dst_ref.at[me],
            send_sem=send_sem,
            recv_sem=recv_sem,
            device_id={"time": t, "region": peer},
            device_id_type=MESH,
        ).start()
        return 0

    lax.fori_loop(1, REGIONS, start, 0)
    rest = dst_ref.at[pl.ds(0, REGIONS - 1)]
    everything = pltpu.make_async_remote_copy(
        src_ref=rest, dst_ref=rest, send_sem=send_sem, recv_sem=recv_sem, device_id={"time": t, "region": me}, device_id_type=MESH
    )
    everything.wait_recv()
    everything.wait_send()
    dst_ref[me] = src_ref[...] if spread else src_ref[me]


def exchange(rows, spread, collective_id):
    block = rows.shape if spread else rows.shape[1:]
    vmem = pl.BlockSpec(memory_space=pltpu.VMEM)
    return pl.pallas_call(
        functools.partial(exchange_kernel, spread),
        out_shape=jax.ShapeDtypeStruct((REGIONS,) + block, rows.dtype),
        in_specs=[vmem],
        out_specs=vmem,
        scratch_shapes=[pltpu.SemaphoreType.DMA, pltpu.SemaphoreType.DMA],
        compiler_params=pltpu.CompilerParams(collective_id=collective_id, has_side_effects=True),
        name="exchange",
    )(rows)


def layer_norm(hidden, ln_gain, ln_shift):
    hid_f32 = hidden.astype(jnp.float32)
    mean_val = jnp.mean(hid_f32, axis=-1, keepdims=True)
    centered = hid_f32 - mean_val
    variance = jnp.mean(centered * centered, axis=-1, keepdims=True)
    return centered * lax.rsqrt(variance + LN_EPS) * ln_gain + ln_shift


def run_block(hidden, vec_rows, w_qkv, w_o, w_one, w_two, collective_id):
    tokens, width = hidden.shape
    heads = w_qkv.shape[2] // 2
    half = heads * HEAD
    normed = layer_norm(hidden, vec_rows[0], vec_rows[1]).astype(jnp.bfloat16)
    w_rows = w_qkv.transpose(1, 2, 3, 0).reshape(3 * width, width)
    projected = lax.dot_general(normed, w_rows, (((1,), (1,)), ((), ())), preferred_element_type=jnp.float32)
    bias = jnp.concatenate([vec_rows[4], jnp.zeros_like(vec_rows[4]), vec_rows[5]])
    projected = (projected + bias).astype(jnp.bfloat16)

    def halves(part):
        return jnp.stack([projected[:, part * width + c * half:part * width + (c + 1) * half] for c in range(2)])

    q, k, v = halves(0), halves(1), halves(2)
    if half % 128 == 0:
        a, b = k, v
    else:
        both = jnp.concatenate([k, v], axis=-1)
        a, b = both[:, :tokens // 2], both[:, tokens // 2:]
    kv_all, q_all = gather(a, b, q, collective_id)
    if half % 128 == 0:
        keys, values, v_lane = kv_all[0].reshape(-1, half), kv_all[1].reshape(-1, half), 0
    else:
        keys = values = kv_all.reshape(-1, 2 * half)
        v_lane = half
    count = ROW * tokens
    queries = q_all.reshape(count, heads, HEAD).transpose(1, 2, 0)
    block = 512 if count % 512 == 0 else 256
    padded = -(-count // block) * block
    rows = jnp.arange(heads) % 2
    zeros = jnp.zeros_like(queries)
    even = jnp.concatenate([queries, zeros], axis=1)
    odd = jnp.concatenate([zeros, queries], axis=1)
    queries = jnp.where((rows == 0)[:, None, None], even, odd)
    queries = jnp.pad(queries, ((0, 0), (0, 0), (0, padded - count)))
    parts = flash(queries, keys, values, v_lane, 768, block)[:count].reshape(ROW, tokens, -1)
    attended = combine(parts, heads, collective_id + 1)
    w_o = w_o.reshape(2, half, width)
    mixed = sum(jnp.dot(attended[c], w_o[c], preferred_element_type=jnp.float32) for c in range(2))
    residual = (hidden.astype(jnp.float32) + mixed + vec_rows[6]).astype(jnp.bfloat16)
    normed_mlp = layer_norm(residual, vec_rows[2], vec_rows[3]).astype(jnp.bfloat16)
    mlp_hidden = jax.nn.gelu(jnp.dot(normed_mlp, w_one, preferred_element_type=jnp.float32) + vec_rows[8:12].reshape(-1), approximate=False).astype(jnp.bfloat16)
    return (residual.astype(jnp.float32) + jnp.dot(mlp_hidden, w_two, preferred_element_type=jnp.float32) + vec_rows[7]).astype(jnp.bfloat16)


def one_hot_rows(selector, rows):
    return jnp.dot(selector.astype(jnp.bfloat16), rows, preferred_element_type=jnp.float32).astype(jnp.bfloat16)


def solution(mesh):
    def local_step(patches, enc_pos, vis_mask, dec_pos, w_embed, b_embed, enc_vec, enc_wqkv, enc_wo, enc_w1, enc_w2, enc_final, w_dec_in, mask_token, dec_vec, dec_wqkv, dec_wo, dec_w1, dec_w2, dec_final, w_out):
        tokens = patches.shape[0]
        per_dev = tokens // 8
        me = lax.axis_index("region")
        own_count = jnp.sum(vis_mask)
        counts = exchange(jnp.full((8, 128), own_count, jnp.int32), True, 1)[:, 0, 0]
        embedded = (jnp.dot(patches, w_embed, preferred_element_type=jnp.float32) + b_embed + enc_pos.astype(jnp.float32)).astype(jnp.bfloat16)

        region_ids = jnp.arange(REGIONS, dtype=jnp.int32)
        starts = jnp.sum(jnp.where(region_ids[None, :] < region_ids[:, None], counts[None, :], 0), axis=1)
        start = jnp.sum(jnp.where(region_ids < me, counts, 0))
        token_ids = jnp.arange(tokens, dtype=jnp.int32)
        local_rank = jnp.sum(jnp.where(token_ids[None, :] < token_ids[:, None], vis_mask[None, :], 0), axis=1)
        send_row = jnp.where(vis_mask == 1, lax.rem(start + local_rank, REGIONS) * 2 + local_rank // REGIONS, -1)
        row_ids = jnp.arange(2 * REGIONS, dtype=jnp.int32)
        deal = row_ids[:, None] == send_row[None, :]
        source_starts, source_counts = jnp.repeat(starts, 2), jnp.repeat(counts, 2)
        rank = lax.rem(me - lax.rem(source_starts, REGIONS) + REGIONS, REGIONS) + REGIONS * lax.rem(row_ids, 2)
        place = jnp.where(rank < source_counts, (source_starts + rank) // REGIONS, -1)
        pack = jnp.arange(per_dev, dtype=jnp.int32)[:, None] == place[None, :]

        sent = one_hot_rows(deal, embedded).reshape(REGIONS, 2, -1)
        hidden = one_hot_rows(pack, exchange(sent, False, 2).reshape(2 * REGIONS, -1))
        for layer in range(enc_vec.shape[0]):
            hidden = run_block(hidden, enc_vec[layer], enc_wqkv[layer], enc_wo[layer], enc_w1[layer], enc_w2[layer], 4 + 2 * layer)
        latent = jnp.dot(layer_norm(hidden, enc_final[0], enc_final[1]).astype(jnp.bfloat16), w_dec_in, preferred_element_type=jnp.float32).astype(jnp.bfloat16)
        back = one_hot_rows(pack.T, latent).reshape(REGIONS, 2, -1)
        returned = exchange(back, False, 3).reshape(2 * REGIONS, -1)
        placed = jnp.dot(deal.T.astype(jnp.bfloat16), returned, preferred_element_type=jnp.float32)
        hidden = (jnp.where(vis_mask[:, None] == 1, placed, mask_token.astype(jnp.float32)) + dec_pos.astype(jnp.float32)).astype(jnp.bfloat16)
        for layer in range(dec_vec.shape[0]):
            hidden = run_block(hidden, dec_vec[layer], dec_wqkv[layer], dec_wo[layer], dec_w1[layer], dec_w2[layer], 8 + 2 * layer)
        return jnp.dot(layer_norm(hidden, dec_final[0], dec_final[1]).astype(jnp.bfloat16), w_out, preferred_element_type=jnp.float32)

    token_rows = P(TOKEN_AXES, None)
    token_flags = P(TOKEN_AXES)
    replicated = P()
    in_specs = (token_rows, token_rows, token_flags, token_rows) + (replicated,) * 17
    return jax.shard_map(local_step, mesh=mesh, in_specs=in_specs, out_specs=token_rows, check_vma=False)
```

```python
import functools
import jax
import jax.numpy as jnp
from jax import lax
from jax.experimental import pallas as pl
from jax.experimental.pallas import tpu as pltpu
from jax.sharding import PartitionSpec as P

LN_EPS = 1e-6
TOKEN_AXES = ("batch", "time", "region")
SIDE = 4
REGIONS = SIDE ** 3
PLANE = SIDE * SIDE * 2
ROW = SIDE * 2
HEAD = 64
MESH = pl.DeviceIdType.MESH
RING = (1, 3, 2)
VMEM_LIMIT = 60 * 1024 * 1024
LOG2E = 1.4426950408889634
SAFE_SCORE = 60.0
SAFE_VALUE = 1e7


def position():
    t, r = lax.axis_index("time"), lax.axis_index("region")
    return t, r // 16, lax.rem(r // 4, 4), lax.rem(r, 4)


def device(t, z, y, x):
    return {"time": t, "region": z * 16 + y * 4 + x}


def turn(a, d):
    return lax.rem(a + d, SIDE)


def gather_kernel(a_ref, b_ref, q_ref, kv_ref, qall_ref, a_send, a_recv, b_send, b_recv, q_send, q_recv):
    t, z, y, x = position()
    other = 1 - t
    barrier = pltpu.get_barrier_semaphore()
    peers = [(other, z, y, x)]
    for d in RING:
        for c in range(2):
            peers += [(c, turn(z, d), y, x), (c, z, turn(y, d), x), (c, z, y, turn(x, d))]
    for peer in peers:
        pl.semaphore_signal(barrier, inc=1, device_id=device(*peer), device_id_type=MESH)
    pl.semaphore_wait(barrier, len(peers))

    def slot(z_, y_, t_):
        return (z_ * SIDE + y_) * 2 + t_

    mine = slot(z, y, t)
    row_mine = x * 2 + t
    sends = []
    counts = {"a": 0, "b": 0, "q": 0}
    send_sems = {"a": a_send, "b": b_send, "q": q_send}
    recv_sems = {"a": a_recv, "b": b_recv, "q": q_recv}
    dests = {"a": kv_ref.at[0], "b": kv_ref.at[1], "q": qall_ref}
    sources = {"a": a_ref, "b": b_ref, "q": q_ref}

    def send(kind, src, to_slot, peer):
        copy = pltpu.make_async_remote_copy(
            src_ref=src,
            dst_ref=dests[kind].at[to_slot],
            send_sem=send_sems[kind].at[counts[kind]],
            recv_sem=recv_sems[kind].at[to_slot],
            device_id=device(*peer),
            device_id_type=MESH,
        )
        counts[kind] += 1
        copy.start()
        sends.append(copy)

    def arrived(kind, at):
        pltpu.make_async_remote_copy(
            src_ref=dests[kind].at[at],
            dst_ref=dests[kind].at[at],
            send_sem=send_sems[kind].at[0],
            recv_sem=recv_sems[kind].at[at],
            device_id=device(t, z, y, x),
            device_id_type=MESH,
        ).wait_recv()

    send("q", q_ref.at[other], row_mine, (other, z, y, x))
    send("a", a_ref.at[other], mine, (other, z, y, x))
    send("b", b_ref.at[other], mine, (other, z, y, x))
    for d in RING:
        for c in range(2):
            send("q", q_ref.at[c], row_mine, (c, z, y, turn(x, d)))
            send("a", a_ref.at[c], mine, (c, z, turn(y, d), x))
            send("b", b_ref.at[c], mine, (c, turn(z, d), y, x))
    for d in RING:
        send("a", a_ref.at[t], mine, (t, turn(z, d), y, x))
        send("b", b_ref.at[t], mine, (t, z, turn(y, d), x))
    kv_ref[0, mine] = a_ref[t]
    kv_ref[1, mine] = b_ref[t]
    qall_ref[row_mine] = q_ref[t]

    arrivals = [(0, other)] + [(4 - d, c) for d in RING for c in range(2)]
    for d0, c in arrivals:
        at = slot(z, turn(y, d0), c)
        arrived("a", at)
        for d in RING:
            send("a", dests["a"].at[at], at, (t, turn(z, d), y, x))
        at = slot(turn(z, d0), y, c)
        arrived("b", at)
        for d in RING:
            send("b", dests["b"].at[at], at, (t, z, turn(y, d), x))
    for dz in RING:
        for dy in range(SIDE):
            for c in range(2):
                arrived("a", slot(turn(z, dz), turn(y, dy), c))
                arrived("b", slot(turn(z, dy), turn(y, dz), c))
    for d0, c in arrivals:
        arrived("q", turn(x, d0) * 2 + c)
    for copy in sends:
        copy.wait_send()


def gather(a, b, q, collective_id):
    halves, rows, lanes = a.shape
    n = 31
    vmem = pl.BlockSpec(memory_space=pltpu.VMEM)
    return pl.pallas_call(
        gather_kernel,
        out_shape=(
            jax.ShapeDtypeStruct((2, PLANE, rows, lanes), a.dtype),
            jax.ShapeDtypeStruct((ROW,) + q.shape[1:], q.dtype),
        ),
        in_specs=[vmem] * 3,
        out_specs=(vmem, vmem),
        scratch_shapes=[
            pltpu.SemaphoreType.DMA((n,)),
            pltpu.SemaphoreType.DMA((PLANE,)),
            pltpu.SemaphoreType.DMA((n,)),
            pltpu.SemaphoreType.DMA((PLANE,)),
            pltpu.SemaphoreType.DMA((ROW,)),
            pltpu.SemaphoreType.DMA((ROW,)),
        ],
        compiler_params=pltpu.CompilerParams(collective_id=collective_id, has_side_effects=True, vmem_limit_bytes=VMEM_LIMIT),
        name="gather_kv",
    )(a, b, q)


def flash_kernel(heads, key_block, steps, v_lane, q_ref, k_ref, v_ref, out_ref, acc_ref, stat_ref, vt_ref, norm_ref):
    width = heads * HEAD
    lanes = q_ref.shape[-1]
    pairs = -(-heads // 2) * 128
    scale = HEAD ** -0.5
    v_base = v_lane % 128
    v_first = v_lane - v_base

    @pl.when(pl.program_id(0) == 0)
    def prepare():
        rows = lax.broadcasted_iota(jnp.int32, (pairs, 128), 0)
        cols = lax.broadcasted_iota(jnp.int32, (pairs, 128), 1)
        picks = ((rows // HEAD == cols) & (cols < heads)).astype(jnp.bfloat16)
        norm_ref[...] = jnp.zeros_like(norm_ref)

        def turn_block(i, _):
            at = pl.multiple_of(i * key_block, key_block)
            values = v_ref[pl.ds(at, key_block), v_first:v_first + vt_ref.shape[0]]
            vt_ref[:, pl.ds(at, key_block)] = values.T
            k_rows = k_ref[pl.ds(at, key_block), :pairs].astype(jnp.float32)
            sums = jnp.dot((k_rows * k_rows).astype(jnp.bfloat16), picks, preferred_element_type=jnp.float32)
            norm_ref[0] = jnp.maximum(norm_ref[0], jnp.max(sums.reshape(key_block // 8, 8, 128), axis=0))
            sizes = jnp.abs(values.astype(jnp.float32))
            for j in range(vt_ref.shape[0] // 128):
                part = sizes[:, j * 128:(j + 1) * 128].reshape(key_block // 8, 8, 128)
                norm_ref[1] = jnp.maximum(norm_ref[1], jnp.max(part, axis=0))
            return 0

        lax.fori_loop(0, steps, turn_block, 0)

    acc_ref[...] = jnp.zeros_like(acc_ref)
    stat_ref[...] = jnp.zeros_like(stat_ref)
    k_norm = jnp.max(norm_ref[0], axis=0, keepdims=True)
    lane = lax.broadcasted_iota(jnp.int32, (1, 128), 1)
    bound = jnp.zeros((1, 128), jnp.float32)
    for h in range(heads):
        q_rows = q_ref[h].astype(jnp.float32)
        q_norm = jnp.max(jnp.sum(q_rows * q_rows, axis=0, keepdims=True), axis=1, keepdims=True)
        bound = jnp.where(lane == h, q_norm * k_norm, bound)
    limit = (SAFE_SCORE / scale) ** 2 / 1.05
    safe = (jnp.max(bound) <= limit) & (jnp.max(norm_ref[1]) <= SAFE_VALUE)

    def scores_of(at, size, h):
        k_rows = k_ref[pl.ds(at, size), (h // 2) * 128:(h // 2 + 1) * 128]
        return jnp.dot(k_rows, q_ref[h], preferred_element_type=jnp.float32)

    def weighted(at, size, h, weights):
        values = vt_ref[v_base + h * HEAD:v_base + (h + 1) * HEAD, pl.ds(at, size)]
        return jnp.dot(values, weights.astype(jnp.bfloat16), preferred_element_type=jnp.float32)

    @pl.when(safe)
    def plain():
        def step(i, _):
            at = pl.multiple_of(i * key_block, key_block)
            for h in range(heads):
                weights = jnp.exp2(scores_of(at, key_block, h) * (scale * LOG2E))
                stat_ref[heads + h] += jnp.sum(weights.reshape(key_block // 8, 8, lanes), axis=0)
                acc_ref[h * HEAD:(h + 1) * HEAD] += weighted(at, key_block, h, weights)
            return 0

        lax.fori_loop(0, steps, step, 0)
        for h in range(heads):
            acc_ref[width + heads + h:width + heads + h + 1] = jnp.sum(stat_ref[heads + h], axis=0, keepdims=True)

    @pl.when(jnp.logical_not(safe))
    def shifted():
        size = 256
        for h in range(heads):
            stat_ref[h] = jnp.full((8, lanes), -jnp.inf, jnp.float32)

        def step(i, _):
            at = pl.multiple_of(i * size, size)
            for h in range(heads):
                scores = scores_of(at, size, h) * scale
                old = stat_ref[h, 0:1]
                new = jnp.maximum(old, jnp.max(scores, axis=0, keepdims=True))
                weights = jnp.exp(scores - new)
                fade = jnp.exp(old - new)
                stat_ref[h, 0:1] = new
                stat_ref[heads + h, 0:1] = stat_ref[heads + h, 0:1] * fade + jnp.sum(weights, axis=0, keepdims=True)
                acc_ref[h * HEAD:(h + 1) * HEAD] = acc_ref[h * HEAD:(h + 1) * HEAD] * fade + weighted(at, size, h, weights)
            return 0

        lax.fori_loop(0, steps * key_block // size, step, 0)
        for h in range(heads):
            acc_ref[width + h:width + h + 1] = stat_ref[h, 0:1]
            acc_ref[width + heads + h:width + heads + h + 1] = stat_ref[heads + h, 0:1]

    out_ref[...] = acc_ref[...].T


def flash(q, k, v, v_lane, key_block, block):
    heads, _, queries = q.shape
    keys, lanes = k.shape
    out_lanes = -(-(heads * HEAD + 2 * heads) // 128) * 128
    v_rows = v.shape[1] - v_lane // 128 * 128
    whole = pl.BlockSpec((keys, lanes), lambda i: (0, 0))
    return pl.pallas_call(
        functools.partial(flash_kernel, heads, key_block, keys // key_block, v_lane),
        grid=(queries // block,),
        out_shape=jax.ShapeDtypeStruct((queries, out_lanes), jnp.float32),
        in_specs=[pl.BlockSpec((heads, 128, block), lambda i: (0, 0, i)), whole, whole],
        out_specs=pl.BlockSpec((block, out_lanes), lambda i: (i, 0)),
        scratch_shapes=[
            pltpu.VMEM((out_lanes, block), jnp.float32),
            pltpu.VMEM((2 * heads, 8, block), jnp.float32),
            pltpu.VMEM((v_rows, keys), jnp.bfloat16),
            pltpu.VMEM((2, 8, 128), jnp.float32),
        ],
        compiler_params=pltpu.CompilerParams(vmem_limit_bytes=VMEM_LIMIT),
        name="flash",
    )(q, k, v)


def attend_kernel(heads, a_ref, b_ref, q_ref, part_ref, kv_ref, qz_ref, guard_ref, qall_ref, acc_ref, stat_ref, vt_ref, norm_ref, one_send, two_send, q_send, one_recv, chunk_recv, q_recv):
    t, z, y, x = position()
    other = 1 - t
    barrier = pltpu.get_barrier_semaphore()
    peers = [(other, z, y, x)]
    for d in RING:
        for c in range(2):
            peers += [(c, turn(z, d), y, x), (c, z, turn(y, d), x), (c, z, y, turn(x, d))]
    for peer in peers:
        pl.semaphore_signal(barrier, inc=1, device_id=device(*peer), device_id_type=MESH)
    pl.semaphore_wait(barrier, len(peers))

    sources = (a_ref, b_ref)
    lines = (z, y)
    places = (y, z)
    sends = []

    def along(half, first, d, c):
        return (c, z, turn(y, d), x) if (half == 0) == first else (c, turn(z, d), y, x)

    def send(src, dst, send_sem, recv_sem, peer):
        copy = pltpu.make_async_remote_copy(
            src_ref=src, dst_ref=dst, send_sem=send_sem, recv_sem=recv_sem, device_id=device(*peer), device_id_type=MESH
        )
        copy.start()
        sends.append(copy)

    def arrived(ref, recv_sem):
        pltpu.make_async_remote_copy(
            src_ref=ref, dst_ref=ref, send_sem=q_send.at[0], recv_sem=recv_sem, device_id=device(t, z, y, x), device_id_type=MESH
        ).wait_recv()

    def block(half, place, c):
        return kv_ref.at[half, lines[half], place * 2 + c]

    hops = [(0, other)] + [(d, c) for d in RING for c in range(2)]
    for i, (d, c) in enumerate(hops):
        send(q_ref.at[c], qall_ref.at[x * 2 + t], q_send.at[i], q_recv.at[x * 2 + t], (c, z, y, turn(x, d)))
        for half in range(2):
            mine = block(half, places[half], t)
            send(sources[half].at[c], mine, one_send.at[half, i], one_recv.at[half, places[half] * 2 + t], along(half, True, d, c))
    for half in range(2):
        for i, d in enumerate(RING):
            send(sources[half].at[t], block(half, places[half], t), two_send.at[half, i], chunk_recv.at[half, lines[half]], along(half, False, d, t))
        kv_ref[half, lines[half], places[half] * 2 + t] = sources[half][t]
    qall_ref[x * 2 + t] = q_ref[t]

    acc_ref[...] = jnp.zeros_like(acc_ref)
    stat_ref[...] = jnp.zeros_like(stat_ref)
    norm_ref[...] = jnp.zeros_like(norm_ref)

    late = []
    count = 3
    for step in range(4):
        for half in range(2):
            if step == 0:
                group = block(half, places[half], other)
                arrived(group, one_recv.at[half, places[half] * 2 + other])
            else:
                place = turn(places[half], 4 - RING[step - 1])
                for c in range(2):
                    arrived(block(half, place, c), one_recv.at[half, place * 2 + c])
                group = kv_ref.at[half, lines[half], pl.ds(place * 2, 2)]
            dst = group
            for i, d in enumerate(RING):
                args = (group, dst, two_send.at[half, 3 + step * 3 + i], chunk_recv.at[half, lines[half]], along(half, False, d, t))
                if d == 2:
                    late.append(args)
                else:
                    send(*args)
    for args in late:
        send(*args)

    for d, c in hops:
        at = turn(x, 4 - d) * 2 + c
        arrived(qall_ref.at[at], q_recv.at[at])
    tokens = q_ref.shape[1]
    count = ROW * tokens
    lanes = acc_ref.shape[-1]
    lane = lax.broadcasted_iota(jnp.int32, (1, 128), 1)
    q_norm = jnp.zeros((1, 128), jnp.float32)
    for p in range((heads + 1) // 2):
        turned = qall_ref[:, :, p * 128:(p + 1) * 128].reshape(count, 128).T
        zeros = jnp.zeros((HEAD, count), jnp.bfloat16)
        for h in range(2 * p, min(2 * p + 2, heads)):
            own = turned[(h % 2) * HEAD:(h % 2 + 1) * HEAD]
            qz_ref[h, (h % 2) * HEAD:(h % 2 + 1) * HEAD] = own
            qz_ref[h, (1 - h % 2) * HEAD:(2 - h % 2) * HEAD] = zeros
            size = jnp.sum(own.astype(jnp.float32) ** 2, axis=0, keepdims=True)
            q_norm = jnp.where(lane == h, jnp.max(size, axis=1, keepdims=True), q_norm)

    width = heads * HEAD
    v_first = width // 128 * 128
    v_base = width - v_first
    pairs = -(-heads // 2) * 128
    keys = ROW * a_ref.shape[1]
    rows = lax.broadcasted_iota(jnp.int32, (pairs, 128), 0)
    cols = lax.broadcasted_iota(jnp.int32, (pairs, 128), 1)
    picks = ((rows // HEAD == cols) & (cols < heads)).astype(jnp.bfloat16)

    def chunk(n, _):
        half = lax.rem(n, 2)
        j = n // 2
        ahead = j + j // 2 - 2 * (j // 3)
        line = turn((1 - half) * z + half * y, ahead)

        @pl.when(n >= 2)
        def ready():
            arrived(kv_ref.at[half, line], chunk_recv.at[half, line])

        def load(first, last):
            return kv_ref[half, line, :, :, first:last].reshape(keys, last - first)

        values = load(v_first, v_first + vt_ref.shape[0])
        vt_ref[...] = values.T
        sizes = jnp.abs(values.astype(jnp.float32))
        for p in range(vt_ref.shape[0] // 128):
            part = sizes[:, p * 128:(p + 1) * 128].reshape(keys // 8, 8, 128)
            norm_ref[1] = jnp.maximum(norm_ref[1], jnp.max(part, axis=0))
        k_rows = load(0, pairs).astype(jnp.float32)
        sums = jnp.dot((k_rows * k_rows).astype(jnp.bfloat16), picks, preferred_element_type=jnp.float32)
        norm_ref[0] = jnp.maximum(norm_ref[0], jnp.max(sums.reshape(keys // 8, 8, 128), axis=0))

        def query_block(b, _):
            at = pl.multiple_of(b * lanes, lanes)
            for h in range(heads):
                scores = jnp.dot(load(h // 2 * 128, h // 2 * 128 + 128), qz_ref[h, :, pl.ds(at, lanes)], preferred_element_type=jnp.float32)
                weights = jnp.exp2(scores * (HEAD ** -0.5 * LOG2E))
                stat_ref[b, h] += jnp.sum(weights.reshape(keys // 8, 8, lanes), axis=0)
                acc_ref[b, h * HEAD:(h + 1) * HEAD] += jnp.dot(vt_ref[v_base + h * HEAD:v_base + (h + 1) * HEAD], weights.astype(jnp.bfloat16), preferred_element_type=jnp.float32)
            return 0

        lax.fori_loop(0, count // lanes, query_block, 0)
        return 0

    lax.fori_loop(0, 8, chunk, 0)
    for b in range(count // lanes):
        for h in range(heads):
            acc_ref[b, width + heads + h:width + heads + h + 1] = jnp.sum(stat_ref[b, h], axis=0, keepdims=True)
        part_ref[b * lanes:(b + 1) * lanes] = acc_ref[b].T
    guard_ref[0] = jnp.broadcast_to(jnp.max(norm_ref[0], axis=0, keepdims=True) * q_norm, (8, 128))
    guard_ref[1] = norm_ref[1]
    for copy in sends:
        copy.wait_send()


def mend_kernel(heads, guard_ref, part_in, kv_ref, qz_ref, part_ref, keys_ref, q_ref, acc_ref, stat_ref, out_ref):
    del part_in
    limit = (SAFE_SCORE * HEAD ** 0.5) ** 2 / 1.05
    safe = (jnp.max(guard_ref[0]) <= limit) & (jnp.max(guard_ref[1]) <= SAFE_VALUE)

    @pl.when(jnp.logical_not(safe))
    def again():
        width = heads * HEAD
        lanes = q_ref.shape[-1]
        tokens = keys_ref.shape[-2]

        def query_block(b, _):
            at = pl.multiple_of(b * lanes, lanes)
            pltpu.sync_copy(qz_ref.at[:, :, pl.ds(at, lanes)], q_ref)
            acc_ref[...] = jnp.zeros_like(acc_ref)
            for h in range(heads):
                stat_ref[h] = jnp.full((8, lanes), -jnp.inf, jnp.float32)
                stat_ref[heads + h] = jnp.zeros((8, lanes), jnp.float32)

            def keys_block(i, _):
                pltpu.sync_copy(kv_ref.at[i // (4 * ROW), lax.rem(i // ROW, 4), lax.rem(i, ROW)], keys_ref)
                everything = keys_ref[...]
                values_t = everything.astype(jnp.float32).T.astype(jnp.bfloat16)
                for h in range(heads):
                    scores = jnp.dot(everything[:, h // 2 * 128:h // 2 * 128 + 128], q_ref[h], preferred_element_type=jnp.float32) * (HEAD ** -0.5)
                    old = stat_ref[h, 0:1]
                    new = jnp.maximum(old, jnp.max(scores, axis=0, keepdims=True))
                    weights = jnp.exp(scores - new)
                    fade = jnp.exp(old - new)
                    stat_ref[h, 0:1] = new
                    stat_ref[heads + h, 0:1] = stat_ref[heads + h, 0:1] * fade + jnp.sum(weights, axis=0, keepdims=True)
                    summed = jnp.dot(values_t[width + h * HEAD:width + (h + 1) * HEAD], weights.astype(jnp.bfloat16), preferred_element_type=jnp.float32)
                    acc_ref[h * HEAD:(h + 1) * HEAD] = acc_ref[h * HEAD:(h + 1) * HEAD] * fade + summed
                return 0

            lax.fori_loop(0, 8 * ROW, keys_block, 0)
            for h in range(heads):
                acc_ref[width + h:width + h + 1] = stat_ref[h, 0:1]
                acc_ref[width + heads + h:width + heads + h + 1] = stat_ref[heads + h, 0:1]
            out_ref[...] = acc_ref[...].T
            pltpu.sync_copy(out_ref, part_ref.at[pl.ds(at, lanes)])
            return 0

        lax.fori_loop(0, part_ref.shape[0] // lanes, query_block, 0)


def attend(a, b, q, heads, collective_id):
    _, rows, lanes = a.shape
    tokens = q.shape[1]
    count = ROW * tokens
    block = 512
    blocks = count // block
    out_lanes = -(-(heads * HEAD + 2 * heads) // 128) * 128
    v_rows = lanes - heads * HEAD // 128 * 128
    vmem = pl.BlockSpec(memory_space=pltpu.VMEM)
    anywhere = pl.BlockSpec(memory_space=pl.ANY)
    part, kv, qz, guard = pl.pallas_call(
        functools.partial(attend_kernel, heads),
        out_shape=(
            jax.ShapeDtypeStruct((count, out_lanes), jnp.float32),
            jax.ShapeDtypeStruct((2, SIDE, ROW, rows, lanes), a.dtype),
            jax.ShapeDtypeStruct((heads, 128, count), q.dtype),
            jax.ShapeDtypeStruct((2, 8, 128), jnp.float32),
        ),
        in_specs=[vmem] * 3,
        out_specs=(vmem,) * 4,
        scratch_shapes=[
            pltpu.VMEM((ROW,) + q.shape[1:], q.dtype),
            pltpu.VMEM((blocks, out_lanes, block), jnp.float32),
            pltpu.VMEM((blocks, heads, 8, block), jnp.float32),
            pltpu.VMEM((v_rows, ROW * rows), jnp.bfloat16),
            pltpu.VMEM((2, 8, 128), jnp.float32),
            pltpu.SemaphoreType.DMA((2, ROW)),
            pltpu.SemaphoreType.DMA((2, 15)),
            pltpu.SemaphoreType.DMA((ROW,)),
            pltpu.SemaphoreType.DMA((2, ROW)),
            pltpu.SemaphoreType.DMA((2, SIDE)),
            pltpu.SemaphoreType.DMA((ROW,)),
        ],
        compiler_params=pltpu.CompilerParams(collective_id=collective_id, has_side_effects=True, vmem_limit_bytes=VMEM_LIMIT),
        name="attend",
    )(a, b, q)
    return pl.pallas_call(
        functools.partial(mend_kernel, heads),
        out_shape=jax.ShapeDtypeStruct(part.shape, part.dtype),
        in_specs=[vmem, anywhere, anywhere, anywhere],
        out_specs=anywhere,
        input_output_aliases={1: 0},
        scratch_shapes=[
            pltpu.VMEM((rows, lanes), a.dtype),
            pltpu.VMEM((heads, 128, block), q.dtype),
            pltpu.VMEM((out_lanes, block), jnp.float32),
            pltpu.VMEM((2 * heads, 8, block), jnp.float32),
            pltpu.VMEM((block, out_lanes), jnp.float32),
        ],
        compiler_params=pltpu.CompilerParams(vmem_limit_bytes=8 * 1024 * 1024),
        name="mend",
    )(guard, part, kv, qz)


def combine_kernel(heads, part_ref, out_ref, got_ref, send_sem, recv_sem):
    t, z, y, x = position()
    barrier = pltpu.get_barrier_semaphore()
    peers = [(1 - t, z, y, x)] + [(c, z, y, turn(x, d)) for d in RING for c in range(2)]
    for peer in peers:
        pl.semaphore_signal(barrier, inc=1, device_id=device(*peer), device_id_type=MESH)
    pl.semaphore_wait(barrier, len(peers))
    mine = x * 2 + t
    sends = []
    for i, peer in enumerate(peers):
        copy = pltpu.make_async_remote_copy(
            src_ref=part_ref.at[peer[3] * 2 + peer[0]],
            dst_ref=got_ref.at[mine],
            send_sem=send_sem.at[i],
            recv_sem=recv_sem.at[mine],
            device_id=device(*peer),
            device_id_type=MESH,
        )
        copy.start()
        sends.append(copy)
    got_ref[mine] = part_ref[mine]
    for peer in peers:
        at = peer[3] * 2 + peer[0]
        pltpu.make_async_remote_copy(
            src_ref=got_ref.at[at],
            dst_ref=got_ref.at[at],
            send_sem=send_sem.at[0],
            recv_sem=recv_sem.at[at],
            device_id=device(t, z, y, x),
            device_id_type=MESH,
        ).wait_recv()
    width = heads * HEAD
    tokens = part_ref.shape[1]
    out_width = out_ref.shape[-1]
    head_of = lax.broadcasted_iota(jnp.int32, (tokens, out_width), 1) // HEAD

    def spread(columns):
        full = jnp.broadcast_to(columns[:, 0:1], (tokens, out_width))
        for h in range(1, heads):
            full = jnp.where(head_of == h, columns[:, h:h + 1], full)
        return full

    for c in range(2):
        blocks = [got_ref[2 * i + c] for i in range(SIDE)]
        tops = [b[:, width:width + heads] for b in blocks]
        top = functools.reduce(jnp.maximum, tops)
        fades = [jnp.exp(m - top) for m in tops]
        total = sum(f * b[:, width + heads:width + 2 * heads] for f, b in zip(fades, blocks))
        merged = sum(spread(f / total) * b[:, :out_width] for f, b in zip(fades, blocks))
        out_ref[c] = jnp.where(head_of < heads, merged, 0.0).astype(jnp.bfloat16)
    for copy in sends:
        copy.wait_send()


def combine(parts, heads, collective_id):
    _, tokens, lanes = parts.shape
    out_width = -(-heads * HEAD // 128) * 128
    vmem = pl.BlockSpec(memory_space=pltpu.VMEM)
    out = pl.pallas_call(
        functools.partial(combine_kernel, heads),
        out_shape=jax.ShapeDtypeStruct((2, tokens, out_width), jnp.bfloat16),
        in_specs=[vmem],
        out_specs=vmem,
        scratch_shapes=[
            pltpu.VMEM(parts.shape, jnp.float32),
            pltpu.SemaphoreType.DMA((ROW,)),
            pltpu.SemaphoreType.DMA((ROW,)),
        ],
        compiler_params=pltpu.CompilerParams(collective_id=collective_id, has_side_effects=True, vmem_limit_bytes=VMEM_LIMIT),
        name="combine",
    )(parts)
    return out[:, :, :heads * HEAD]


def exchange_kernel(spread, src_ref, dst_ref, send_sem, recv_sem):
    t, me = lax.axis_index("time"), lax.axis_index("region")
    barrier = pltpu.get_barrier_semaphore()

    def signal(d, _):
        pl.semaphore_signal(barrier, inc=1, device_id={"time": t, "region": lax.rem(me + d, REGIONS)}, device_id_type=MESH)
        return 0

    lax.fori_loop(1, REGIONS, signal, 0)
    pl.semaphore_wait(barrier, REGIONS - 1)

    def start(d, _):
        peer = lax.rem(me + d, REGIONS)
        pltpu.make_async_remote_copy(
            src_ref=src_ref if spread else src_ref.at[peer],
            dst_ref=dst_ref.at[me],
            send_sem=send_sem,
            recv_sem=recv_sem,
            device_id={"time": t, "region": peer},
            device_id_type=MESH,
        ).start()
        return 0

    lax.fori_loop(1, REGIONS, start, 0)
    rest = dst_ref.at[pl.ds(0, REGIONS - 1)]
    everything = pltpu.make_async_remote_copy(
        src_ref=rest, dst_ref=rest, send_sem=send_sem, recv_sem=recv_sem, device_id={"time": t, "region": me}, device_id_type=MESH
    )
    everything.wait_recv()
    everything.wait_send()
    dst_ref[me] = src_ref[...] if spread else src_ref[me]


def exchange(rows, spread, collective_id):
    block = rows.shape if spread else rows.shape[1:]
    vmem = pl.BlockSpec(memory_space=pltpu.VMEM)
    return pl.pallas_call(
        functools.partial(exchange_kernel, spread),
        out_shape=jax.ShapeDtypeStruct((REGIONS,) + block, rows.dtype),
        in_specs=[vmem],
        out_specs=vmem,
        scratch_shapes=[pltpu.SemaphoreType.DMA, pltpu.SemaphoreType.DMA],
        compiler_params=pltpu.CompilerParams(collective_id=collective_id, has_side_effects=True),
        name="exchange",
    )(rows)


def gather_then_attend(q, k, v, heads, collective_id):
    tokens, half = q.shape[1:]
    kv_all, q_all = gather(k, v, q, collective_id)
    keys, values = kv_all[0].reshape(-1, half), kv_all[1].reshape(-1, half)
    count = ROW * tokens
    queries = q_all.reshape(count, heads, HEAD).transpose(1, 2, 0)
    padded = -(-count // 256) * 256
    zeros = jnp.zeros_like(queries)
    even = jnp.concatenate([queries, zeros], axis=1)
    odd = jnp.concatenate([zeros, queries], axis=1)
    queries = jnp.where((jnp.arange(heads) % 2 == 0)[:, None, None], even, odd)
    queries = jnp.pad(queries, ((0, 0), (0, 0), (0, padded - count)))
    return flash(queries, keys, values, 0, 768, 256)[:count]


def layer_norm(hidden, ln_gain, ln_shift):
    hid_f32 = hidden.astype(jnp.float32)
    mean_val = jnp.mean(hid_f32, axis=-1, keepdims=True)
    centered = hid_f32 - mean_val
    variance = jnp.mean(centered * centered, axis=-1, keepdims=True)
    return centered * lax.rsqrt(variance + LN_EPS) * ln_gain + ln_shift


def run_block(hidden, vec_rows, w_qkv, w_o, w_one, w_two, collective_id):
    tokens, width = hidden.shape
    heads = w_qkv.shape[2] // 2
    half = heads * HEAD
    normed = layer_norm(hidden, vec_rows[0], vec_rows[1]).astype(jnp.bfloat16)
    w_rows = w_qkv.transpose(1, 2, 3, 0).reshape(3 * width, width)
    projected = lax.dot_general(normed, w_rows, (((1,), (1,)), ((), ())), preferred_element_type=jnp.float32)
    bias = jnp.concatenate([vec_rows[4], jnp.zeros_like(vec_rows[4]), vec_rows[5]])
    projected = (projected + bias).astype(jnp.bfloat16)

    def halves(part):
        return jnp.stack([projected[:, part * width + c * half:part * width + (c + 1) * half] for c in range(2)])

    q, k, v = halves(0), halves(1), halves(2)
    count = ROW * tokens
    if half % 128 == 0:
        parts = gather_then_attend(q, k, v, heads, collective_id)
    else:
        both = jnp.concatenate([k, v], axis=-1)
        q = jnp.pad(q, ((0, 0), (0, 0), (0, -half % 128)))
        parts = attend(both[:, :tokens // 2], both[:, tokens // 2:], q, heads, collective_id)
    parts = parts.reshape(ROW, tokens, -1)
    attended = combine(parts, heads, collective_id + 1)
    w_o = w_o.reshape(2, half, width)
    mixed = sum(jnp.dot(attended[c], w_o[c], preferred_element_type=jnp.float32) for c in range(2))
    residual = (hidden.astype(jnp.float32) + mixed + vec_rows[6]).astype(jnp.bfloat16)
    normed_mlp = layer_norm(residual, vec_rows[2], vec_rows[3]).astype(jnp.bfloat16)
    mlp_hidden = jax.nn.gelu(jnp.dot(normed_mlp, w_one, preferred_element_type=jnp.float32) + vec_rows[8:12].reshape(-1), approximate=False).astype(jnp.bfloat16)
    return (residual.astype(jnp.float32) + jnp.dot(mlp_hidden, w_two, preferred_element_type=jnp.float32) + vec_rows[7]).astype(jnp.bfloat16)


def one_hot_rows(selector, rows):
    return jnp.dot(selector.astype(jnp.bfloat16), rows, preferred_element_type=jnp.float32).astype(jnp.bfloat16)


def solution(mesh):
    def local_step(patches, enc_pos, vis_mask, dec_pos, w_embed, b_embed, enc_vec, enc_wqkv, enc_wo, enc_w1, enc_w2, enc_final, w_dec_in, mask_token, dec_vec, dec_wqkv, dec_wo, dec_w1, dec_w2, dec_final, w_out):
        tokens = patches.shape[0]
        per_dev = tokens // 8
        me = lax.axis_index("region")
        own_count = jnp.sum(vis_mask)
        counts = exchange(jnp.full((8, 128), own_count, jnp.int32), True, 1)[:, 0, 0]
        embedded = (jnp.dot(patches, w_embed, preferred_element_type=jnp.float32) + b_embed + enc_pos.astype(jnp.float32)).astype(jnp.bfloat16)

        region_ids = jnp.arange(REGIONS, dtype=jnp.int32)
        starts = jnp.sum(jnp.where(region_ids[None, :] < region_ids[:, None], counts[None, :], 0), axis=1)
        start = jnp.sum(jnp.where(region_ids < me, counts, 0))
        token_ids = jnp.arange(tokens, dtype=jnp.int32)
        local_rank = jnp.sum(jnp.where(token_ids[None, :] < token_ids[:, None], vis_mask[None, :], 0), axis=1)
        send_row = jnp.where(vis_mask == 1, lax.rem(start + local_rank, REGIONS) * 2 + local_rank // REGIONS, -1)
        row_ids = jnp.arange(2 * REGIONS, dtype=jnp.int32)
        deal = row_ids[:, None] == send_row[None, :]
        source_starts, source_counts = jnp.repeat(starts, 2), jnp.repeat(counts, 2)
        rank = lax.rem(me - lax.rem(source_starts, REGIONS) + REGIONS, REGIONS) + REGIONS * lax.rem(row_ids, 2)
        place = jnp.where(rank < source_counts, (source_starts + rank) // REGIONS, -1)
        pack = jnp.arange(per_dev, dtype=jnp.int32)[:, None] == place[None, :]

        sent = one_hot_rows(deal, embedded).reshape(REGIONS, 2, -1)
        hidden = one_hot_rows(pack, exchange(sent, False, 2).reshape(2 * REGIONS, -1))
        for layer in range(enc_vec.shape[0]):
            hidden = run_block(hidden, enc_vec[layer], enc_wqkv[layer], enc_wo[layer], enc_w1[layer], enc_w2[layer], 4 + 2 * layer)
        latent = jnp.dot(layer_norm(hidden, enc_final[0], enc_final[1]).astype(jnp.bfloat16), w_dec_in, preferred_element_type=jnp.float32).astype(jnp.bfloat16)
        back = one_hot_rows(pack.T, latent).reshape(REGIONS, 2, -1)
        returned = exchange(back, False, 3).reshape(2 * REGIONS, -1)
        placed = jnp.dot(deal.T.astype(jnp.bfloat16), returned, preferred_element_type=jnp.float32)
        hidden = (jnp.where(vis_mask[:, None] == 1, placed, mask_token.astype(jnp.float32)) + dec_pos.astype(jnp.float32)).astype(jnp.bfloat16)
        for layer in range(dec_vec.shape[0]):
            hidden = run_block(hidden, dec_vec[layer], dec_wqkv[layer], dec_wo[layer], dec_w1[layer], dec_w2[layer], 8 + 2 * layer)
        return jnp.dot(layer_norm(hidden, dec_final[0], dec_final[1]).astype(jnp.bfloat16), w_out, preferred_element_type=jnp.float32)

    token_rows = P(TOKEN_AXES, None)
    token_flags = P(TOKEN_AXES)
    replicated = P()
    in_specs = (token_rows, token_rows, token_flags, token_rows) + (replicated,) * 17
    return jax.shard_map(local_step, mesh=mesh, in_specs=in_specs, out_specs=token_rows, check_vma=False)
```

```python
import functools
import jax
import jax.numpy as jnp
from jax import lax
from jax.experimental import pallas as pl
from jax.experimental.pallas import tpu as pltpu
from jax.sharding import PartitionSpec as P

LN_EPS = 1e-6
TOKEN_AXES = ("batch", "time", "region")
SIDE = 4
REGIONS = SIDE ** 3
ROW = SIDE * 2
HEAD = 64
MESH = pl.DeviceIdType.MESH
NEAR = (1, SIDE - 1)
VMEM_LIMIT = 60 * 1024 * 1024
LOG2E = 1.4426950408889634
SAFE_SCORE = 60.0
SAFE_VALUE = 1e7


def position():
    t, r = lax.axis_index("time"), lax.axis_index("region")
    return t, r // 16, lax.rem(r // 4, 4), lax.rem(r, 4)


def device(t, z, y, x):
    return {"time": t, "region": z * 16 + y * 4 + x}


def turn(a, d):
    return lax.rem(a + d, SIDE)


def signal_all(peers):
    barrier = pltpu.get_barrier_semaphore()
    for peer in peers:
        pl.semaphore_signal(barrier, inc=1, device_id=device(*peer), device_id_type=MESH)
    pl.semaphore_wait(barrier, len(peers))


class Sender:
    def __init__(self, sems, place):
        self.sems, self.place, self.used, self.started = sems, place, 0, []

    def __call__(self, src, dst, recv_sem, peer):
        copy = remote_copy(src, dst, self.sems.at[self.used], recv_sem, peer)
        copy.start()
        self.used += 1
        self.started.append(copy)

    def arrived(self, ref, recv_sem):
        remote_copy(ref, ref, self.sems.at[0], recv_sem, self.place).wait_recv()

    def drain(self):
        for copy in self.started:
            copy.wait_send()


def remote_copy(src, dst, send_sem, recv_sem, peer):
    return pltpu.make_async_remote_copy(
        src_ref=src, dst_ref=dst, send_sem=send_sem, recv_sem=recv_sem, device_id=device(*peer), device_id_type=MESH
    )


def attend_kernel(heads, a_ref, b_ref, q_ref, part_ref, kva_ref, kvb_ref, qz_ref, guard_ref, qall_ref, acc_ref, stat_ref, vta_ref, vtb_ref, norm_ref, send_sem, one_recv, chunk_recv, q_recv):
    t, z, y, x = position()
    other = 1 - t
    near = [(0, other)] + [(d, c) for d in NEAR for c in range(2)]
    peers = [(other, z, y, x)]
    for d, c in near[1:]:
        peers += [(c, turn(z, d), y, x), (c, z, turn(y, d), x), (c, z, y, turn(x, d))]
    signal_all(peers)

    sources, chunks, turned_values = (a_ref, b_ref), (kva_ref, kvb_ref), (vta_ref, vtb_ref)
    lines, places = (z, y), (y, z)
    send = Sender(send_sem, (t, z, y, x))

    def along(half, first, d, c):
        return (c, z, turn(y, d), x) if (half == 0) == first else (c, turn(z, d), y, x)

    def block(half, place, c, size=1):
        at = chunks[half].at[lines[half]]
        return at.at[place * 2 + c] if size == 1 else at.at[pl.ds(place * 2, size)]

    def one(half, place, c):
        return one_recv.at[half, place * 2 + c]

    def onward(half, ref):
        for d in NEAR:
            send(ref, ref, chunk_recv.at[half, lines[half]], along(half, False, d, t))

    row = x * 2 + t
    for d, c in near:
        send(q_ref.at[c], qall_ref.at[row], q_recv.at[row], (c, z, y, turn(x, d)))
        for half in range(2):
            send(sources[half].at[c], block(half, places[half], t), one(half, places[half], t), along(half, True, d, c))
    for half in range(2):
        for d in NEAR:
            send(sources[half].at[t], block(half, places[half], t), chunk_recv.at[half, lines[half]], along(half, False, d, t))
        chunks[half][lines[half], places[half] * 2 + t] = sources[half][t]
    qall_ref[row] = q_ref[t]

    acc_ref[...] = jnp.zeros_like(acc_ref)
    stat_ref[...] = jnp.zeros_like(stat_ref)
    norm_ref[...] = jnp.zeros_like(norm_ref)
    qz_ref[...] = jnp.zeros_like(qz_ref)

    def q_arrived(d, c):
        at = turn(x, SIDE - d) * 2 + c
        send.arrived(qall_ref.at[at], q_recv.at[at])
        return at

    for d, relayed in zip(NEAR, range(2)):
        for c in range(2):
            at = q_arrived(d, c)
            if c == relayed:
                send(qall_ref.at[at], qall_ref.at[at], q_recv.at[at], (t, z, y, turn(x, d)))
        for half in range(2):
            place = turn(places[half], SIDE - d)
            for c in range(2):
                send.arrived(block(half, place, c), one(half, place, c))
            ref = block(half, place, relayed)
            send(ref, ref, one(half, place, relayed), along(half, True, d, t))
            onward(half, block(half, place, 0, 2))
    q_arrived(0, other)
    for half in range(2):
        ref = block(half, places[half], other)
        send.arrived(ref, one(half, places[half], other))
        onward(half, ref)
    for half in range(2):
        place = turn(places[half], 2)
        for c in range(2):
            send.arrived(block(half, place, c), one(half, place, c))
        onward(half, block(half, place, 0, 2))
    for c in range(2):
        q_arrived(2, c)

    rows = q_ref.shape[1]
    count = ROW * rows
    padded = qz_ref.shape[-1] * heads * HEAD // q_ref.shape[-1]
    lane = lax.broadcasted_iota(jnp.int32, (1, 128), 1)
    q_norm = jnp.zeros((1, 128), jnp.float32)
    for p in range(q_ref.shape[-1] // 128):
        flat = qall_ref[:, :, p * 128:(p + 1) * 128].reshape(count, 128)
        if padded > count:
            flat = jnp.concatenate([flat, jnp.zeros((padded - count, 128), flat.dtype)], axis=0)
        turned = flat.T
        for i in range(2):
            group, h = divmod(2 * p + i, heads)
            own = turned[i * HEAD:(i + 1) * HEAD]
            at = h % 2 * HEAD
            qz_ref[h, at:at + HEAD, group * padded:(group + 1) * padded] = own
            size = jnp.sum(own.astype(jnp.float32) ** 2, axis=0, keepdims=True)
            q_norm = jnp.where(lane == h, jnp.maximum(q_norm, jnp.max(size, axis=1, keepdims=True)), q_norm)

    width = heads * HEAD
    lanes = acc_ref.shape[-1]
    v_first = width // 128 * 128
    v_base = width - v_first
    pairs = -(-heads // 2) * 128
    picks = lax.broadcasted_iota(jnp.int32, (pairs, 128), 0) // HEAD == lax.broadcasted_iota(jnp.int32, (pairs, 128), 1)
    picks = (picks & (lane < heads)).astype(jnp.bfloat16)
    far = [len(send.started) + i for i in range(4)]

    def passed_on(half, i):
        d = NEAR[i]
        line = turn(lines[half], SIDE - d)
        ref = chunks[half].at[line, pl.ds(i * SIDE, SIDE)]
        return remote_copy(ref, ref, send_sem.at[far[2 * half + i]], chunk_recv.at[half, line], along(half, False, d, t))

    def chunk(j, _):
        ahead = j + j // 2 - 2 * (j // 3)

        @pl.when(j == 1)
        def near_chunks():
            for i in range(2):
                for half in range(2):
                    line = turn(lines[half], SIDE - NEAR[i])
                    send.arrived(chunks[half].at[line], chunk_recv.at[half, line])
                    passed_on(half, i).start()

        @pl.when(j == 3)
        def far_chunks():
            for half in range(2):
                line = turn(lines[half], 2)
                send.arrived(chunks[half].at[line], chunk_recv.at[half, line])

        for half in range(2):
            line = turn(lines[half], ahead)
            keys = ROW * sources[half].shape[1]
            vt_ref = turned_values[half]

            def load(first, last, half=half, line=line, keys=keys):
                return chunks[half][line, :, :, first:last].reshape(keys, last - first)

            values = load(v_first, v_first + vt_ref.shape[0])
            vt_ref[...] = values.T
            sizes = jnp.abs(values.astype(jnp.float32))
            for p in range(vt_ref.shape[0] // 128):
                part = sizes[:, p * 128:(p + 1) * 128].reshape(keys // 8, 8, 128)
                norm_ref[1] = jnp.maximum(norm_ref[1], jnp.max(part, axis=0))
            k_rows = load(0, pairs).astype(jnp.float32)
            sums = jnp.dot((k_rows * k_rows).astype(jnp.bfloat16), picks, preferred_element_type=jnp.float32)
            norm_ref[0] = jnp.maximum(norm_ref[0], jnp.max(sums.reshape(keys // 8, 8, 128), axis=0))

            def query_block(b, _, load=load, keys=keys, vt_ref=vt_ref):
                at = pl.multiple_of(b * lanes, lanes)
                for h in range(heads):
                    first = h // 2 * 128
                    scores = jnp.dot(load(first, first + 128), qz_ref[h, :, pl.ds(at, lanes)], preferred_element_type=jnp.float32)
                    weights = jnp.exp2(scores * (HEAD ** -0.5 * LOG2E))
                    stat_ref[b, h] += jnp.sum(weights.reshape(keys // 8, 8, lanes), axis=0)
                    values_t = vt_ref[v_base + h * HEAD:v_base + (h + 1) * HEAD]
                    acc_ref[b, h * HEAD:(h + 1) * HEAD] += jnp.dot(values_t, weights.astype(jnp.bfloat16), preferred_element_type=jnp.float32)
                return 0

            lax.fori_loop(0, acc_ref.shape[0], query_block, 0)
        return 0

    lax.fori_loop(0, SIDE, chunk, 0)
    total = part_ref.shape[0]
    for b in range(acc_ref.shape[0]):
        for h in range(heads):
            at = width + heads + h
            acc_ref[b, at:at + 1] = jnp.sum(stat_ref[b, h], axis=0, keepdims=True)
        last = min(total, (b + 1) * lanes)
        part_ref[b * lanes:last] = acc_ref[b].T[:last - b * lanes]
    guard_ref[0] = jnp.broadcast_to(jnp.max(norm_ref[0], axis=0, keepdims=True) * q_norm, (8, 128))
    guard_ref[1] = norm_ref[1]
    send.drain()
    for half in range(2):
        for i in range(2):
            passed_on(half, i).wait_send()


def mend_kernel(heads, guard_ref, part_in, kva_ref, kvb_ref, qz_ref, part_ref, a_ref, b_ref, q_ref, acc_ref, stat_ref, out_ref, sem):
    del part_in
    limit = (SAFE_SCORE * HEAD ** 0.5) ** 2 / 1.05
    safe = (jnp.max(guard_ref[0]) <= limit) & (jnp.max(guard_ref[1]) <= SAFE_VALUE)

    def fetch(src, dst):
        copy = pltpu.make_async_copy(src, dst, sem)
        copy.start()
        copy.wait()

    @pl.when(jnp.logical_not(safe))
    def again():
        width = heads * HEAD
        lanes = q_ref.shape[-1]
        total = out_ref.shape[0]

        def query_block(b, _):
            at = pl.multiple_of(b * lanes, lanes)
            fetch(qz_ref.at[:, :, pl.ds(at, lanes)], q_ref)
            acc_ref[...] = jnp.zeros_like(acc_ref)
            for h in range(heads):
                stat_ref[h] = jnp.full((8, lanes), -jnp.inf, jnp.float32)
                stat_ref[heads + h] = jnp.zeros((8, lanes), jnp.float32)
            for kv_ref, keys_ref in ((kva_ref, a_ref), (kvb_ref, b_ref)):

                def keys_block(i, _, kv_ref=kv_ref, keys_ref=keys_ref):
                    fetch(kv_ref.at[i // ROW, lax.rem(i, ROW)], keys_ref)
                    for h in range(heads):
                        first = h // 2 * 128
                        scores = jnp.dot(keys_ref[:, first:first + 128], q_ref[h], preferred_element_type=jnp.float32) * HEAD ** -0.5
                        old = stat_ref[h, 0:1]
                        new = jnp.maximum(old, jnp.max(scores, axis=0, keepdims=True))
                        weights = jnp.exp(scores - new)
                        fade = jnp.exp(old - new)
                        stat_ref[h, 0:1] = new
                        stat_ref[heads + h, 0:1] = stat_ref[heads + h, 0:1] * fade + jnp.sum(weights, axis=0, keepdims=True)
                        values = keys_ref[:, width + h * HEAD:width + (h + 1) * HEAD]
                        summed = lax.dot_general(values, weights.astype(jnp.bfloat16), (((0,), (0,)), ((), ())), preferred_element_type=jnp.float32)
                        acc_ref[h * HEAD:(h + 1) * HEAD] = acc_ref[h * HEAD:(h + 1) * HEAD] * fade + summed
                    return 0

                lax.fori_loop(0, SIDE * ROW, keys_block, 0)
            for h in range(heads):
                acc_ref[width + h:width + h + 1] = stat_ref[h, 0:1]
                acc_ref[width + heads + h:width + heads + h + 1] = stat_ref[heads + h, 0:1]
            out_ref[...] = acc_ref[...].T[:total]
            fetch(out_ref, part_ref.at[pl.ds(pl.multiple_of(b * total, 8), total)])
            return 0

        lax.fori_loop(0, part_ref.shape[0] // total, query_block, 0)


def attend(a, b, q, heads, collective_id):
    lanes = a.shape[-1]
    sets = q.shape[-1] // (heads * HEAD)
    count = ROW * q.shape[1] * sets
    block = 512 if count % 512 == 0 else 256
    blocks = -(-count // block)
    out_lanes = -(-(heads * HEAD + 2 * heads) // 128) * 128
    v_rows = lanes - heads * HEAD // 128 * 128
    vmem = pl.BlockSpec(memory_space=pltpu.VMEM)
    anywhere = pl.BlockSpec(memory_space=pl.ANY)
    part, kva, kvb, qz, guard = pl.pallas_call(
        functools.partial(attend_kernel, heads),
        out_shape=(
            jax.ShapeDtypeStruct((count, out_lanes), jnp.float32),
            jax.ShapeDtypeStruct((SIDE, ROW) + a.shape[1:], a.dtype),
            jax.ShapeDtypeStruct((SIDE, ROW) + b.shape[1:], b.dtype),
            jax.ShapeDtypeStruct((heads, 128, blocks * block), q.dtype),
            jax.ShapeDtypeStruct((2, 8, 128), jnp.float32),
        ),
        in_specs=[vmem] * 3,
        out_specs=(vmem,) * 5,
        scratch_shapes=[
            pltpu.VMEM((ROW,) + q.shape[1:], q.dtype),
            pltpu.VMEM((blocks, out_lanes, block), jnp.float32),
            pltpu.VMEM((blocks, heads, 8, block), jnp.float32),
            pltpu.VMEM((v_rows, ROW * a.shape[1]), jnp.bfloat16),
            pltpu.VMEM((v_rows, ROW * b.shape[1]), jnp.bfloat16),
            pltpu.VMEM((2, 8, 128), jnp.float32),
            pltpu.SemaphoreType.DMA((64,)),
            pltpu.SemaphoreType.DMA((2, ROW)),
            pltpu.SemaphoreType.DMA((2, SIDE)),
            pltpu.SemaphoreType.DMA((ROW,)),
        ],
        compiler_params=pltpu.CompilerParams(collective_id=collective_id, has_side_effects=True, vmem_limit_bytes=VMEM_LIMIT),
        name="attend",
    )(a, b, q)
    return pl.pallas_call(
        functools.partial(mend_kernel, heads),
        out_shape=jax.ShapeDtypeStruct(part.shape, part.dtype),
        in_specs=[vmem] + [anywhere] * 4,
        out_specs=anywhere,
        input_output_aliases={1: 0},
        scratch_shapes=[
            pltpu.VMEM(a.shape[1:], a.dtype),
            pltpu.VMEM(b.shape[1:], b.dtype),
            pltpu.VMEM((heads, 128, block), q.dtype),
            pltpu.VMEM((out_lanes, block), jnp.float32),
            pltpu.VMEM((2 * heads, 8, block), jnp.float32),
            pltpu.VMEM((min(count, block), out_lanes), jnp.float32),
            pltpu.SemaphoreType.DMA,
        ],
        compiler_params=pltpu.CompilerParams(vmem_limit_bytes=VMEM_LIMIT),
        name="mend",
    )(guard, part, kva, kvb, qz)


def combine_kernel(heads, part_ref, out_ref, got_ref, relay_ref, send_sem, recv_sem, relay_recv):
    t, z, y, x = position()
    sets, _, rows, _ = part_ref.shape
    near = [(0, 1 - t)] + [(d, c) for d in NEAR for c in range(2)]
    distant = [(2, c) for c in range(2)]
    if sets == 1:
        near += distant
    signal_all([(c, z, y, turn(x, d)) for d, c in near])
    send = Sender(send_sem, (t, z, y, x))
    mine = x * 2 + t
    if sets == 2:
        for _, c in distant:
            for s, d in enumerate(NEAR):
                send(part_ref.at[s, turn(x, 2) * 2 + c], relay_ref.at[s, t], relay_recv.at[s, t], (c, z, y, turn(x, d)))
    for d, c in near:
        for s in range(sets):
            send(part_ref.at[s, turn(x, d) * 2 + c], got_ref.at[s, mine], recv_sem.at[s, mine], (c, z, y, turn(x, d)))
    for s in range(sets):
        got_ref[s, mine] = part_ref[s, mine]
    if sets == 2:
        for c in range(2):
            for s, d in enumerate(NEAR):
                at = turn(x, SIDE - d) * 2 + c
                send.arrived(relay_ref.at[s, c], relay_recv.at[s, c])
                send(relay_ref.at[s, c], got_ref.at[s, at], recv_sem.at[s, at], (t, z, y, turn(x, d)))
    for d, c in near + (distant if sets == 2 else []):
        at = turn(x, SIDE - d) * 2 + c
        for s in range(sets):
            send.arrived(got_ref.at[s, at], recv_sem.at[s, at])
    width = heads * HEAD
    out_width = out_ref.shape[-1]
    head_of = lax.broadcasted_iota(jnp.int32, (rows, out_width), 1) // HEAD

    def spread(columns):
        full = jnp.broadcast_to(columns[:, 0:1], (rows, out_width))
        for h in range(1, heads):
            full = jnp.where(head_of == h, columns[:, h:h + 1], full)
        return full

    for c in range(2):
        for s in range(sets):
            blocks = [got_ref[s, 2 * i + c] for i in range(SIDE)]
            tops = [b[:, width:width + heads] for b in blocks]
            top = functools.reduce(jnp.maximum, tops)
            fades = [jnp.exp(m - top) for m in tops]
            total = sum(f * b[:, width + heads:width + 2 * heads] for f, b in zip(fades, blocks))
            merged = sum(spread(f / total) * b[:, :out_width] for f, b in zip(fades, blocks))
            out_ref[c, s] = jnp.where(head_of < heads, merged, 0.0).astype(jnp.bfloat16)
    send.drain()


def combine(parts, heads, collective_id):
    sets, _, rows, lanes = parts.shape
    out_width = -(-heads * HEAD // 128) * 128
    vmem = pl.BlockSpec(memory_space=pltpu.VMEM)
    out = pl.pallas_call(
        functools.partial(combine_kernel, heads),
        out_shape=jax.ShapeDtypeStruct((2, sets, rows, out_width), jnp.bfloat16),
        in_specs=[vmem],
        out_specs=vmem,
        scratch_shapes=[
            pltpu.VMEM(parts.shape, jnp.float32),
            pltpu.VMEM((2, 2, rows, lanes), jnp.float32),
            pltpu.SemaphoreType.DMA((24,)),
            pltpu.SemaphoreType.DMA((2, ROW)),
            pltpu.SemaphoreType.DMA((2, 2)),
        ],
        compiler_params=pltpu.CompilerParams(collective_id=collective_id, has_side_effects=True, vmem_limit_bytes=VMEM_LIMIT),
        name="combine",
    )(parts)
    return out.reshape(2, sets * rows, out_width)[:, :, :heads * HEAD]


def exchange_kernel(spread, src_ref, dst_ref, send_sem, recv_sem):
    t, me = lax.axis_index("time"), lax.axis_index("region")
    barrier = pltpu.get_barrier_semaphore()

    def signal(d, _):
        pl.semaphore_signal(barrier, inc=1, device_id={"time": t, "region": lax.rem(me + d, REGIONS)}, device_id_type=MESH)
        return 0

    lax.fori_loop(1, REGIONS, signal, 0)
    pl.semaphore_wait(barrier, REGIONS - 1)

    def start(d, _):
        peer = lax.rem(me + d, REGIONS)
        pltpu.make_async_remote_copy(
            src_ref=src_ref if spread else src_ref.at[peer],
            dst_ref=dst_ref.at[me],
            send_sem=send_sem,
            recv_sem=recv_sem,
            device_id={"time": t, "region": peer},
            device_id_type=MESH,
        ).start()
        return 0

    lax.fori_loop(1, REGIONS, start, 0)
    rest = dst_ref.at[pl.ds(0, REGIONS - 1)]
    everything = pltpu.make_async_remote_copy(
        src_ref=rest, dst_ref=rest, send_sem=send_sem, recv_sem=recv_sem, device_id={"time": t, "region": me}, device_id_type=MESH
    )
    everything.wait_recv()
    everything.wait_send()
    dst_ref[me] = src_ref[...] if spread else src_ref[me]


def exchange(rows, spread, collective_id):
    block = rows.shape if spread else rows.shape[1:]
    vmem = pl.BlockSpec(memory_space=pltpu.VMEM)
    return pl.pallas_call(
        functools.partial(exchange_kernel, spread),
        out_shape=jax.ShapeDtypeStruct((REGIONS,) + block, rows.dtype),
        in_specs=[vmem],
        out_specs=vmem,
        scratch_shapes=[pltpu.SemaphoreType.DMA, pltpu.SemaphoreType.DMA],
        compiler_params=pltpu.CompilerParams(collective_id=collective_id, has_side_effects=True),
        name="exchange",
    )(rows)


def layer_norm(hidden, ln_gain, ln_shift):
    hid_f32 = hidden.astype(jnp.float32)
    mean_val = jnp.mean(hid_f32, axis=-1, keepdims=True)
    centered = hid_f32 - mean_val
    variance = jnp.mean(centered * centered, axis=-1, keepdims=True)
    return centered * lax.rsqrt(variance + LN_EPS) * ln_gain + ln_shift


def run_block(hidden, vec_rows, w_qkv, w_o, w_one, w_two, collective_id):
    tokens, width = hidden.shape
    heads = w_qkv.shape[2] // 2
    half = heads * HEAD
    normed = layer_norm(hidden, vec_rows[0], vec_rows[1]).astype(jnp.bfloat16)
    w_rows = w_qkv.transpose(1, 2, 3, 0).reshape(3 * width, width)
    projected = lax.dot_general(normed, w_rows, (((1,), (1,)), ((), ())), preferred_element_type=jnp.float32)
    bias = jnp.concatenate([vec_rows[4], jnp.zeros_like(vec_rows[4]), vec_rows[5]])
    projected = (projected + bias).astype(jnp.bfloat16)

    def halves(part):
        return jnp.stack([projected[:, part * width + c * half:part * width + (c + 1) * half] for c in range(2)])

    q, k, v = halves(0), halves(1), halves(2)
    both = jnp.concatenate([k, v], axis=-1)
    split = tokens // 2 if tokens % 32 == 0 else 16
    sets = 2 if half % 128 else 1
    rows = tokens // sets
    q = jnp.concatenate([q[:, i * rows:(i + 1) * rows] for i in range(sets)], axis=-1)
    parts = attend(both[:, :split], both[:, split:], q, heads, collective_id)
    attended = combine(parts.reshape(sets, ROW, rows, -1), heads, collective_id + 1)
    w_o = w_o.reshape(2, half, width)
    mixed = sum(jnp.dot(attended[c], w_o[c], preferred_element_type=jnp.float32) for c in range(2))
    residual = (hidden.astype(jnp.float32) + mixed + vec_rows[6]).astype(jnp.bfloat16)
    normed_mlp = layer_norm(residual, vec_rows[2], vec_rows[3]).astype(jnp.bfloat16)
    mlp_hidden = jax.nn.gelu(jnp.dot(normed_mlp, w_one, preferred_element_type=jnp.float32) + vec_rows[8:12].reshape(-1), approximate=False).astype(jnp.bfloat16)
    return (residual.astype(jnp.float32) + jnp.dot(mlp_hidden, w_two, preferred_element_type=jnp.float32) + vec_rows[7]).astype(jnp.bfloat16)


def one_hot_rows(selector, rows):
    return jnp.dot(selector.astype(jnp.bfloat16), rows, preferred_element_type=jnp.float32).astype(jnp.bfloat16)


def solution(mesh):
    def local_step(patches, enc_pos, vis_mask, dec_pos, w_embed, b_embed, enc_vec, enc_wqkv, enc_wo, enc_w1, enc_w2, enc_final, w_dec_in, mask_token, dec_vec, dec_wqkv, dec_wo, dec_w1, dec_w2, dec_final, w_out):
        tokens = patches.shape[0]
        per_dev = tokens // 8
        me = lax.axis_index("region")
        own_count = jnp.sum(vis_mask)
        counts = exchange(jnp.full((8, 128), own_count, jnp.int32), True, 1)[:, 0, 0]
        embedded = (jnp.dot(patches, w_embed, preferred_element_type=jnp.float32) + b_embed + enc_pos.astype(jnp.float32)).astype(jnp.bfloat16)

        region_ids = jnp.arange(REGIONS, dtype=jnp.int32)
        starts = jnp.sum(jnp.where(region_ids[None, :] < region_ids[:, None], counts[None, :], 0), axis=1)
        start = jnp.sum(jnp.where(region_ids < me, counts, 0))
        token_ids = jnp.arange(tokens, dtype=jnp.int32)
        local_rank = jnp.sum(jnp.where(token_ids[None, :] < token_ids[:, None], vis_mask[None, :], 0), axis=1)
        send_row = jnp.where(vis_mask == 1, lax.rem(start + local_rank, REGIONS) * 2 + local_rank // REGIONS, -1)
        row_ids = jnp.arange(2 * REGIONS, dtype=jnp.int32)
        deal = row_ids[:, None] == send_row[None, :]
        source_starts, source_counts = jnp.repeat(starts, 2), jnp.repeat(counts, 2)
        rank = lax.rem(me - lax.rem(source_starts, REGIONS) + REGIONS, REGIONS) + REGIONS * lax.rem(row_ids, 2)
        place = jnp.where(rank < source_counts, (source_starts + rank) // REGIONS, -1)
        pack = jnp.arange(per_dev, dtype=jnp.int32)[:, None] == place[None, :]

        sent = one_hot_rows(deal, embedded).reshape(REGIONS, 2, -1)
        hidden = one_hot_rows(pack, exchange(sent, False, 2).reshape(2 * REGIONS, -1))
        for layer in range(enc_vec.shape[0]):
            hidden = run_block(hidden, enc_vec[layer], enc_wqkv[layer], enc_wo[layer], enc_w1[layer], enc_w2[layer], 4 + 2 * layer)
        latent = jnp.dot(layer_norm(hidden, enc_final[0], enc_final[1]).astype(jnp.bfloat16), w_dec_in, preferred_element_type=jnp.float32).astype(jnp.bfloat16)
        back = one_hot_rows(pack.T, latent).reshape(REGIONS, 2, -1)
        returned = exchange(back, False, 3).reshape(2 * REGIONS, -1)
        placed = jnp.dot(deal.T.astype(jnp.bfloat16), returned, preferred_element_type=jnp.float32)
        hidden = (jnp.where(vis_mask[:, None] == 1, placed, mask_token.astype(jnp.float32)) + dec_pos.astype(jnp.float32)).astype(jnp.bfloat16)
        for layer in range(dec_vec.shape[0]):
            hidden = run_block(hidden, dec_vec[layer], dec_wqkv[layer], dec_wo[layer], dec_w1[layer], dec_w2[layer], 8 + 2 * layer)
        return jnp.dot(layer_norm(hidden, dec_final[0], dec_final[1]).astype(jnp.bfloat16), w_out, preferred_element_type=jnp.float32)

    token_rows = P(TOKEN_AXES, None)
    token_flags = P(TOKEN_AXES)
    replicated = P()
    in_specs = (token_rows, token_rows, token_flags, token_rows) + (replicated,) * 17
    return jax.shard_map(local_step, mesh=mesh, in_specs=in_specs, out_specs=token_rows, check_vma=False)
```

```python
import functools
import jax
import jax.numpy as jnp
from jax import lax
from jax.experimental import pallas as pl
from jax.experimental.pallas import tpu as pltpu
from jax.sharding import PartitionSpec as P

LN_EPS = 1e-6
TOKEN_AXES = ("batch", "time", "region")
SIDE = 4
REGIONS = SIDE ** 3
ROW = SIDE * 2
HEAD = 64
MESH = pl.DeviceIdType.MESH
NEAR = (1, SIDE - 1)
VMEM_LIMIT = 60 * 1024 * 1024
LOG2E = 1.4426950408889634
SAFE_SCORE = 60.0
SAFE_VALUE = 1e7


def position():
    t, r = lax.axis_index("time"), lax.axis_index("region")
    return t, r // 16, lax.rem(r // 4, 4), lax.rem(r, 4)


def device(t, z, y, x):
    return {"time": t, "region": z * 16 + y * 4 + x}


def turn(a, d):
    return lax.rem(a + d, SIDE)


def signal_all(peers):
    barrier = pltpu.get_barrier_semaphore()
    for peer in peers:
        pl.semaphore_signal(barrier, inc=1, device_id=device(*peer), device_id_type=MESH)
    pl.semaphore_wait(barrier, len(peers))


class Sender:
    def __init__(self, sems, place):
        self.sems, self.place, self.used, self.started = sems, place, 0, []

    def __call__(self, src, dst, recv_sem, peer):
        copy = remote_copy(src, dst, self.sems.at[self.used], recv_sem, peer)
        copy.start()
        self.used += 1
        self.started.append(copy)

    def arrived(self, ref, recv_sem):
        remote_copy(ref, ref, self.sems.at[0], recv_sem, self.place).wait_recv()

    def drain(self):
        for copy in self.started:
            copy.wait_send()


def remote_copy(src, dst, send_sem, recv_sem, peer):
    return pltpu.make_async_remote_copy(
        src_ref=src, dst_ref=dst, send_sem=send_sem, recv_sem=recv_sem, device_id=device(*peer), device_id_type=MESH
    )


def attend_kernel(heads, relay, ahead_of, a_ref, b_ref, q_ref, part_ref, kva_ref, kvb_ref, qz_ref, guard_ref, qall_ref, stat_ref, vta_ref, vtb_ref, norm_ref, send_sem, one_recv, chunk_recv, q_recv):
    t, z, y, x = position()
    other = 1 - t
    ring = NEAR if relay else NEAR + (2,)
    near = [(0, other)] + [(d, c) for d in ring for c in range(2)]
    peers = [(other, z, y, x)]
    for d, c in near[1:]:
        peers += [(c, turn(z, d), y, x), (c, z, turn(y, d), x), (c, z, y, turn(x, d))]
    signal_all(peers)

    sources, chunks, turned_values = (a_ref, b_ref), (kva_ref, kvb_ref), (vta_ref, vtb_ref)
    lines, places = (z, y), (y, z)
    send = Sender(send_sem, (t, z, y, x))

    def along(half, first, d, c):
        return (c, z, turn(y, d), x) if (half == 0) == first else (c, turn(z, d), y, x)

    def block(half, place, c, size=1):
        at = chunks[half].at[lines[half]]
        return at.at[place * 2 + c] if size == 1 else at.at[pl.ds(place * 2, size)]

    def one(half, place, c):
        return one_recv.at[half, place * 2 + c]

    def onward(half, ref):
        for d in ring:
            send(ref, ref, chunk_recv.at[half, lines[half]], along(half, False, d, t))

    row = x * 2 + t
    for d, c in near:
        send(q_ref.at[c], qall_ref.at[row], q_recv.at[row], (c, z, y, turn(x, d)))
        for half in range(2):
            send(sources[half].at[c], block(half, places[half], t), one(half, places[half], t), along(half, True, d, c))
    for half in range(2):
        for d in ring:
            send(sources[half].at[t], block(half, places[half], t), chunk_recv.at[half, lines[half]], along(half, False, d, t))
        chunks[half][lines[half], places[half] * 2 + t] = sources[half][t]
    qall_ref[row] = q_ref[t]

    part_ref[...] = jnp.zeros_like(part_ref)
    stat_ref[...] = jnp.zeros_like(stat_ref)
    norm_ref[...] = jnp.zeros_like(norm_ref)
    qz_ref[...] = jnp.zeros_like(qz_ref)

    def q_arrived(d, c):
        at = turn(x, SIDE - d) * 2 + c
        send.arrived(qall_ref.at[at], q_recv.at[at])
        return at

    for d, relayed in zip(NEAR, range(2)):
        for c in range(2):
            at = q_arrived(d, c)
            if relay and c == relayed:
                send(qall_ref.at[at], qall_ref.at[at], q_recv.at[at], (t, z, y, turn(x, d)))
        for half in range(2):
            place = turn(places[half], SIDE - d)
            for c in range(2):
                send.arrived(block(half, place, c), one(half, place, c))
            if relay:
                ref = block(half, place, relayed)
                send(ref, ref, one(half, place, relayed), along(half, True, d, t))
            onward(half, block(half, place, 0, 2))
    q_arrived(0, other)
    for half in range(2):
        ref = block(half, places[half], other)
        send.arrived(ref, one(half, places[half], other))
        onward(half, ref)
    for half in range(2):
        place = turn(places[half], 2)
        for c in range(2):
            send.arrived(block(half, place, c), one(half, place, c))
        onward(half, block(half, place, 0, 2))
    for c in range(2):
        q_arrived(2, c)

    rows = q_ref.shape[1]
    count = ROW * rows
    chip_lanes = qz_ref.shape[-1] // SIDE
    lane = lax.broadcasted_iota(jnp.int32, (1, 128), 1)
    q_norm = jnp.zeros((1, 128), jnp.float32)
    for p in range(q_ref.shape[-1] // 128):
        flat = qall_ref[:, :, p * 128:(p + 1) * 128].reshape(count, 128)
        if count % 128:
            flat = jnp.concatenate([flat, jnp.zeros((-count % 128, 128), flat.dtype)], axis=0)
        turned = flat.T
        for i in range(2):
            group, h = divmod(2 * p + i, heads)
            own = turned[i * HEAD:(i + 1) * HEAD]
            at = h % 2 * HEAD
            for chip in range(SIDE):
                first = chip * chip_lanes + group * 2 * rows
                qz_ref[h, at:at + HEAD, first:first + 2 * rows] = own[:, chip * 2 * rows:(chip + 1) * 2 * rows]
            size = jnp.sum(own.astype(jnp.float32) ** 2, axis=0, keepdims=True)
            q_norm = jnp.where(lane == h, jnp.maximum(q_norm, jnp.max(size, axis=1, keepdims=True)), q_norm)

    width = heads * HEAD
    lanes = 512
    v_first = width // 128 * 128
    v_base = width - v_first
    pairs = -(-heads // 2) * 128
    picks = lax.broadcasted_iota(jnp.int32, (pairs, 128), 0) // HEAD == lax.broadcasted_iota(jnp.int32, (pairs, 128), 1)
    picks = (picks & (lane < heads)).astype(jnp.bfloat16)
    far = [len(send.started) + i for i in range(4)]

    def passed_on(half, i):
        d = NEAR[i]
        line = turn(lines[half], SIDE - d)
        ref = chunks[half].at[line, pl.ds(i * SIDE, SIDE)]
        return remote_copy(ref, ref, send_sem.at[far[2 * half + i]], chunk_recv.at[half, line], along(half, False, d, t))

    def work(half, line):
        vt_ref = turned_values[half]
        keys = vt_ref.shape[-1]

        def load(first, last):
            return chunks[half][line, :, :, first:last].reshape(keys, last - first)

        values = load(v_first, v_first + vt_ref.shape[0])
        vt_ref[...] = values.T
        sizes = jnp.abs(values.astype(jnp.float32))
        for p in range(vt_ref.shape[0] // 128):
            part = sizes[:, p * 128:(p + 1) * 128].reshape(keys // 8, 8, 128)
            norm_ref[1] = jnp.maximum(norm_ref[1], jnp.max(part, axis=0))
        k_rows = load(0, pairs).astype(jnp.float32)
        sums = jnp.dot((k_rows * k_rows).astype(jnp.bfloat16), picks, preferred_element_type=jnp.float32)
        norm_ref[0] = jnp.maximum(norm_ref[0], jnp.max(sums.reshape(keys // 8, 8, 128), axis=0))
        pieces = 2 if ahead_of else 1
        size = keys // pieces
        tasks = [(h, i) for h in range(heads) for i in range(pieces)]

        def query_block(b, _):
            at = pl.ds(pl.multiple_of(b * lanes, lanes), lanes)

            def scores_of(h, i):
                first = h // 2 * 128
                k_rows = load(first, first + 128)[i * size:(i + 1) * size]
                return jnp.dot(k_rows, qz_ref[h, :, at], preferred_element_type=jnp.float32)

            ready = [scores_of(*task) for task in tasks[:ahead_of]]
            for n, (h, i) in enumerate(tasks):
                if n + ahead_of < len(tasks):
                    ready.append(scores_of(*tasks[n + ahead_of]))
                weights = jnp.exp2(ready.pop(0) * (HEAD ** -0.5 * LOG2E))
                total = jnp.sum(weights.reshape(size // 8, 8, lanes), axis=0)
                values_t = vt_ref[v_base + h * HEAD:v_base + (h + 1) * HEAD, i * size:(i + 1) * size]
                summed = jnp.dot(values_t, weights.astype(jnp.bfloat16), preferred_element_type=jnp.float32)
                totals, sums = (total, summed) if i == 0 else (totals + total, sums + summed)
                if i == pieces - 1:
                    stat_ref[h, :, at] += totals
                    part_ref[h * HEAD:(h + 1) * HEAD, at] += sums
            return 0

        lax.fori_loop(0, part_ref.shape[-1] // lanes, query_block, 0)

    def wait_for(half, d):
        line = turn(lines[half], SIDE - d)
        send.arrived(chunks[half].at[line], chunk_recv.at[half, line])

    if relay:

        def chunk(j, _):
            ahead = j + j // 2 - 2 * (j // 3)

            @pl.when(j == 1)
            def near_chunks():
                for i in range(2):
                    for half in range(2):
                        wait_for(half, NEAR[i])
                        passed_on(half, i).start()

            @pl.when(j == 3)
            def far_chunks():
                for half in range(2):
                    wait_for(half, 2)

            for half in range(2):
                work(half, turn(lines[half], ahead))
            return 0

        lax.fori_loop(0, SIDE, chunk, 0)
    else:
        for half in range(2):
            for d in ring:
                wait_for(half, d)
            work(half, slice(None))
    for h in range(heads):
        at = width + heads + h
        part_ref[at:at + 1] = jnp.sum(stat_ref[h], axis=0, keepdims=True)
    guard_ref[0] = jnp.broadcast_to(jnp.max(norm_ref[0], axis=0, keepdims=True) * q_norm, (8, 128))
    guard_ref[1] = norm_ref[1]
    send.drain()
    if relay:
        for half in range(2):
            for i in range(2):
                passed_on(half, i).wait_send()


def mend_kernel(heads, guard_ref, part_in, kva_ref, kvb_ref, qz_ref, part_ref, a_ref, b_ref, q_ref, acc_ref, stat_ref, sem):
    del part_in
    limit = (SAFE_SCORE * HEAD ** 0.5) ** 2 / 1.05
    safe = (jnp.max(guard_ref[0]) <= limit) & (jnp.max(guard_ref[1]) <= SAFE_VALUE)

    def fetch(src, dst):
        copy = pltpu.make_async_copy(src, dst, sem)
        copy.start()
        copy.wait()

    @pl.when(jnp.logical_not(safe))
    def again():
        width = heads * HEAD
        lanes = q_ref.shape[-1]

        def query_block(b, _):
            at = pl.multiple_of(b * lanes, lanes)
            fetch(qz_ref.at[:, :, pl.ds(at, lanes)], q_ref)
            acc_ref[...] = jnp.zeros_like(acc_ref)
            for h in range(heads):
                stat_ref[h] = jnp.full((8, lanes), -jnp.inf, jnp.float32)
                stat_ref[heads + h] = jnp.zeros((8, lanes), jnp.float32)
            for kv_ref, keys_ref in ((kva_ref, a_ref), (kvb_ref, b_ref)):

                def keys_block(i, _, kv_ref=kv_ref, keys_ref=keys_ref):
                    fetch(kv_ref.at[i // ROW, lax.rem(i, ROW)], keys_ref)
                    for h in range(heads):
                        first = h // 2 * 128
                        scores = jnp.dot(keys_ref[:, first:first + 128], q_ref[h], preferred_element_type=jnp.float32) * HEAD ** -0.5
                        old = stat_ref[h, 0:1]
                        new = jnp.maximum(old, jnp.max(scores, axis=0, keepdims=True))
                        weights = jnp.exp(scores - new)
                        fade = jnp.exp(old - new)
                        stat_ref[h, 0:1] = new
                        stat_ref[heads + h, 0:1] = stat_ref[heads + h, 0:1] * fade + jnp.sum(weights, axis=0, keepdims=True)
                        values = keys_ref[:, width + h * HEAD:width + (h + 1) * HEAD]
                        summed = lax.dot_general(values, weights.astype(jnp.bfloat16), (((0,), (0,)), ((), ())), preferred_element_type=jnp.float32)
                        acc_ref[h * HEAD:(h + 1) * HEAD] = acc_ref[h * HEAD:(h + 1) * HEAD] * fade + summed
                    return 0

                lax.fori_loop(0, SIDE * ROW, keys_block, 0)
            for h in range(heads):
                acc_ref[width + h:width + h + 1] = stat_ref[h, 0:1]
                acc_ref[width + heads + h:width + heads + h + 1] = stat_ref[heads + h, 0:1]
            fetch(acc_ref, part_ref.at[:, pl.ds(at, lanes)])
            return 0

        lax.fori_loop(0, part_ref.shape[-1] // lanes, query_block, 0)


def attend(a, b, q, heads, ahead_of, collective_id):
    lanes = a.shape[-1]
    sets = q.shape[-1] // (heads * HEAD)
    relay = sets == 2
    count = SIDE * (-(-2 * q.shape[1] * sets // 128) * 128)
    block = 512
    out_rows = -(-(heads * HEAD + 2 * heads) // 8) * 8
    keys = ROW if relay else ROW * SIDE
    v_rows = lanes - heads * HEAD // 128 * 128
    vmem = pl.BlockSpec(memory_space=pltpu.VMEM)
    anywhere = pl.BlockSpec(memory_space=pl.ANY)
    part, kva, kvb, qz, guard = pl.pallas_call(
        functools.partial(attend_kernel, heads, relay, ahead_of),
        out_shape=(
            jax.ShapeDtypeStruct((out_rows, count), jnp.float32),
            jax.ShapeDtypeStruct((SIDE, ROW) + a.shape[1:], a.dtype),
            jax.ShapeDtypeStruct((SIDE, ROW) + b.shape[1:], b.dtype),
            jax.ShapeDtypeStruct((heads, 128, count), q.dtype),
            jax.ShapeDtypeStruct((2, 8, 128), jnp.float32),
        ),
        in_specs=[vmem] * 3,
        out_specs=(vmem,) * 5,
        scratch_shapes=[
            pltpu.VMEM((ROW,) + q.shape[1:], q.dtype),
            pltpu.VMEM((heads, 8, count), jnp.float32),
            pltpu.VMEM((v_rows, keys * a.shape[1]), jnp.bfloat16),
            pltpu.VMEM((v_rows, keys * b.shape[1]), jnp.bfloat16),
            pltpu.VMEM((2, 8, 128), jnp.float32),
            pltpu.SemaphoreType.DMA((64,)),
            pltpu.SemaphoreType.DMA((2, ROW)),
            pltpu.SemaphoreType.DMA((2, SIDE)),
            pltpu.SemaphoreType.DMA((ROW,)),
        ],
        compiler_params=pltpu.CompilerParams(collective_id=collective_id, has_side_effects=True, vmem_limit_bytes=VMEM_LIMIT),
        name="attend",
    )(a, b, q)
    return pl.pallas_call(
        functools.partial(mend_kernel, heads),
        out_shape=jax.ShapeDtypeStruct(part.shape, part.dtype),
        in_specs=[vmem] + [anywhere] * 4,
        out_specs=anywhere,
        input_output_aliases={1: 0},
        scratch_shapes=[
            pltpu.VMEM(a.shape[1:], a.dtype),
            pltpu.VMEM(b.shape[1:], b.dtype),
            pltpu.VMEM((heads, 128, block), q.dtype),
            pltpu.VMEM((out_rows, block), jnp.float32),
            pltpu.VMEM((2 * heads, 8, block), jnp.float32),
            pltpu.SemaphoreType.DMA,
        ],
        compiler_params=pltpu.CompilerParams(vmem_limit_bytes=VMEM_LIMIT),
        name="mend",
    )(guard, part, kva, kvb, qz)


def combine_kernel(heads, part_ref, out_ref, got_ref, send_sem, recv_sem):
    t, z, y, x = position()
    partner = (1 - t, z, y, x)
    ring = NEAR + (2,)
    signal_all([partner] + [(t, z, y, turn(x, d)) for d in ring])
    send = Sender(send_sem, (t, z, y, x))
    lanes = got_ref.shape[-1]

    def chip(i):
        return part_ref.at[:, pl.ds(pl.multiple_of(i * lanes, 128), lanes)]

    for d in (2,) + NEAR:
        to = turn(x, d)
        send(chip(to), got_ref.at[x], recv_sem.at[x], (t, z, y, to))
    got_ref[x] = chip(x)[...]
    for d in ring:
        at = turn(x, d)
        send.arrived(got_ref.at[at], recv_sem.at[at])
    width = heads * HEAD
    for h in range(heads):
        tops = [got_ref[i, width + h:width + h + 1] for i in range(SIDE)]
        top = functools.reduce(jnp.maximum, tops)
        fades = [jnp.exp(m - top) for m in tops]
        total = sum(f * got_ref[i, width + heads + h:width + heads + h + 1] for i, f in enumerate(fades))
        merged = sum(f / total * got_ref[i, h * HEAD:(h + 1) * HEAD] for i, f in enumerate(fades))
        out_ref[t, h * HEAD:(h + 1) * HEAD] = merged.astype(jnp.bfloat16)
    send(out_ref.at[t], out_ref.at[t], recv_sem.at[SIDE], partner)
    send.arrived(out_ref.at[1 - t], recv_sem.at[SIDE])
    send.drain()


def combine(parts, heads, collective_id):
    rows, queries = parts.shape
    vmem = pl.BlockSpec(memory_space=pltpu.VMEM)
    return pl.pallas_call(
        functools.partial(combine_kernel, heads),
        out_shape=jax.ShapeDtypeStruct((2, heads * HEAD, queries // SIDE), jnp.bfloat16),
        in_specs=[vmem],
        out_specs=vmem,
        scratch_shapes=[
            pltpu.VMEM((SIDE, rows, queries // SIDE), jnp.float32),
            pltpu.SemaphoreType.DMA((SIDE,)),
            pltpu.SemaphoreType.DMA((SIDE + 1,)),
        ],
        compiler_params=pltpu.CompilerParams(collective_id=collective_id, has_side_effects=True, vmem_limit_bytes=VMEM_LIMIT),
        name="combine",
    )(parts)


def exchange_kernel(spread, src_ref, dst_ref, send_sem, recv_sem):
    t, me = lax.axis_index("time"), lax.axis_index("region")
    barrier = pltpu.get_barrier_semaphore()

    def signal(d, _):
        pl.semaphore_signal(barrier, inc=1, device_id={"time": t, "region": lax.rem(me + d, REGIONS)}, device_id_type=MESH)
        return 0

    lax.fori_loop(1, REGIONS, signal, 0)
    pl.semaphore_wait(barrier, REGIONS - 1)

    def start(d, _):
        peer = lax.rem(me + d, REGIONS)
        pltpu.make_async_remote_copy(
            src_ref=src_ref if spread else src_ref.at[peer],
            dst_ref=dst_ref.at[me],
            send_sem=send_sem,
            recv_sem=recv_sem,
            device_id={"time": t, "region": peer},
            device_id_type=MESH,
        ).start()
        return 0

    lax.fori_loop(1, REGIONS, start, 0)
    rest = dst_ref.at[pl.ds(0, REGIONS - 1)]
    everything = pltpu.make_async_remote_copy(
        src_ref=rest, dst_ref=rest, send_sem=send_sem, recv_sem=recv_sem, device_id={"time": t, "region": me}, device_id_type=MESH
    )
    everything.wait_recv()
    everything.wait_send()
    dst_ref[me] = src_ref[...] if spread else src_ref[me]


def exchange(rows, spread, collective_id):
    block = rows.shape if spread else rows.shape[1:]
    vmem = pl.BlockSpec(memory_space=pltpu.VMEM)
    return pl.pallas_call(
        functools.partial(exchange_kernel, spread),
        out_shape=jax.ShapeDtypeStruct((REGIONS,) + block, rows.dtype),
        in_specs=[vmem],
        out_specs=vmem,
        scratch_shapes=[pltpu.SemaphoreType.DMA, pltpu.SemaphoreType.DMA],
        compiler_params=pltpu.CompilerParams(collective_id=collective_id, has_side_effects=True),
        name="exchange",
    )(rows)


def layer_norm(hidden, ln_gain, ln_shift):
    hid_f32 = hidden.astype(jnp.float32)
    mean_val = jnp.mean(hid_f32, axis=-1, keepdims=True)
    centered = hid_f32 - mean_val
    variance = jnp.mean(centered * centered, axis=-1, keepdims=True)
    return centered * lax.rsqrt(variance + LN_EPS) * ln_gain + ln_shift


def run_block(hidden, vec_rows, w_qkv, w_o, w_one, w_two, ahead_of, collective_id):
    tokens, width = hidden.shape
    heads = w_qkv.shape[2] // 2
    half = heads * HEAD
    normed = layer_norm(hidden, vec_rows[0], vec_rows[1]).astype(jnp.bfloat16)
    w_rows = w_qkv.transpose(1, 2, 3, 0).reshape(3 * width, width)
    projected = lax.dot_general(normed, w_rows, (((1,), (1,)), ((), ())), preferred_element_type=jnp.float32)
    bias = jnp.concatenate([vec_rows[4], jnp.zeros_like(vec_rows[4]), vec_rows[5]])
    projected = (projected + bias).astype(jnp.bfloat16)

    def halves(part):
        return jnp.stack([projected[:, part * width + c * half:part * width + (c + 1) * half] for c in range(2)])

    q, k, v = halves(0), halves(1), halves(2)
    both = jnp.concatenate([k, v], axis=-1)
    split = tokens // 2 if tokens % 32 == 0 else 16
    sets = 2 if half % 128 else 1
    rows = tokens // sets
    q = jnp.concatenate([q[:, i * rows:(i + 1) * rows] for i in range(sets)], axis=-1)
    parts = attend(both[:, :split], both[:, split:], q, heads, ahead_of, collective_id)
    attended = combine(parts, heads, collective_id + 1)
    mixed = lax.dot_general(attended.reshape(width, -1), w_o.reshape(width, width), (((0,), (0,)), ((), ())), preferred_element_type=jnp.float32)
    mixed = mixed[:2 * tokens].reshape(sets, 2, rows, width)
    mixed = lax.dynamic_index_in_dim(mixed, lax.axis_index("time"), axis=1, keepdims=False).reshape(tokens, width)
    residual = (hidden.astype(jnp.float32) + mixed + vec_rows[6]).astype(jnp.bfloat16)
    normed_mlp = layer_norm(residual, vec_rows[2], vec_rows[3]).astype(jnp.bfloat16)
    mlp_hidden = jax.nn.gelu(jnp.dot(normed_mlp, w_one, preferred_element_type=jnp.float32) + vec_rows[8:12].reshape(-1), approximate=False).astype(jnp.bfloat16)
    return (residual.astype(jnp.float32) + jnp.dot(mlp_hidden, w_two, preferred_element_type=jnp.float32) + vec_rows[7]).astype(jnp.bfloat16)


def one_hot_rows(selector, rows):
    return jnp.dot(selector.astype(jnp.bfloat16), rows, preferred_element_type=jnp.float32).astype(jnp.bfloat16)


def solution(mesh):
    def local_step(patches, enc_pos, vis_mask, dec_pos, w_embed, b_embed, enc_vec, enc_wqkv, enc_wo, enc_w1, enc_w2, enc_final, w_dec_in, mask_token, dec_vec, dec_wqkv, dec_wo, dec_w1, dec_w2, dec_final, w_out):
        tokens = patches.shape[0]
        per_dev = tokens // 8
        me = lax.axis_index("region")
        own_count = jnp.sum(vis_mask)
        counts = exchange(jnp.full((8, 128), own_count, jnp.int32), True, 1)[:, 0, 0]
        embedded = (jnp.dot(patches, w_embed, preferred_element_type=jnp.float32) + b_embed + enc_pos.astype(jnp.float32)).astype(jnp.bfloat16)

        region_ids = jnp.arange(REGIONS, dtype=jnp.int32)
        starts = jnp.sum(jnp.where(region_ids[None, :] < region_ids[:, None], counts[None, :], 0), axis=1)
        start = jnp.sum(jnp.where(region_ids < me, counts, 0))
        token_ids = jnp.arange(tokens, dtype=jnp.int32)
        local_rank = jnp.sum(jnp.where(token_ids[None, :] < token_ids[:, None], vis_mask[None, :], 0), axis=1)
        send_row = jnp.where(vis_mask == 1, lax.rem(start + local_rank, REGIONS) * 2 + local_rank // REGIONS, -1)
        row_ids = jnp.arange(2 * REGIONS, dtype=jnp.int32)
        deal = row_ids[:, None] == send_row[None, :]
        source_starts, source_counts = jnp.repeat(starts, 2), jnp.repeat(counts, 2)
        rank = lax.rem(me - lax.rem(source_starts, REGIONS) + REGIONS, REGIONS) + REGIONS * lax.rem(row_ids, 2)
        place = jnp.where(rank < source_counts, (source_starts + rank) // REGIONS, -1)
        pack = jnp.arange(per_dev, dtype=jnp.int32)[:, None] == place[None, :]

        sent = one_hot_rows(deal, embedded).reshape(REGIONS, 2, -1)
        hidden = one_hot_rows(pack, exchange(sent, False, 2).reshape(2 * REGIONS, -1))
        for layer in range(enc_vec.shape[0]):
            hidden = run_block(hidden, enc_vec[layer], enc_wqkv[layer], enc_wo[layer], enc_w1[layer], enc_w2[layer], 0, 4 + 2 * layer)
        latent = jnp.dot(layer_norm(hidden, enc_final[0], enc_final[1]).astype(jnp.bfloat16), w_dec_in, preferred_element_type=jnp.float32).astype(jnp.bfloat16)
        back = one_hot_rows(pack.T, latent).reshape(REGIONS, 2, -1)
        returned = exchange(back, False, 3).reshape(2 * REGIONS, -1)
        placed = jnp.dot(deal.T.astype(jnp.bfloat16), returned, preferred_element_type=jnp.float32)
        hidden = (jnp.where(vis_mask[:, None] == 1, placed, mask_token.astype(jnp.float32)) + dec_pos.astype(jnp.float32)).astype(jnp.bfloat16)
        for layer in range(dec_vec.shape[0]):
            hidden = run_block(hidden, dec_vec[layer], dec_wqkv[layer], dec_wo[layer], dec_w1[layer], dec_w2[layer], layer, 8 + 2 * layer)
        return jnp.dot(layer_norm(hidden, dec_final[0], dec_final[1]).astype(jnp.bfloat16), w_out, preferred_element_type=jnp.float32)

    token_rows = P(TOKEN_AXES, None)
    token_flags = P(TOKEN_AXES)
    replicated = P()
    in_specs = (token_rows, token_rows, token_flags, token_rows) + (replicated,) * 17
    return jax.shard_map(local_step, mesh=mesh, in_specs=in_specs, out_specs=token_rows, check_vma=False)
```

```python
import functools
import jax
import jax.numpy as jnp
from jax import lax
from jax.experimental import pallas as pl
from jax.experimental.pallas import tpu as pltpu
from jax.sharding import PartitionSpec as P

LN_EPS = 1e-6
TOKEN_AXES = ("batch", "time", "region")
SIDE = 4
REGIONS = SIDE ** 3
ROW = SIDE * 2
GROUP = 3
HEAD = 64
MESH = pl.DeviceIdType.MESH
NEAR = (1, SIDE - 1)
VMEM_LIMIT = 60 * 1024 * 1024
LOG2E = 1.4426950408889634
SAFE_SCORE = 60.0
SAFE_VALUE = 1e7


def position():
    t, r = lax.axis_index("time"), lax.axis_index("region")
    return t, r // 16, lax.rem(r // 4, 4), lax.rem(r, 4)


def device(t, z, y, x):
    return {"time": t, "region": z * 16 + y * 4 + x}


def turn(a, d):
    return lax.rem(a + d, SIDE)


def signal_all(peers):
    barrier = pltpu.get_barrier_semaphore()
    for peer in peers:
        pl.semaphore_signal(barrier, inc=1, device_id=device(*peer), device_id_type=MESH)
    pl.semaphore_wait(barrier, len(peers))


class Sender:
    def __init__(self, sems, place):
        self.sems, self.place, self.used, self.started = sems, place, 0, []

    def __call__(self, src, dst, recv_sem, peer):
        copy = remote_copy(src, dst, self.sems.at[self.used], recv_sem, peer)
        copy.start()
        self.used += 1
        self.started.append(copy)

    def arrived(self, ref, recv_sem):
        remote_copy(ref, ref, self.sems.at[0], recv_sem, self.place).wait_recv()

    def drain(self):
        for copy in self.started:
            copy.wait_send()


def remote_copy(src, dst, send_sem, recv_sem, peer):
    return pltpu.make_async_remote_copy(
        src_ref=src, dst_ref=dst, send_sem=send_sem, recv_sem=recv_sem, device_id=device(*peer), device_id_type=MESH
    )


def folded(rows):
    if len(rows) == GROUP:
        return rows
    low = lax.broadcasted_iota(jnp.int32, rows[0].shape, 1) % 128 < HEAD
    return [jnp.where(low, a, pltpu.roll(b, HEAD, axis=1)) for a, b in zip(rows, rows[GROUP:])]


def attend_kernel(heads, relay, ahead_of, a_ref, b_ref, q_ref, part_ref, kva_ref, kvb_ref, qz_ref, guard_ref, qall_ref, acc_ref, stat_ref, vta_ref, vtb_ref, norm_ref, send_sem, one_recv, chunk_recv, q_recv):
    t, z, y, x = position()
    other = 1 - t
    ring = NEAR if relay else NEAR + (2,)
    near = [(0, other)] + [(d, c) for d in ring for c in range(2)]
    peers = [(other, z, y, x)]
    for d, c in near[1:]:
        peers += [(c, turn(z, d), y, x), (c, z, turn(y, d), x), (c, z, y, turn(x, d))]
    signal_all(peers)

    sources, chunks, turned_values = (a_ref, b_ref), (kva_ref, kvb_ref), (vta_ref, vtb_ref)
    lines, places = (z, y), (y, z)
    send = Sender(send_sem, (t, z, y, x))

    def along(half, first, d, c):
        return (c, z, turn(y, d), x) if (half == 0) == first else (c, turn(z, d), y, x)

    def block(half, place, c, size=1):
        at = chunks[half].at[lines[half]]
        return at.at[place * 2 + c] if size == 1 else at.at[pl.ds(place * 2, size)]

    def one(half, place, c):
        return one_recv.at[half, place * 2 + c]

    def onward(half, ref):
        for d in ring:
            send(ref, ref, chunk_recv.at[half, lines[half]], along(half, False, d, t))

    row = x * 2 + t
    for d, c in near:
        send(q_ref.at[c], qall_ref.at[row], q_recv.at[row], (c, z, y, turn(x, d)))
        for half in range(2):
            send(sources[half].at[c], block(half, places[half], t), one(half, places[half], t), along(half, True, d, c))
    for half in range(2):
        for d in ring:
            send(sources[half].at[t], block(half, places[half], t), chunk_recv.at[half, lines[half]], along(half, False, d, t))
        chunks[half][lines[half], places[half] * 2 + t] = sources[half][t]
    qall_ref[row] = q_ref[t]

    part_ref[...] = jnp.zeros_like(part_ref)
    if heads == GROUP:
        acc_ref = part_ref
    else:
        acc_ref[...] = jnp.zeros_like(acc_ref)
    stat_ref[...] = jnp.zeros_like(stat_ref)
    norm_ref[...] = jnp.zeros_like(norm_ref)
    qz_ref[...] = jnp.zeros_like(qz_ref)

    def q_arrived(d, c):
        at = turn(x, SIDE - d) * 2 + c
        send.arrived(qall_ref.at[at], q_recv.at[at])
        return at

    for d, relayed in zip(NEAR, range(2)):
        for c in range(2):
            at = q_arrived(d, c)
            if relay and c == relayed:
                send(qall_ref.at[at], qall_ref.at[at], q_recv.at[at], (t, z, y, turn(x, d)))
        for half in range(2):
            place = turn(places[half], SIDE - d)
            for c in range(2):
                send.arrived(block(half, place, c), one(half, place, c))
            if relay:
                ref = block(half, place, relayed)
                send(ref, ref, one(half, place, relayed), along(half, True, d, t))
            onward(half, block(half, place, 0, 2))
    q_arrived(0, other)
    for half in range(2):
        ref = block(half, places[half], other)
        send.arrived(ref, one(half, places[half], other))
        onward(half, ref)
    for half in range(2):
        place = turn(places[half], 2)
        for c in range(2):
            send.arrived(block(half, place, c), one(half, place, c))
        onward(half, block(half, place, 0, 2))
    for c in range(2):
        q_arrived(2, c)

    rows = q_ref.shape[1]
    count = ROW * rows
    chip_lanes = qz_ref.shape[-1] // SIDE
    lane = lax.broadcasted_iota(jnp.int32, (1, 128), 1)
    q_norm = jnp.zeros((1, 128), jnp.float32)
    for p in range(q_ref.shape[-1] // 128):
        flat = qall_ref[:, :, p * 128:(p + 1) * 128].reshape(count, 128)
        if count % 128:
            flat = jnp.concatenate([flat, jnp.zeros((-count % 128, 128), flat.dtype)], axis=0)
        turned = flat.T
        for i in range(2):
            group, h = divmod(2 * p + i, heads)
            own = turned[i * HEAD:(i + 1) * HEAD]
            at = h % 2 * HEAD
            for chip in range(SIDE):
                first = chip * chip_lanes + group * 2 * rows
                qz_ref[h, at:at + HEAD, first:first + 2 * rows] = own[:, chip * 2 * rows:(chip + 1) * 2 * rows]
            size = jnp.sum(own.astype(jnp.float32) ** 2, axis=0, keepdims=True)
            q_norm = jnp.where(lane == h, jnp.maximum(q_norm, jnp.max(size, axis=1, keepdims=True)), q_norm)

    width = heads * HEAD
    lanes = 512
    v_first = width // 128 * 128
    v_base = width - v_first
    pairs = -(-heads // 2) * 128
    picks = lax.broadcasted_iota(jnp.int32, (pairs, 128), 0) // HEAD == lax.broadcasted_iota(jnp.int32, (pairs, 128), 1)
    picks = (picks & (lane < heads)).astype(jnp.bfloat16)
    far = [len(send.started) + i for i in range(4)]

    def passed_on(half, i):
        d = NEAR[i]
        line = turn(lines[half], SIDE - d)
        ref = chunks[half].at[line, pl.ds(i * SIDE, SIDE)]
        return remote_copy(ref, ref, send_sem.at[far[2 * half + i]], chunk_recv.at[half, line], along(half, False, d, t))

    def work(half, line):
        vt_ref = turned_values[half]
        keys = vt_ref.shape[-1]

        def load(first, last):
            return chunks[half][line, :, :, first:last].reshape(keys, last - first)

        values = load(v_first, v_first + vt_ref.shape[0])
        vt_ref[...] = values.T
        sizes = jnp.abs(values.astype(jnp.float32))
        for p in range(vt_ref.shape[0] // 128):
            part = sizes[:, p * 128:(p + 1) * 128].reshape(keys // 8, 8, 128)
            norm_ref[1] = jnp.maximum(norm_ref[1], jnp.max(part, axis=0))
        k_rows = load(0, pairs).astype(jnp.float32)
        sums = jnp.dot((k_rows * k_rows).astype(jnp.bfloat16), picks, preferred_element_type=jnp.float32)
        norm_ref[0] = jnp.maximum(norm_ref[0], jnp.max(sums.reshape(keys // 8, 8, 128), axis=0))
        pieces = 2 if ahead_of else 1
        size = keys // pieces
        tasks = [(h, i) for h in range(heads) for i in range(pieces)]

        def query_block(b, _):
            at = pl.ds(pl.multiple_of(b * lanes, lanes), lanes)

            def scores_of(h, i):
                first = h // 2 * 128
                k_rows = load(first, first + 128)[i * size:(i + 1) * size]
                return jnp.dot(k_rows, qz_ref[h, :, at], preferred_element_type=jnp.float32)

            ready = [scores_of(*task) for task in tasks[:ahead_of]]
            for n, (h, i) in enumerate(tasks):
                if n + ahead_of < len(tasks):
                    ready.append(scores_of(*tasks[n + ahead_of]))
                weights = jnp.exp2(ready.pop(0) * (HEAD ** -0.5 * LOG2E))
                total = jnp.sum(weights.reshape(size // 8, 8, lanes), axis=0)
                values_t = vt_ref[v_base + h * HEAD:v_base + (h + 1) * HEAD, i * size:(i + 1) * size]
                summed = jnp.dot(values_t, weights.astype(jnp.bfloat16), preferred_element_type=jnp.float32)
                totals, sums = (total, summed) if i == 0 else (totals + total, sums + summed)
                if i == pieces - 1:
                    stat_ref[h, :, at] += totals
                    acc_ref[h * HEAD:(h + 1) * HEAD, at] += sums
            return 0

        lax.fori_loop(0, part_ref.shape[-1] // lanes, query_block, 0, unroll=1 if ahead_of else part_ref.shape[-1] // lanes)

    def wait_for(half, d):
        line = turn(lines[half], SIDE - d)
        send.arrived(chunks[half].at[line], chunk_recv.at[half, line])

    if relay:

        def chunk(j, _):
            ahead = j + j // 2 - 2 * (j // 3)

            @pl.when(j == 1)
            def near_chunks():
                for i in range(2):
                    for half in range(2):
                        wait_for(half, NEAR[i])
                        passed_on(half, i).start()

            @pl.when(j == 3)
            def far_chunks():
                for half in range(2):
                    wait_for(half, 2)

            for half in range(2):
                work(half, turn(lines[half], ahead))
            return 0

        lax.fori_loop(0, SIDE, chunk, 0)
    else:
        for half in range(2):
            for d in ring:
                wait_for(half, d)
            work(half, slice(None))
    totals = folded([jnp.broadcast_to(jnp.sum(stat_ref[h], axis=0, keepdims=True), stat_ref[h].shape) for h in range(heads)])
    for h in range(GROUP):
        at = GROUP * (HEAD + 1) + h
        part_ref[at:at + 1] = totals[h][:1]
    if heads > GROUP:
        for h, rows in enumerate(folded([acc_ref[h * HEAD:(h + 1) * HEAD] for h in range(heads)])):
            part_ref[h * HEAD:(h + 1) * HEAD] = rows
    guard_ref[0] = jnp.broadcast_to(jnp.max(norm_ref[0], axis=0, keepdims=True) * q_norm, (8, 128))
    guard_ref[1] = norm_ref[1]
    send.drain()
    if relay:
        for half in range(2):
            for i in range(2):
                passed_on(half, i).wait_send()


def mend_kernel(heads, guard_ref, part_in, kva_ref, kvb_ref, qz_ref, part_ref, a_ref, b_ref, q_ref, acc_ref, out_ref, stat_ref, sem):
    del part_in
    limit = (SAFE_SCORE * HEAD ** 0.5) ** 2 / 1.05
    safe = (jnp.max(guard_ref[0]) <= limit) & (jnp.max(guard_ref[1]) <= SAFE_VALUE)

    def fetch(src, dst):
        copy = pltpu.make_async_copy(src, dst, sem)
        copy.start()
        copy.wait()

    @pl.when(jnp.logical_not(safe))
    def again():
        width = heads * HEAD
        lanes = q_ref.shape[-1]

        def query_block(b, _):
            at = pl.multiple_of(b * lanes, lanes)
            fetch(qz_ref.at[:, :, pl.ds(at, lanes)], q_ref)
            acc_ref[...] = jnp.zeros_like(acc_ref)
            for h in range(heads):
                stat_ref[h] = jnp.full((8, lanes), -jnp.inf, jnp.float32)
                stat_ref[heads + h] = jnp.zeros((8, lanes), jnp.float32)
            for kv_ref, keys_ref in ((kva_ref, a_ref), (kvb_ref, b_ref)):

                def keys_block(i, _, kv_ref=kv_ref, keys_ref=keys_ref):
                    fetch(kv_ref.at[i // ROW, lax.rem(i, ROW)], keys_ref)
                    for h in range(heads):
                        first = h // 2 * 128
                        scores = jnp.dot(keys_ref[:, first:first + 128], q_ref[h], preferred_element_type=jnp.float32) * HEAD ** -0.5
                        old = stat_ref[h, 0:1]
                        new = jnp.maximum(old, jnp.max(scores, axis=0, keepdims=True))
                        weights = jnp.exp(scores - new)
                        fade = jnp.exp(old - new)
                        stat_ref[h, 0:1] = new
                        stat_ref[heads + h, 0:1] = stat_ref[heads + h, 0:1] * fade + jnp.sum(weights, axis=0, keepdims=True)
                        values = keys_ref[:, width + h * HEAD:width + (h + 1) * HEAD]
                        summed = lax.dot_general(values, weights.astype(jnp.bfloat16), (((0,), (0,)), ((), ())), preferred_element_type=jnp.float32)
                        acc_ref[h * HEAD:(h + 1) * HEAD] = acc_ref[h * HEAD:(h + 1) * HEAD] * fade + summed
                    return 0

                lax.fori_loop(0, SIDE * ROW, keys_block, 0)
            sums = folded([acc_ref[h * HEAD:(h + 1) * HEAD] for h in range(heads)])
            tops, totals = (folded([jnp.broadcast_to(stat_ref[i + h, 0:1], stat_ref.shape[1:]) for h in range(heads)]) for i in (0, heads))
            for h in range(GROUP):
                out_ref[h * HEAD:(h + 1) * HEAD] = sums[h]
                row = GROUP * HEAD + h
                out_ref[row:row + 1] = tops[h][:1]
                out_ref[row + GROUP:row + GROUP + 1] = totals[h][:1]
            fetch(out_ref, part_ref.at[:, pl.ds(at, lanes)])
            return 0

        lax.fori_loop(0, part_ref.shape[-1] // lanes, query_block, 0)


def attend(a, b, q, heads, ahead_of, collective_id):
    lanes = a.shape[-1]
    sets = q.shape[-1] // (heads * HEAD)
    relay = sets == 2
    count = SIDE * (-(-2 * q.shape[1] * sets // 128) * 128)
    block = 512
    out_rows = -(-GROUP * (HEAD + 2) // 8) * 8
    keys = ROW if relay else ROW * SIDE
    v_rows = lanes - heads * HEAD // 128 * 128
    vmem = pl.BlockSpec(memory_space=pltpu.VMEM)
    anywhere = pl.BlockSpec(memory_space=pl.ANY)
    part, kva, kvb, qz, guard = pl.pallas_call(
        functools.partial(attend_kernel, heads, relay, ahead_of),
        out_shape=(
            jax.ShapeDtypeStruct((out_rows, count), jnp.float32),
            jax.ShapeDtypeStruct((SIDE, ROW) + a.shape[1:], a.dtype),
            jax.ShapeDtypeStruct((SIDE, ROW) + b.shape[1:], b.dtype),
            jax.ShapeDtypeStruct((heads, 128, count), q.dtype),
            jax.ShapeDtypeStruct((2, 8, 128), jnp.float32),
        ),
        in_specs=[vmem] * 3,
        out_specs=(vmem,) * 5,
        scratch_shapes=[
            pltpu.VMEM((ROW,) + q.shape[1:], q.dtype),
            pltpu.VMEM((heads * HEAD, count) if heads > GROUP else (8, 128), jnp.float32),
            pltpu.VMEM((heads, 8, count), jnp.float32),
            pltpu.VMEM((v_rows, keys * a.shape[1]), jnp.bfloat16),
            pltpu.VMEM((v_rows, keys * b.shape[1]), jnp.bfloat16),
            pltpu.VMEM((2, 8, 128), jnp.float32),
            pltpu.SemaphoreType.DMA((64,)),
            pltpu.SemaphoreType.DMA((2, ROW)),
            pltpu.SemaphoreType.DMA((2, SIDE)),
            pltpu.SemaphoreType.DMA((ROW,)),
        ],
        compiler_params=pltpu.CompilerParams(collective_id=collective_id, has_side_effects=True, vmem_limit_bytes=VMEM_LIMIT),
        name="attend",
    )(a, b, q)
    return pl.pallas_call(
        functools.partial(mend_kernel, heads),
        out_shape=jax.ShapeDtypeStruct(part.shape, part.dtype),
        in_specs=[vmem] + [anywhere] * 4,
        out_specs=anywhere,
        input_output_aliases={1: 0},
        scratch_shapes=[
            pltpu.VMEM(a.shape[1:], a.dtype),
            pltpu.VMEM(b.shape[1:], b.dtype),
            pltpu.VMEM((heads, 128, block), q.dtype),
            pltpu.VMEM((heads * HEAD, block), jnp.float32),
            pltpu.VMEM((out_rows, block), jnp.float32),
            pltpu.VMEM((2 * heads, 8, block), jnp.float32),
            pltpu.SemaphoreType.DMA,
        ],
        compiler_params=pltpu.CompilerParams(vmem_limit_bytes=VMEM_LIMIT),
        name="mend",
    )(guard, part, kva, kvb, qz)


def combine_kernel(part_ref, out_ref, got_ref, send_sem, recv_sem):
    t, z, y, x = position()
    partner = (1 - t, z, y, x)
    ring = NEAR + (2,)
    signal_all([partner] + [(t, z, y, turn(x, d)) for d in ring])
    send = Sender(send_sem, (t, z, y, x))
    lanes = got_ref.shape[-1]

    def chip(i):
        return part_ref.at[:, pl.ds(pl.multiple_of(i * lanes, 128), lanes)]

    for d in (2,) + NEAR:
        to = turn(x, d)
        send(chip(to), got_ref.at[x], recv_sem.at[x], (t, z, y, to))
    got_ref[x] = chip(x)[...]
    for d in ring:
        at = turn(x, d)
        send.arrived(got_ref.at[at], recv_sem.at[at])
    width = GROUP * HEAD
    for h in range(GROUP):
        tops = [got_ref[i, width + h:width + h + 1] for i in range(SIDE)]
        top = functools.reduce(jnp.maximum, tops)
        fades = [jnp.exp(m - top) for m in tops]
        total = sum(f * got_ref[i, width + GROUP + h:width + GROUP + h + 1] for i, f in enumerate(fades))
        merged = sum(f / total * got_ref[i, h * HEAD:(h + 1) * HEAD] for i, f in enumerate(fades))
        out_ref[t, h * HEAD:(h + 1) * HEAD] = merged.astype(jnp.bfloat16)
    send(out_ref.at[t], out_ref.at[t], recv_sem.at[SIDE], partner)
    send.arrived(out_ref.at[1 - t], recv_sem.at[SIDE])
    send.drain()


def combine(parts, collective_id):
    rows, queries = parts.shape
    vmem = pl.BlockSpec(memory_space=pltpu.VMEM)
    return pl.pallas_call(
        combine_kernel,
        out_shape=jax.ShapeDtypeStruct((2, GROUP * HEAD, queries // SIDE), jnp.bfloat16),
        in_specs=[vmem],
        out_specs=vmem,
        scratch_shapes=[
            pltpu.VMEM((SIDE, rows, queries // SIDE), jnp.float32),
            pltpu.SemaphoreType.DMA((SIDE,)),
            pltpu.SemaphoreType.DMA((SIDE + 1,)),
        ],
        compiler_params=pltpu.CompilerParams(collective_id=collective_id, has_side_effects=True, vmem_limit_bytes=VMEM_LIMIT),
        name="combine",
    )(parts)


def deal_kernel(mask_ref, count_ref, patch_ref, pos_ref, w_ref, bias_ref, hidden_ref, deal_ref, pack_ref, counts_ref, wide_ref, out_ref, in_ref, count_send, count_recv, row_send, row_recv):
    t, me = lax.axis_index("time"), lax.axis_index("region")
    barrier = pltpu.get_barrier_semaphore()

    def each(act):
        def step(d, _):
            act(lax.rem(me + d, REGIONS))
            return 0

        lax.fori_loop(1, REGIONS, step, 0)

    def to(peer):
        return {"time": t, "region": peer}

    def copy(src, dst, send_sem, recv_sem, peer):
        return pltpu.make_async_remote_copy(src_ref=src, dst_ref=dst, send_sem=send_sem, recv_sem=recv_sem, device_id=to(peer), device_id_type=MESH)

    def finish(ref, send_sem, recv_sem):
        rest = ref.at[pl.ds(0, REGIONS - 1)]
        everything = copy(rest, rest, send_sem, recv_sem, me)
        everything.wait_recv()
        everything.wait_send()

    each(lambda peer: pl.semaphore_signal(barrier, inc=1, device_id=to(peer), device_id_type=MESH))
    pl.semaphore_wait(barrier, REGIONS - 1)
    each(lambda peer: copy(count_ref, counts_ref.at[me], count_send, count_recv, peer).start())

    tokens, width = pos_ref.shape
    wide_ref[...] = jnp.zeros_like(wide_ref)
    embedded = jnp.dot(patch_ref[...], w_ref[...], preferred_element_type=jnp.float32) + bias_ref[...] + pos_ref[...].astype(jnp.float32)
    embedded = embedded.astype(jnp.bfloat16)
    mask = mask_ref[...]
    before = lax.broadcasted_iota(jnp.int32, (tokens, tokens), 0) < lax.broadcasted_iota(jnp.int32, (tokens, tokens), 1)
    local_rank = jnp.dot(mask.astype(jnp.bfloat16), before.astype(jnp.bfloat16), preferred_element_type=jnp.float32).astype(jnp.int32)[:1]

    finish(counts_ref, count_send, count_recv)
    counts_ref[me] = count_ref[...]
    counts = counts_ref[:, 0, :]
    region = lax.broadcasted_iota(jnp.int32, (REGIONS, 128), 0)
    lane = lax.broadcasted_iota(jnp.int32, (REGIONS, 128), 1)
    lower = lax.broadcasted_iota(jnp.int32, (REGIONS, REGIONS), 1) < lax.broadcasted_iota(jnp.int32, (REGIONS, REGIONS), 0)
    starts = jnp.dot(lower.astype(jnp.bfloat16), counts.astype(jnp.bfloat16), preferred_element_type=jnp.float32)
    own_start = jnp.sum(jnp.where(region == me, starts, 0.0), axis=0, keepdims=True).astype(jnp.int32)[:, :1]
    on_lanes = [jnp.sum(jnp.where(region == lane, v, 0.0), axis=0, keepdims=True).astype(jnp.int32) for v in (counts, starts)]

    goes_to = jnp.where(mask[:1] > 0.5, ((own_start + local_rank) & (REGIONS - 1)) + REGIONS * (local_rank >> 6), -1)
    deal = (lax.broadcasted_iota(jnp.int32, (2 * REGIONS, tokens), 0) == goes_to).astype(jnp.bfloat16)
    deal_ref[...] = deal
    rows = jnp.dot(deal, embedded, preferred_element_type=jnp.float32)
    pieces = width // 128
    for i in range(2):
        for p in range(pieces):
            wide_ref[:, i * 8 + p, :] = rows[i * REGIONS:(i + 1) * REGIONS, p * 128:(p + 1) * 128]
    out_ref[...] = wide_ref[...].astype(jnp.bfloat16)

    source_counts, source_starts = on_lanes
    places = lax.broadcasted_iota(jnp.int32, (hidden_ref.shape[0], 128), 0)
    first = (me - source_starts) & (REGIONS - 1)
    packs = []
    for i in range(2):
        rank = first + i * REGIONS
        there = (rank < source_counts) & (lane[:1] < REGIONS)
        place = jnp.where(there, (source_starts + rank) >> 6, -1)
        packs.append((places == place).astype(jnp.bfloat16)[:, :REGIONS])
        pack_ref[i] = packs[i]

    each(lambda peer: copy(out_ref.at[peer], in_ref.at[me], row_send, row_recv, peer).start())
    finish(in_ref, row_send, row_recv)
    in_ref[me] = out_ref[me]
    wide_ref[...] = in_ref[...].astype(jnp.float32)
    for p in range(pieces):
        parts = [jnp.dot(packs[i], wide_ref[:, i * 8 + p, :].astype(jnp.bfloat16), preferred_element_type=jnp.float32) for i in range(2)]
        hidden_ref[:, p * 128:(p + 1) * 128] = (parts[0] + parts[1]).astype(jnp.bfloat16)


def deal_out(vis_mask, patches, enc_pos, w_embed, b_embed, collective_id):
    tokens, width = enc_pos.shape
    mask = vis_mask.astype(jnp.float32)
    vmem = pl.BlockSpec(memory_space=pltpu.VMEM)
    return pl.pallas_call(
        deal_kernel,
        out_shape=(
            jax.ShapeDtypeStruct((tokens // 8, width), jnp.bfloat16),
            jax.ShapeDtypeStruct((2 * REGIONS, tokens), jnp.bfloat16),
            jax.ShapeDtypeStruct((2, tokens // 8, REGIONS), jnp.bfloat16),
        ),
        in_specs=[vmem] * 6,
        out_specs=(vmem,) * 3,
        scratch_shapes=[
            pltpu.VMEM((REGIONS, 8, 128), jnp.float32),
            pltpu.VMEM((REGIONS, 16, 128), jnp.float32),
            pltpu.VMEM((REGIONS, 16, 128), jnp.bfloat16),
            pltpu.VMEM((REGIONS, 16, 128), jnp.bfloat16),
        ] + [pltpu.SemaphoreType.DMA] * 4,
        compiler_params=pltpu.CompilerParams(collective_id=collective_id, has_side_effects=True, vmem_limit_bytes=VMEM_LIMIT),
        name="deal",
    )(jnp.broadcast_to(mask, (8, tokens)), jnp.full((8, 128), jnp.sum(mask)), patches, enc_pos, w_embed, b_embed[None])


def exchange_kernel(src_ref, dst_ref, send_sem, recv_sem):
    t, me = lax.axis_index("time"), lax.axis_index("region")
    barrier = pltpu.get_barrier_semaphore()

    def signal(d, _):
        pl.semaphore_signal(barrier, inc=1, device_id={"time": t, "region": lax.rem(me + d, REGIONS)}, device_id_type=MESH)
        return 0

    lax.fori_loop(1, REGIONS, signal, 0)
    pl.semaphore_wait(barrier, REGIONS - 1)

    def start(d, _):
        peer = lax.rem(me + d, REGIONS)
        pltpu.make_async_remote_copy(
            src_ref=src_ref.at[peer],
            dst_ref=dst_ref.at[me],
            send_sem=send_sem,
            recv_sem=recv_sem,
            device_id={"time": t, "region": peer},
            device_id_type=MESH,
        ).start()
        return 0

    lax.fori_loop(1, REGIONS, start, 0)
    rest = dst_ref.at[pl.ds(0, REGIONS - 1)]
    everything = pltpu.make_async_remote_copy(
        src_ref=rest, dst_ref=rest, send_sem=send_sem, recv_sem=recv_sem, device_id={"time": t, "region": me}, device_id_type=MESH
    )
    everything.wait_recv()
    everything.wait_send()
    dst_ref[me] = src_ref[me]


def exchange(rows, collective_id):
    vmem = pl.BlockSpec(memory_space=pltpu.VMEM)
    return pl.pallas_call(
        exchange_kernel,
        out_shape=jax.ShapeDtypeStruct(rows.shape, rows.dtype),
        in_specs=[vmem],
        out_specs=vmem,
        scratch_shapes=[pltpu.SemaphoreType.DMA, pltpu.SemaphoreType.DMA],
        compiler_params=pltpu.CompilerParams(collective_id=collective_id, has_side_effects=True),
        name="exchange",
    )(rows)


def layer_norm(hidden, ln_gain, ln_shift):
    hid_f32 = hidden.astype(jnp.float32)
    mean_val = jnp.mean(hid_f32, axis=-1, keepdims=True)
    centered = hid_f32 - mean_val
    variance = jnp.mean(centered * centered, axis=-1, keepdims=True)
    return centered * lax.rsqrt(variance + LN_EPS) * ln_gain + ln_shift


def run_block(hidden, vec_rows, w_qkv, w_o, w_one, w_two, ahead_of, collective_id):
    tokens, width = hidden.shape
    heads = w_qkv.shape[2] // 2
    half = heads * HEAD
    normed = layer_norm(hidden, vec_rows[0], vec_rows[1]).astype(jnp.bfloat16)
    w_rows = w_qkv.transpose(1, 2, 3, 0).reshape(3 * width, width)
    projected = lax.dot_general(normed, w_rows, (((1,), (1,)), ((), ())), preferred_element_type=jnp.float32)
    bias = jnp.concatenate([vec_rows[4], jnp.zeros_like(vec_rows[4]), vec_rows[5]])
    projected = (projected + bias).astype(jnp.bfloat16)

    def halves(part):
        return jnp.stack([projected[:, part * width + c * half:part * width + (c + 1) * half] for c in range(2)])

    q, k, v = halves(0), halves(1), halves(2)
    both = jnp.concatenate([k, v], axis=-1)
    split = tokens // 2 if tokens % 32 == 0 else 16
    sets = 2 if half % 128 else 1
    rows = tokens // sets
    q = jnp.concatenate([q[:, i * rows:(i + 1) * rows] for i in range(sets)], axis=-1)
    parts = attend(both[:, :split], both[:, split:], q, heads, ahead_of, collective_id)
    attended = combine(parts, collective_id + 1)
    if heads > GROUP:
        attended = jnp.concatenate([attended[:, :, :HEAD], attended[:, :, HEAD:]], axis=1)
    mixed = lax.dot_general(attended.reshape(width, -1), w_o.reshape(width, width), (((0,), (0,)), ((), ())), preferred_element_type=jnp.float32)
    mixed = mixed[:2 * tokens].reshape(sets, 2, rows, width)
    mixed = lax.dynamic_index_in_dim(mixed, lax.axis_index("time"), axis=1, keepdims=False).reshape(tokens, width)
    residual = (hidden.astype(jnp.float32) + mixed + vec_rows[6]).astype(jnp.bfloat16)
    normed_mlp = layer_norm(residual, vec_rows[2], vec_rows[3]).astype(jnp.bfloat16)
    mlp_hidden = jax.nn.gelu(jnp.dot(normed_mlp, w_one, preferred_element_type=jnp.float32) + vec_rows[8:12].reshape(-1), approximate=False).astype(jnp.bfloat16)
    return (residual.astype(jnp.float32) + jnp.dot(mlp_hidden, w_two, preferred_element_type=jnp.float32) + vec_rows[7]).astype(jnp.bfloat16)


def solution(mesh):
    def local_step(patches, enc_pos, vis_mask, dec_pos, w_embed, b_embed, enc_vec, enc_wqkv, enc_wo, enc_w1, enc_w2, enc_final, w_dec_in, mask_token, dec_vec, dec_wqkv, dec_wo, dec_w1, dec_w2, dec_final, w_out):
        hidden, deal, pack = deal_out(vis_mask, patches, enc_pos, w_embed, b_embed, 1)
        for layer in range(enc_vec.shape[0]):
            hidden = run_block(hidden, enc_vec[layer], enc_wqkv[layer], enc_wo[layer], enc_w1[layer], enc_w2[layer], 0, 4 + 2 * layer)
        latent = jnp.dot(layer_norm(hidden, enc_final[0], enc_final[1]).astype(jnp.bfloat16), w_dec_in, preferred_element_type=jnp.float32).astype(jnp.bfloat16)
        back = jnp.stack([lax.dot_general(pack[i], latent, (((0,), (0,)), ((), ())), preferred_element_type=jnp.float32).astype(jnp.bfloat16) for i in range(2)], axis=1)
        returned = exchange(back, 3)
        placed = sum(lax.dot_general(deal[i * REGIONS:(i + 1) * REGIONS], returned[:, i], (((0,), (0,)), ((), ())), preferred_element_type=jnp.float32) for i in range(2))
        hidden = (jnp.where(vis_mask[:, None] == 1, placed, mask_token.astype(jnp.float32)) + dec_pos.astype(jnp.float32)).astype(jnp.bfloat16)
        for layer in range(dec_vec.shape[0]):
            hidden = run_block(hidden, dec_vec[layer], dec_wqkv[layer], dec_wo[layer], dec_w1[layer], dec_w2[layer], layer, 8 + 2 * layer)
        return jnp.dot(layer_norm(hidden, dec_final[0], dec_final[1]).astype(jnp.bfloat16), w_out, preferred_element_type=jnp.float32)

    token_rows = P(TOKEN_AXES, None)
    token_flags = P(TOKEN_AXES)
    replicated = P()
    in_specs = (token_rows, token_rows, token_flags, token_rows) + (replicated,) * 17
    return jax.shard_map(local_step, mesh=mesh, in_specs=in_specs, out_specs=token_rows, check_vma=False)
```

```python
import functools
import jax
import jax.numpy as jnp
from jax import lax
from jax.experimental import pallas as pl
from jax.experimental.pallas import tpu as pltpu
from jax.sharding import PartitionSpec as P

LN_EPS = 1e-6
TOKEN_AXES = ("batch", "time", "region")
SIDE = 4
REGIONS = SIDE ** 3
ROW = SIDE * 2
ENC_FORMS = ((2, 1), (1, 0))
FORMS = ((2, 1), (3, 2))
GROUP = 3
HEAD = 64
MESH = pl.DeviceIdType.MESH
NEAR = (1, SIDE - 1)
VMEM_LIMIT = 60 * 1024 * 1024
LOG2E = 1.4426950408889634
SAFE_SCORE = 60.0
SAFE_VALUE = 1e7


def position():
    t, r = lax.axis_index("time"), lax.axis_index("region")
    return t, r // 16, lax.rem(r // 4, 4), lax.rem(r, 4)


def device(t, z, y, x):
    return {"time": t, "region": z * 16 + y * 4 + x}


def turn(a, d):
    return lax.rem(a + d, SIDE)


def signal_all(peers):
    barrier = pltpu.get_barrier_semaphore()
    for peer in peers:
        pl.semaphore_signal(barrier, inc=1, device_id=device(*peer), device_id_type=MESH)
    pl.semaphore_wait(barrier, len(peers))


class Sender:
    def __init__(self, sems, place):
        self.sems, self.place, self.used, self.started = sems, place, 0, []

    def __call__(self, src, dst, recv_sem, peer):
        copy = remote_copy(src, dst, self.sems.at[self.used], recv_sem, peer)
        copy.start()
        self.used += 1
        self.started.append(copy)

    def arrived(self, ref, recv_sem):
        remote_copy(ref, ref, self.sems.at[0], recv_sem, self.place).wait_recv()

    def drain(self):
        for copy in self.started:
            copy.wait_send()


def remote_copy(src, dst, send_sem, recv_sem, peer):
    return pltpu.make_async_remote_copy(
        src_ref=src, dst_ref=dst, send_sem=send_sem, recv_sem=recv_sem, device_id=device(*peer), device_id_type=MESH
    )


def folded(rows):
    if len(rows) == GROUP:
        return rows
    low = lax.broadcasted_iota(jnp.int32, rows[0].shape, 1) % 128 < HEAD
    return [jnp.where(low, a, pltpu.roll(b, HEAD, axis=1)) for a, b in zip(rows, rows[GROUP:])]


def attend_kernel(heads, relay, form, a_ref, b_ref, q_ref, part_ref, kva_out, kvb_out, qz_ref, guard_ref, kva_ref, kvb_ref, qall_ref, acc_ref, stat_ref, vta_ref, vtb_ref, norm_ref, send_sem, one_recv, chunk_recv, q_recv, keep_sem):
    pieces, ahead_of = form
    kept = (kva_out, kvb_out)
    t, z, y, x = position()
    other = 1 - t
    ring = NEAR if relay else NEAR + (2,)
    near = [(0, other)] + [(d, c) for d in ring for c in range(2)]
    peers = [(other, z, y, x)]
    for d, c in near[1:]:
        peers += [(c, turn(z, d), y, x), (c, z, turn(y, d), x), (c, z, y, turn(x, d))]
    signal_all(peers)

    sources, chunks, turned_values = (a_ref, b_ref), (kva_ref, kvb_ref), (vta_ref, vtb_ref)
    lines, places = (z, y), (y, z)
    send = Sender(send_sem, (t, z, y, x))

    def along(half, first, d, c):
        return (c, z, turn(y, d), x) if (half == 0) == first else (c, turn(z, d), y, x)

    def block(half, place, c, size=1):
        at = chunks[half].at[lines[half]]
        return at.at[place * 2 + c] if size == 1 else at.at[pl.ds(place * 2, size)]

    def one(half, place, c):
        return one_recv.at[half, place * 2 + c]

    def onward(half, ref):
        for d in ring:
            send(ref, ref, chunk_recv.at[half, lines[half]], along(half, False, d, t))

    row = x * 2 + t
    for d, c in near:
        send(q_ref.at[c], qall_ref.at[row], q_recv.at[row], (c, z, y, turn(x, d)))
        for half in range(2):
            send(sources[half].at[c], block(half, places[half], t), one(half, places[half], t), along(half, True, d, c))
    for half in range(2):
        for d in ring:
            send(sources[half].at[t], block(half, places[half], t), chunk_recv.at[half, lines[half]], along(half, False, d, t))
        chunks[half][lines[half], places[half] * 2 + t] = sources[half][t]
    qall_ref[row] = q_ref[t]

    part_ref[...] = jnp.zeros_like(part_ref)
    if heads == GROUP:
        acc_ref = part_ref
    else:
        acc_ref[...] = jnp.zeros_like(acc_ref)
    stat_ref[...] = jnp.zeros_like(stat_ref)
    norm_ref[...] = jnp.zeros_like(norm_ref)
    qz_ref[...] = jnp.zeros_like(qz_ref)

    def q_arrived(d, c):
        at = turn(x, SIDE - d) * 2 + c
        send.arrived(qall_ref.at[at], q_recv.at[at])
        return at

    for d, relayed in zip(NEAR, range(2)):
        for c in range(2):
            at = q_arrived(d, c)
            if relay and c == relayed:
                send(qall_ref.at[at], qall_ref.at[at], q_recv.at[at], (t, z, y, turn(x, d)))
        for half in range(2):
            place = turn(places[half], SIDE - d)
            for c in range(2):
                send.arrived(block(half, place, c), one(half, place, c))
            if relay:
                ref = block(half, place, relayed)
                send(ref, ref, one(half, place, relayed), along(half, True, d, t))
            onward(half, block(half, place, 0, 2))
    q_arrived(0, other)
    for half in range(2):
        ref = block(half, places[half], other)
        send.arrived(ref, one(half, places[half], other))
        onward(half, ref)
    for half in range(2):
        place = turn(places[half], 2)
        for c in range(2):
            send.arrived(block(half, place, c), one(half, place, c))
        onward(half, block(half, place, 0, 2))
    for c in range(2):
        q_arrived(2, c)

    rows = q_ref.shape[1]
    count = ROW * rows
    chip_lanes = qz_ref.shape[-1] // SIDE
    lane = lax.broadcasted_iota(jnp.int32, (1, 128), 1)
    q_norm = jnp.zeros((1, 128), jnp.float32)
    for p in range(q_ref.shape[-1] // 128):
        flat = qall_ref[:, :, p * 128:(p + 1) * 128].reshape(count, 128)
        if count % 128:
            flat = jnp.concatenate([flat, jnp.zeros((-count % 128, 128), flat.dtype)], axis=0)
        turned = flat.T
        for i in range(2):
            group, h = divmod(2 * p + i, heads)
            own = turned[i * HEAD:(i + 1) * HEAD]
            at = h % 2 * HEAD
            for chip in range(SIDE):
                first = chip * chip_lanes + group * 2 * rows
                qz_ref[h, at:at + HEAD, first:first + 2 * rows] = own[:, chip * 2 * rows:(chip + 1) * 2 * rows]
            size = jnp.sum(own.astype(jnp.float32) ** 2, axis=0, keepdims=True)
            q_norm = jnp.where(lane == h, jnp.maximum(q_norm, jnp.max(size, axis=1, keepdims=True)), q_norm)

    width = heads * HEAD
    lanes = 512
    v_first = width // 128 * 128
    v_base = width - v_first
    pairs = -(-heads // 2) * 128
    picks = lax.broadcasted_iota(jnp.int32, (pairs, 128), 0) // HEAD == lax.broadcasted_iota(jnp.int32, (pairs, 128), 1)
    picks = (picks & (lane < heads)).astype(jnp.bfloat16)
    far = [len(send.started) + i for i in range(4)]

    def passed_on(half, i):
        d = NEAR[i]
        line = turn(lines[half], SIDE - d)
        ref = chunks[half].at[line, pl.ds(i * SIDE, SIDE)]
        return remote_copy(ref, ref, send_sem.at[far[2 * half + i]], chunk_recv.at[half, line], along(half, False, d, t))

    def work(half, line):
        vt_ref = turned_values[half]
        keys = vt_ref.shape[-1]

        def load(first, last):
            return chunks[half][line, :, :, first:last].reshape(keys, last - first)

        values = load(v_first, v_first + vt_ref.shape[0])
        vt_ref[...] = values.T
        sizes = jnp.abs(values.astype(jnp.float32))
        for p in range(vt_ref.shape[0] // 128):
            part = sizes[:, p * 128:(p + 1) * 128].reshape(keys // 8, 8, 128)
            norm_ref[1] = jnp.maximum(norm_ref[1], jnp.max(part, axis=0))
        k_rows = load(0, pairs).astype(jnp.float32)
        sums = jnp.dot((k_rows * k_rows).astype(jnp.bfloat16), picks, preferred_element_type=jnp.float32)
        norm_ref[0] = jnp.maximum(norm_ref[0], jnp.max(sums.reshape(keys // 8, 8, 128), axis=0))
        size = keys // pieces
        blocks = part_ref.shape[-1] // lanes
        tasks = [(b, h, i) for b in range(blocks) for h in range(heads) for i in range(pieces)]

        def scores_of(b, h, i):
            first = h // 2 * 128
            k_rows = load(first, first + 128)[i * size:(i + 1) * size]
            return jnp.dot(k_rows, qz_ref[h, :, b * lanes:(b + 1) * lanes], preferred_element_type=jnp.float32)

        ready = [scores_of(*task) for task in tasks[:ahead_of]]
        for n, (b, h, i) in enumerate(tasks):
            if n + ahead_of < len(tasks):
                ready.append(scores_of(*tasks[n + ahead_of]))
            weights = jnp.exp2(ready.pop(0) * (HEAD ** -0.5 * LOG2E))
            total = jnp.sum(weights.reshape(size // 8, 8, lanes), axis=0)
            values_t = vt_ref[v_base + h * HEAD:v_base + (h + 1) * HEAD, i * size:(i + 1) * size]
            summed = jnp.dot(values_t, weights.astype(jnp.bfloat16), preferred_element_type=jnp.float32)
            totals, sums = (total, summed) if i == 0 else (totals + total, sums + summed)
            if i == pieces - 1:
                at = slice(b * lanes, (b + 1) * lanes)
                stat_ref[h, :, at] += totals
                acc_ref[h * HEAD:(h + 1) * HEAD, at] += sums

    def wait_for(half, d):
        line = turn(lines[half], SIDE - d)
        send.arrived(chunks[half].at[line], chunk_recv.at[half, line])

    if relay:

        def chunk(j, _):
            ahead = j + j // 2 - 2 * (j // 3)

            @pl.when(j == 1)
            def near_chunks():
                for i in range(2):
                    for half in range(2):
                        wait_for(half, NEAR[i])
                        passed_on(half, i).start()

            @pl.when(j == 3)
            def far_chunks():
                for half in range(2):
                    wait_for(half, 2)

            for half in range(2):
                line = turn(lines[half], ahead)
                pltpu.make_async_copy(chunks[half].at[line], kept[half].at[line], keep_sem.at[half]).start()
                work(half, line)
            return 0

        lax.fori_loop(0, SIDE, chunk, 0)
    else:
        for half in range(2):
            for d in ring:
                wait_for(half, d)
            pltpu.make_async_copy(chunks[half], kept[half], keep_sem.at[half]).start()
            work(half, slice(None))
    totals = folded([jnp.broadcast_to(jnp.sum(stat_ref[h], axis=0, keepdims=True), stat_ref[h].shape) for h in range(heads)])
    for h in range(GROUP):
        at = GROUP * (HEAD + 1) + h
        part_ref[at:at + 1] = totals[h][:1]
    if heads > GROUP:
        for h, rows in enumerate(folded([acc_ref[h * HEAD:(h + 1) * HEAD] for h in range(heads)])):
            part_ref[h * HEAD:(h + 1) * HEAD] = rows
    guard_ref[0] = jnp.broadcast_to(jnp.max(norm_ref[0], axis=0, keepdims=True) * q_norm, (8, 128))
    guard_ref[1] = norm_ref[1]
    for half in range(2):
        pltpu.make_async_copy(chunks[half], kept[half], keep_sem.at[half]).wait()
    send.drain()
    if relay:
        for half in range(2):
            for i in range(2):
                passed_on(half, i).wait_send()


def mend_kernel(heads, guard_ref, part_in, kva_ref, kvb_ref, qz_ref, part_ref, a_ref, b_ref, q_ref, acc_ref, out_ref, stat_ref, sem):
    del part_in
    limit = (SAFE_SCORE * HEAD ** 0.5) ** 2 / 1.05
    safe = (jnp.max(guard_ref[0]) <= limit) & (jnp.max(guard_ref[1]) <= SAFE_VALUE)

    def fetch(src, dst):
        copy = pltpu.make_async_copy(src, dst, sem)
        copy.start()
        copy.wait()

    @pl.when(jnp.logical_not(safe))
    def again():
        width = heads * HEAD
        lanes = q_ref.shape[-1]

        def query_block(b, _):
            at = pl.multiple_of(b * lanes, lanes)
            fetch(qz_ref.at[:, :, pl.ds(at, lanes)], q_ref)
            acc_ref[...] = jnp.zeros_like(acc_ref)
            for h in range(heads):
                stat_ref[h] = jnp.full((8, lanes), -jnp.inf, jnp.float32)
                stat_ref[heads + h] = jnp.zeros((8, lanes), jnp.float32)
            for kv_ref, keys_ref in ((kva_ref, a_ref), (kvb_ref, b_ref)):

                def keys_block(i, _, kv_ref=kv_ref, keys_ref=keys_ref):
                    fetch(kv_ref.at[i // ROW, lax.rem(i, ROW)], keys_ref)
                    for h in range(heads):
                        first = h // 2 * 128
                        scores = jnp.dot(keys_ref[:, first:first + 128], q_ref[h], preferred_element_type=jnp.float32) * HEAD ** -0.5
                        old = stat_ref[h, 0:1]
                        new = jnp.maximum(old, jnp.max(scores, axis=0, keepdims=True))
                        weights = jnp.exp(scores - new)
                        fade = jnp.exp(old - new)
                        stat_ref[h, 0:1] = new
                        stat_ref[heads + h, 0:1] = stat_ref[heads + h, 0:1] * fade + jnp.sum(weights, axis=0, keepdims=True)
                        values = keys_ref[:, width + h * HEAD:width + (h + 1) * HEAD]
                        summed = lax.dot_general(values, weights.astype(jnp.bfloat16), (((0,), (0,)), ((), ())), preferred_element_type=jnp.float32)
                        acc_ref[h * HEAD:(h + 1) * HEAD] = acc_ref[h * HEAD:(h + 1) * HEAD] * fade + summed
                    return 0

                lax.fori_loop(0, SIDE * ROW, keys_block, 0)
            sums = folded([acc_ref[h * HEAD:(h + 1) * HEAD] for h in range(heads)])
            tops, totals = (folded([jnp.broadcast_to(stat_ref[i + h, 0:1], stat_ref.shape[1:]) for h in range(heads)]) for i in (0, heads))
            for h in range(GROUP):
                out_ref[h * HEAD:(h + 1) * HEAD] = sums[h]
                row = GROUP * HEAD + h
                out_ref[row:row + 1] = tops[h][:1]
                out_ref[row + GROUP:row + GROUP + 1] = totals[h][:1]
            fetch(out_ref, part_ref.at[:, pl.ds(at, lanes)])
            return 0

        lax.fori_loop(0, part_ref.shape[-1] // lanes, query_block, 0)


def attend(a, b, q, heads, form, collective_id):
    lanes = a.shape[-1]
    sets = q.shape[-1] // (heads * HEAD)
    relay = sets == 2
    count = SIDE * (-(-2 * q.shape[1] * sets // 128) * 128)
    block = 512
    out_rows = -(-GROUP * (HEAD + 2) // 8) * 8
    keys = ROW if relay else ROW * SIDE
    v_rows = lanes - heads * HEAD // 128 * 128
    vmem = pl.BlockSpec(memory_space=pltpu.VMEM)
    anywhere = pl.BlockSpec(memory_space=pl.ANY)
    part, kva, kvb, qz, guard = pl.pallas_call(
        functools.partial(attend_kernel, heads, relay, form),
        out_shape=(
            jax.ShapeDtypeStruct((out_rows, count), jnp.float32),
            jax.ShapeDtypeStruct((SIDE, ROW) + a.shape[1:], a.dtype),
            jax.ShapeDtypeStruct((SIDE, ROW) + b.shape[1:], b.dtype),
            jax.ShapeDtypeStruct((heads, 128, count), q.dtype),
            jax.ShapeDtypeStruct((2, 8, 128), jnp.float32),
        ),
        in_specs=[vmem] * 3,
        out_specs=(vmem, anywhere, anywhere, vmem, vmem),
        scratch_shapes=[
            pltpu.VMEM((SIDE, ROW) + a.shape[1:], a.dtype),
            pltpu.VMEM((SIDE, ROW) + b.shape[1:], b.dtype),
            pltpu.VMEM((ROW,) + q.shape[1:], q.dtype),
            pltpu.VMEM((heads * HEAD, count) if heads > GROUP else (8, 128), jnp.float32),
            pltpu.VMEM((heads, 8, count), jnp.float32),
            pltpu.VMEM((v_rows, keys * a.shape[1]), jnp.bfloat16),
            pltpu.VMEM((v_rows, keys * b.shape[1]), jnp.bfloat16),
            pltpu.VMEM((2, 8, 128), jnp.float32),
            pltpu.SemaphoreType.DMA((64,)),
            pltpu.SemaphoreType.DMA((2, ROW)),
            pltpu.SemaphoreType.DMA((2, SIDE)),
            pltpu.SemaphoreType.DMA((ROW,)),
            pltpu.SemaphoreType.DMA((2,)),
        ],
        compiler_params=pltpu.CompilerParams(collective_id=collective_id, has_side_effects=True, vmem_limit_bytes=VMEM_LIMIT),
        name="attend",
    )(a, b, q)
    return pl.pallas_call(
        functools.partial(mend_kernel, heads),
        out_shape=jax.ShapeDtypeStruct(part.shape, part.dtype),
        in_specs=[vmem] + [anywhere] * 4,
        out_specs=anywhere,
        input_output_aliases={1: 0},
        scratch_shapes=[
            pltpu.VMEM(a.shape[1:], a.dtype),
            pltpu.VMEM(b.shape[1:], b.dtype),
            pltpu.VMEM((heads, 128, block), q.dtype),
            pltpu.VMEM((heads * HEAD, block), jnp.float32),
            pltpu.VMEM((out_rows, block), jnp.float32),
            pltpu.VMEM((2 * heads, 8, block), jnp.float32),
            pltpu.SemaphoreType.DMA,
        ],
        compiler_params=pltpu.CompilerParams(vmem_limit_bytes=VMEM_LIMIT),
        name="mend",
    )(guard, part, kva, kvb, qz)


def combine_kernel(part_ref, out_ref, got_ref, send_sem, recv_sem):
    t, z, y, x = position()
    partner = (1 - t, z, y, x)
    ring = NEAR + (2,)
    signal_all([partner] + [(t, z, y, turn(x, d)) for d in ring])
    send = Sender(send_sem, (t, z, y, x))
    lanes = got_ref.shape[-1]

    def chip(i):
        return part_ref.at[:, pl.ds(pl.multiple_of(i * lanes, 128), lanes)]

    for d in (2,) + NEAR:
        to = turn(x, d)
        send(chip(to), got_ref.at[x], recv_sem.at[x], (t, z, y, to))
    got_ref[x] = chip(x)[...]
    for d in ring:
        at = turn(x, d)
        send.arrived(got_ref.at[at], recv_sem.at[at])
    width = GROUP * HEAD
    for h in range(GROUP):
        tops = [got_ref[i, width + h:width + h + 1] for i in range(SIDE)]
        top = functools.reduce(jnp.maximum, tops)
        fades = [jnp.exp(m - top) for m in tops]
        total = sum(f * got_ref[i, width + GROUP + h:width + GROUP + h + 1] for i, f in enumerate(fades))
        merged = sum(f / total * got_ref[i, h * HEAD:(h + 1) * HEAD] for i, f in enumerate(fades))
        out_ref[t, h * HEAD:(h + 1) * HEAD] = merged.astype(jnp.bfloat16)
    send(out_ref.at[t], out_ref.at[t], recv_sem.at[SIDE], partner)
    send.arrived(out_ref.at[1 - t], recv_sem.at[SIDE])
    send.drain()


def combine(parts, collective_id):
    rows, queries = parts.shape
    vmem = pl.BlockSpec(memory_space=pltpu.VMEM)
    return pl.pallas_call(
        combine_kernel,
        out_shape=jax.ShapeDtypeStruct((2, GROUP * HEAD, queries // SIDE), jnp.bfloat16),
        in_specs=[vmem],
        out_specs=vmem,
        scratch_shapes=[
            pltpu.VMEM((SIDE, rows, queries // SIDE), jnp.float32),
            pltpu.SemaphoreType.DMA((SIDE,)),
            pltpu.SemaphoreType.DMA((SIDE + 1,)),
        ],
        compiler_params=pltpu.CompilerParams(collective_id=collective_id, has_side_effects=True, vmem_limit_bytes=VMEM_LIMIT),
        name="combine",
    )(parts)


def deal_kernel(mask_ref, count_ref, patch_ref, pos_ref, w_ref, bias_ref, hidden_ref, deal_ref, pack_ref, counts_ref, wide_ref, out_ref, in_ref, count_send, count_recv, row_send, row_recv):
    t, me = lax.axis_index("time"), lax.axis_index("region")
    barrier = pltpu.get_barrier_semaphore()

    def each(act):
        def step(d, _):
            act(lax.rem(me + d, REGIONS))
            return 0

        lax.fori_loop(1, REGIONS, step, 0)

    def to(peer):
        return {"time": t, "region": peer}

    def copy(src, dst, send_sem, recv_sem, peer):
        return pltpu.make_async_remote_copy(src_ref=src, dst_ref=dst, send_sem=send_sem, recv_sem=recv_sem, device_id=to(peer), device_id_type=MESH)

    def finish(ref, send_sem, recv_sem):
        rest = ref.at[pl.ds(0, REGIONS - 1)]
        everything = copy(rest, rest, send_sem, recv_sem, me)
        everything.wait_recv()
        everything.wait_send()

    each(lambda peer: pl.semaphore_signal(barrier, inc=1, device_id=to(peer), device_id_type=MESH))
    pl.semaphore_wait(barrier, REGIONS - 1)
    each(lambda peer: copy(count_ref, counts_ref.at[me], count_send, count_recv, peer).start())

    tokens, width = pos_ref.shape
    wide_ref[...] = jnp.zeros_like(wide_ref)
    embedded = jnp.dot(patch_ref[...], w_ref[...], preferred_element_type=jnp.float32) + bias_ref[...] + pos_ref[...].astype(jnp.float32)
    embedded = embedded.astype(jnp.bfloat16)
    mask = mask_ref[...]
    before = lax.broadcasted_iota(jnp.int32, (tokens, tokens), 0) < lax.broadcasted_iota(jnp.int32, (tokens, tokens), 1)
    local_rank = jnp.dot(mask.astype(jnp.bfloat16), before.astype(jnp.bfloat16), preferred_element_type=jnp.float32).astype(jnp.int32)[:1]

    finish(counts_ref, count_send, count_recv)
    counts_ref[me] = count_ref[...]
    counts = counts_ref[:, 0, :]
    region = lax.broadcasted_iota(jnp.int32, (REGIONS, 128), 0)
    lane = lax.broadcasted_iota(jnp.int32, (REGIONS, 128), 1)
    lower = lax.broadcasted_iota(jnp.int32, (REGIONS, REGIONS), 1) < lax.broadcasted_iota(jnp.int32, (REGIONS, REGIONS), 0)
    starts = jnp.dot(lower.astype(jnp.bfloat16), counts.astype(jnp.bfloat16), preferred_element_type=jnp.float32)
    own_start = jnp.sum(jnp.where(region == me, starts, 0.0), axis=0, keepdims=True).astype(jnp.int32)[:, :1]
    on_lanes = [jnp.sum(jnp.where(region == lane, v, 0.0), axis=0, keepdims=True).astype(jnp.int32) for v in (counts, starts)]

    goes_to = jnp.where(mask[:1] > 0.5, ((own_start + local_rank) & (REGIONS - 1)) + REGIONS * (local_rank >> 6), -1)
    deal = (lax.broadcasted_iota(jnp.int32, (2 * REGIONS, tokens), 0) == goes_to).astype(jnp.bfloat16)
    deal_ref[...] = deal
    rows = jnp.dot(deal, embedded, preferred_element_type=jnp.float32)
    pieces = width // 128
    for i in range(2):
        for p in range(pieces):
            wide_ref[:, i * 8 + p, :] = rows[i * REGIONS:(i + 1) * REGIONS, p * 128:(p + 1) * 128]
    out_ref[...] = wide_ref[...].astype(jnp.bfloat16)

    source_counts, source_starts = on_lanes
    places = lax.broadcasted_iota(jnp.int32, (hidden_ref.shape[0], 128), 0)
    first = (me - source_starts) & (REGIONS - 1)
    packs = []
    for i in range(2):
        rank = first + i * REGIONS
        there = (rank < source_counts) & (lane[:1] < REGIONS)
        place = jnp.where(there, (source_starts + rank) >> 6, -1)
        packs.append((places == place).astype(jnp.bfloat16)[:, :REGIONS])
        pack_ref[i] = packs[i]

    each(lambda peer: copy(out_ref.at[peer], in_ref.at[me], row_send, row_recv, peer).start())
    finish(in_ref, row_send, row_recv)
    in_ref[me] = out_ref[me]
    wide_ref[...] = in_ref[...].astype(jnp.float32)
    for p in range(pieces):
        parts = [jnp.dot(packs[i], wide_ref[:, i * 8 + p, :].astype(jnp.bfloat16), preferred_element_type=jnp.float32) for i in range(2)]
        hidden_ref[:, p * 128:(p + 1) * 128] = (parts[0] + parts[1]).astype(jnp.bfloat16)


def deal_out(vis_mask, patches, enc_pos, w_embed, b_embed, collective_id):
    tokens, width = enc_pos.shape
    mask = vis_mask.astype(jnp.float32)
    vmem = pl.BlockSpec(memory_space=pltpu.VMEM)
    return pl.pallas_call(
        deal_kernel,
        out_shape=(
            jax.ShapeDtypeStruct((tokens // 8, width), jnp.bfloat16),
            jax.ShapeDtypeStruct((2 * REGIONS, tokens), jnp.bfloat16),
            jax.ShapeDtypeStruct((2, tokens // 8, REGIONS), jnp.bfloat16),
        ),
        in_specs=[vmem] * 6,
        out_specs=(vmem,) * 3,
        scratch_shapes=[
            pltpu.VMEM((REGIONS, 8, 128), jnp.float32),
            pltpu.VMEM((REGIONS, 16, 128), jnp.float32),
            pltpu.VMEM((REGIONS, 16, 128), jnp.bfloat16),
            pltpu.VMEM((REGIONS, 16, 128), jnp.bfloat16),
        ] + [pltpu.SemaphoreType.DMA] * 4,
        compiler_params=pltpu.CompilerParams(collective_id=collective_id, has_side_effects=True, vmem_limit_bytes=VMEM_LIMIT),
        name="deal",
    )(jnp.broadcast_to(mask, (8, tokens)), jnp.full((8, 128), jnp.sum(mask)), patches, enc_pos, w_embed, b_embed[None])


def exchange_kernel(src_ref, dst_ref, send_sem, recv_sem):
    t, me = lax.axis_index("time"), lax.axis_index("region")
    barrier = pltpu.get_barrier_semaphore()

    def signal(d, _):
        pl.semaphore_signal(barrier, inc=1, device_id={"time": t, "region": lax.rem(me + d, REGIONS)}, device_id_type=MESH)
        return 0

    lax.fori_loop(1, REGIONS, signal, 0)
    pl.semaphore_wait(barrier, REGIONS - 1)

    def start(d, _):
        peer = lax.rem(me + d, REGIONS)
        pltpu.make_async_remote_copy(
            src_ref=src_ref.at[peer],
            dst_ref=dst_ref.at[me],
            send_sem=send_sem,
            recv_sem=recv_sem,
            device_id={"time": t, "region": peer},
            device_id_type=MESH,
        ).start()
        return 0

    lax.fori_loop(1, REGIONS, start, 0)
    rest = dst_ref.at[pl.ds(0, REGIONS - 1)]
    everything = pltpu.make_async_remote_copy(
        src_ref=rest, dst_ref=rest, send_sem=send_sem, recv_sem=recv_sem, device_id={"time": t, "region": me}, device_id_type=MESH
    )
    everything.wait_recv()
    everything.wait_send()
    dst_ref[me] = src_ref[me]


def exchange(rows, collective_id):
    vmem = pl.BlockSpec(memory_space=pltpu.VMEM)
    return pl.pallas_call(
        exchange_kernel,
        out_shape=jax.ShapeDtypeStruct(rows.shape, rows.dtype),
        in_specs=[vmem],
        out_specs=vmem,
        scratch_shapes=[pltpu.SemaphoreType.DMA, pltpu.SemaphoreType.DMA],
        compiler_params=pltpu.CompilerParams(collective_id=collective_id, has_side_effects=True),
        name="exchange",
    )(rows)


def layer_norm(hidden, ln_gain, ln_shift):
    hid_f32 = hidden.astype(jnp.float32)
    mean_val = jnp.mean(hid_f32, axis=-1, keepdims=True)
    centered = hid_f32 - mean_val
    variance = jnp.mean(centered * centered, axis=-1, keepdims=True)
    return centered * lax.rsqrt(variance + LN_EPS) * ln_gain + ln_shift


def run_block(hidden, vec_rows, w_qkv, w_o, w_one, w_two, form, collective_id):
    tokens, width = hidden.shape
    heads = w_qkv.shape[2] // 2
    half = heads * HEAD
    normed = layer_norm(hidden, vec_rows[0], vec_rows[1]).astype(jnp.bfloat16)
    w_rows = w_qkv.transpose(1, 2, 3, 0).reshape(3 * width, width)
    projected = lax.dot_general(normed, w_rows, (((1,), (1,)), ((), ())), preferred_element_type=jnp.float32)
    bias = jnp.concatenate([vec_rows[4], jnp.zeros_like(vec_rows[4]), vec_rows[5]])
    projected = (projected + bias).astype(jnp.bfloat16)

    def halves(part):
        return jnp.stack([projected[:, part * width + c * half:part * width + (c + 1) * half] for c in range(2)])

    q, k, v = halves(0), halves(1), halves(2)
    both = jnp.concatenate([k, v], axis=-1)
    split = tokens // 2 if tokens % 32 == 0 else 16
    sets = 2 if half % 128 else 1
    rows = tokens // sets
    q = jnp.concatenate([q[:, i * rows:(i + 1) * rows] for i in range(sets)], axis=-1)
    parts = attend(both[:, :split], both[:, split:], q, heads, form, collective_id)
    attended = combine(parts, collective_id + 1)
    if heads > GROUP:
        attended = jnp.concatenate([attended[:, :, :HEAD], attended[:, :, HEAD:]], axis=1)
    mixed = lax.dot_general(attended.reshape(width, -1), w_o.reshape(width, width), (((0,), (0,)), ((), ())), preferred_element_type=jnp.float32)
    mixed = mixed[:2 * tokens].reshape(sets, 2, rows, width)
    mixed = lax.dynamic_index_in_dim(mixed, lax.axis_index("time"), axis=1, keepdims=False).reshape(tokens, width)
    residual = (hidden.astype(jnp.float32) + mixed + vec_rows[6]).astype(jnp.bfloat16)
    normed_mlp = layer_norm(residual, vec_rows[2], vec_rows[3]).astype(jnp.bfloat16)
    mlp_hidden = jax.nn.gelu(jnp.dot(normed_mlp, w_one, preferred_element_type=jnp.float32) + vec_rows[8:12].reshape(-1), approximate=False).astype(jnp.bfloat16)
    return (residual.astype(jnp.float32) + jnp.dot(mlp_hidden, w_two, preferred_element_type=jnp.float32) + vec_rows[7]).astype(jnp.bfloat16)


def solution(mesh):
    def local_step(patches, enc_pos, vis_mask, dec_pos, w_embed, b_embed, enc_vec, enc_wqkv, enc_wo, enc_w1, enc_w2, enc_final, w_dec_in, mask_token, dec_vec, dec_wqkv, dec_wo, dec_w1, dec_w2, dec_final, w_out):
        hidden, deal, pack = deal_out(vis_mask, patches, enc_pos, w_embed, b_embed, 1)
        for layer in range(enc_vec.shape[0]):
            hidden = run_block(hidden, enc_vec[layer], enc_wqkv[layer], enc_wo[layer], enc_w1[layer], enc_w2[layer], ENC_FORMS[layer], 4 + 2 * layer)
        latent = jnp.dot(layer_norm(hidden, enc_final[0], enc_final[1]).astype(jnp.bfloat16), w_dec_in, preferred_element_type=jnp.float32).astype(jnp.bfloat16)
        back = jnp.stack([lax.dot_general(pack[i], latent, (((0,), (0,)), ((), ())), preferred_element_type=jnp.float32).astype(jnp.bfloat16) for i in range(2)], axis=1)
        returned = exchange(back, 3)
        placed = sum(lax.dot_general(deal[i * REGIONS:(i + 1) * REGIONS], returned[:, i], (((0,), (0,)), ((), ())), preferred_element_type=jnp.float32) for i in range(2))
        hidden = (jnp.where(vis_mask[:, None] == 1, placed, mask_token.astype(jnp.float32)) + dec_pos.astype(jnp.float32)).astype(jnp.bfloat16)
        for layer in range(dec_vec.shape[0]):
            hidden = run_block(hidden, dec_vec[layer], dec_wqkv[layer], dec_wo[layer], dec_w1[layer], dec_w2[layer], FORMS[layer], 8 + 2 * layer)
        return jnp.dot(layer_norm(hidden, dec_final[0], dec_final[1]).astype(jnp.bfloat16), w_out, preferred_element_type=jnp.float32)

    token_rows = P(TOKEN_AXES, None)
    token_flags = P(TOKEN_AXES)
    replicated = P()
    in_specs = (token_rows, token_rows, token_flags, token_rows) + (replicated,) * 17
    return jax.shard_map(local_step, mesh=mesh, in_specs=in_specs, out_specs=token_rows, check_vma=False)
```

```python
import functools
import jax
import jax.numpy as jnp
from jax import lax
from jax.experimental import pallas as pl
from jax.experimental.pallas import tpu as pltpu
from jax.sharding import PartitionSpec as P

LN_EPS = 1e-6
TOKEN_AXES = ("batch", "time", "region")
SIDE = 4
REGIONS = SIDE ** 3
ROW = SIDE * 2
ENC_FORMS = ((2, 1), (1, 0))
FORMS = ((3, 2), (4, 3))
GROUP = 3
HEAD = 64
MESH = pl.DeviceIdType.MESH
NEAR = (1, SIDE - 1)
VMEM_LIMIT = 60 * 1024 * 1024
LOG2E = 1.4426950408889634
SAFE_SCORE = 60.0
SAFE_VALUE = 1e7


def position():
    t, r = lax.axis_index("time"), lax.axis_index("region")
    return t, r // 16, lax.rem(r // 4, 4), lax.rem(r, 4)


def device(t, z, y, x):
    return {"time": t, "region": z * 16 + y * 4 + x}


def turn(a, d):
    return lax.rem(a + d, SIDE)


def signal_all(peers):
    barrier = pltpu.get_barrier_semaphore()
    for peer in peers:
        pl.semaphore_signal(barrier, inc=1, device_id=device(*peer), device_id_type=MESH)
    pl.semaphore_wait(barrier, len(peers))


class Sender:
    def __init__(self, sems, place):
        self.sems, self.place, self.used, self.started = sems, place, 0, []

    def __call__(self, src, dst, recv_sem, peer):
        copy = remote_copy(src, dst, self.sems.at[self.used], recv_sem, peer)
        copy.start()
        self.used += 1
        self.started.append(copy)

    def arrived(self, ref, recv_sem):
        remote_copy(ref, ref, self.sems.at[0], recv_sem, self.place).wait_recv()

    def drain(self):
        for copy in self.started:
            copy.wait_send()


def remote_copy(src, dst, send_sem, recv_sem, peer):
    return pltpu.make_async_remote_copy(
        src_ref=src, dst_ref=dst, send_sem=send_sem, recv_sem=recv_sem, device_id=device(*peer), device_id_type=MESH
    )


def folded(rows):
    if len(rows) == GROUP:
        return rows
    low = lax.broadcasted_iota(jnp.int32, rows[0].shape, 1) % 128 < HEAD
    return [jnp.where(low, a, pltpu.roll(b, HEAD, axis=1)) for a, b in zip(rows, rows[GROUP:])]


def attend_kernel(heads, relay, form, a_ref, b_ref, q_ref, part_ref, kva_out, kvb_out, qz_ref, guard_ref, kva_ref, kvb_ref, qall_ref, acc_ref, stat_ref, vta_ref, vtb_ref, norm_ref, send_sem, one_recv, chunk_recv, q_recv, keep_sem):
    pieces, ahead_of = form
    kept = (kva_out, kvb_out)
    t, z, y, x = position()
    other = 1 - t
    ring = NEAR if relay else NEAR + (2,)
    near = [(0, other)] + [(d, c) for d in ring for c in range(2)]
    peers = [(other, z, y, x)]
    for d, c in near[1:]:
        peers += [(c, turn(z, d), y, x), (c, z, turn(y, d), x), (c, z, y, turn(x, d))]
    signal_all(peers)

    sources, chunks, turned_values = (a_ref, b_ref), (kva_ref, kvb_ref), (vta_ref, vtb_ref)
    lines, places = (z, y), (y, z)
    send = Sender(send_sem, (t, z, y, x))

    def along(half, first, d, c):
        return (c, z, turn(y, d), x) if (half == 0) == first else (c, turn(z, d), y, x)

    def block(half, place, c, size=1):
        at = chunks[half].at[lines[half]]
        return at.at[place * 2 + c] if size == 1 else at.at[pl.ds(place * 2, size)]

    def one(half, place, c):
        return one_recv.at[half, place * 2 + c]

    def onward(half, ref):
        for d in ring:
            send(ref, ref, chunk_recv.at[half, lines[half]], along(half, False, d, t))

    row = x * 2 + t
    for d, c in near:
        send(q_ref.at[c], qall_ref.at[row], q_recv.at[row], (c, z, y, turn(x, d)))
        for half in range(2):
            send(sources[half].at[c], block(half, places[half], t), one(half, places[half], t), along(half, True, d, c))
    for half in range(2):
        for d in ring:
            send(sources[half].at[t], block(half, places[half], t), chunk_recv.at[half, lines[half]], along(half, False, d, t))
        chunks[half][lines[half], places[half] * 2 + t] = sources[half][t]
    qall_ref[row] = q_ref[t]

    part_ref[...] = jnp.zeros_like(part_ref)
    if heads == GROUP:
        acc_ref = part_ref
    else:
        acc_ref[...] = jnp.zeros_like(acc_ref)
    stat_ref[...] = jnp.zeros_like(stat_ref)
    norm_ref[...] = jnp.zeros_like(norm_ref)
    qz_ref[...] = jnp.zeros_like(qz_ref)

    def q_arrived(d, c):
        at = turn(x, SIDE - d) * 2 + c
        send.arrived(qall_ref.at[at], q_recv.at[at])
        return at

    for d, relayed in zip(NEAR, range(2)):
        for c in range(2):
            at = q_arrived(d, c)
            if relay and c == relayed:
                send(qall_ref.at[at], qall_ref.at[at], q_recv.at[at], (t, z, y, turn(x, d)))
        for half in range(2):
            place = turn(places[half], SIDE - d)
            for c in range(2):
                send.arrived(block(half, place, c), one(half, place, c))
            if relay:
                ref = block(half, place, relayed)
                send(ref, ref, one(half, place, relayed), along(half, True, d, t))
            onward(half, block(half, place, 0, 2))
    q_arrived(0, other)
    for half in range(2):
        ref = block(half, places[half], other)
        send.arrived(ref, one(half, places[half], other))
        onward(half, ref)
    for half in range(2):
        place = turn(places[half], 2)
        for c in range(2):
            send.arrived(block(half, place, c), one(half, place, c))
        onward(half, block(half, place, 0, 2))
    for c in range(2):
        q_arrived(2, c)

    rows = q_ref.shape[1]
    count = ROW * rows
    chip_lanes = qz_ref.shape[-1] // SIDE
    lane = lax.broadcasted_iota(jnp.int32, (1, 128), 1)
    q_norm = jnp.zeros((1, 128), jnp.float32)
    for p in range(q_ref.shape[-1] // 128):
        flat = qall_ref[:, :, p * 128:(p + 1) * 128].reshape(count, 128)
        if count % 128:
            flat = jnp.concatenate([flat, jnp.zeros((-count % 128, 128), flat.dtype)], axis=0)
        turned = flat.T
        for i in range(2):
            group, h = divmod(2 * p + i, heads)
            own = turned[i * HEAD:(i + 1) * HEAD]
            at = h % 2 * HEAD
            for chip in range(SIDE):
                first = chip * chip_lanes + group * 2 * rows
                qz_ref[h, at:at + HEAD, first:first + 2 * rows] = own[:, chip * 2 * rows:(chip + 1) * 2 * rows]
            size = jnp.sum(own.astype(jnp.float32) ** 2, axis=0, keepdims=True)
            q_norm = jnp.where(lane == h, jnp.maximum(q_norm, jnp.max(size, axis=1, keepdims=True)), q_norm)

    width = heads * HEAD
    lanes = 512
    v_first = width // 128 * 128
    v_base = width - v_first
    pairs = -(-heads // 2) * 128
    picks = lax.broadcasted_iota(jnp.int32, (pairs, 128), 0) // HEAD == lax.broadcasted_iota(jnp.int32, (pairs, 128), 1)
    picks = (picks & (lane < heads)).astype(jnp.bfloat16)
    far = [len(send.started) + i for i in range(4)]

    def passed_on(half, i):
        d = NEAR[i]
        line = turn(lines[half], SIDE - d)
        ref = chunks[half].at[line, pl.ds(i * SIDE, SIDE)]
        return remote_copy(ref, ref, send_sem.at[far[2 * half + i]], chunk_recv.at[half, line], along(half, False, d, t))

    def work(half, line):
        vt_ref = turned_values[half]
        keys = vt_ref.shape[-1]

        def load(first, last):
            return chunks[half][line, :, :, first:last].reshape(keys, last - first)

        values = load(v_first, v_first + vt_ref.shape[0])
        vt_ref[...] = values.T
        sizes = jnp.abs(values.astype(jnp.float32))
        for p in range(vt_ref.shape[0] // 128):
            part = sizes[:, p * 128:(p + 1) * 128].reshape(keys // 8, 8, 128)
            norm_ref[1] = jnp.maximum(norm_ref[1], jnp.max(part, axis=0))
        k_rows = load(0, pairs).astype(jnp.float32)
        sums = jnp.dot((k_rows * k_rows).astype(jnp.bfloat16), picks, preferred_element_type=jnp.float32)
        norm_ref[0] = jnp.maximum(norm_ref[0], jnp.max(sums.reshape(keys // 8, 8, 128), axis=0))
        size = keys // pieces
        blocks = part_ref.shape[-1] // lanes
        tasks = [(b, h, i) for b in range(blocks) for h in range(heads) for i in range(pieces)]

        def scores_of(b, h, i):
            first = h // 2 * 128
            k_rows = load(first, first + 128)[i * size:(i + 1) * size]
            return jnp.dot(k_rows, qz_ref[h, :, b * lanes:(b + 1) * lanes], preferred_element_type=jnp.float32)

        ready = [scores_of(*task) for task in tasks[:ahead_of]]
        for n, (b, h, i) in enumerate(tasks):
            if n + ahead_of < len(tasks):
                ready.append(scores_of(*tasks[n + ahead_of]))
            weights = jnp.exp2(ready.pop(0) * (HEAD ** -0.5 * LOG2E))
            total = jnp.sum(weights.reshape(size // 8, 8, lanes), axis=0)
            values_t = vt_ref[v_base + h * HEAD:v_base + (h + 1) * HEAD, i * size:(i + 1) * size]
            summed = jnp.dot(values_t, weights.astype(jnp.bfloat16), preferred_element_type=jnp.float32)
            totals, sums = (total, summed) if i == 0 else (totals + total, sums + summed)
            if i == pieces - 1:
                at = slice(b * lanes, (b + 1) * lanes)
                stat_ref[h, :, at] += totals
                acc_ref[h * HEAD:(h + 1) * HEAD, at] += sums

    def wait_for(half, d):
        line = turn(lines[half], SIDE - d)
        send.arrived(chunks[half].at[line], chunk_recv.at[half, line])

    if relay:

        def chunk(j, _):
            ahead = j + j // 2 - 2 * (j // 3)

            @pl.when(j == 1)
            def near_chunks():
                for i in range(2):
                    for half in range(2):
                        wait_for(half, NEAR[i])
                        passed_on(half, i).start()

            @pl.when(j == 3)
            def far_chunks():
                for half in range(2):
                    wait_for(half, 2)

            for half in range(2):
                line = turn(lines[half], ahead)
                pltpu.make_async_copy(chunks[half].at[line], kept[half].at[line], keep_sem.at[half]).start()
                work(half, line)
            return 0

        lax.fori_loop(0, SIDE, chunk, 0)
    else:
        for half in range(2):
            for d in ring:
                wait_for(half, d)
            pltpu.make_async_copy(chunks[half], kept[half], keep_sem.at[half]).start()
            work(half, slice(None))
    totals = folded([jnp.broadcast_to(jnp.sum(stat_ref[h], axis=0, keepdims=True), stat_ref[h].shape) for h in range(heads)])
    for h in range(GROUP):
        at = GROUP * (HEAD + 1) + h
        part_ref[at:at + 1] = totals[h][:1]
    if heads > GROUP:
        for h, rows in enumerate(folded([acc_ref[h * HEAD:(h + 1) * HEAD] for h in range(heads)])):
            part_ref[h * HEAD:(h + 1) * HEAD] = rows
    guard_ref[0] = jnp.broadcast_to(jnp.max(norm_ref[0], axis=0, keepdims=True) * q_norm, (8, 128))
    guard_ref[1] = norm_ref[1]
    for half in range(2):
        pltpu.make_async_copy(chunks[half], kept[half], keep_sem.at[half]).wait()
    send.drain()
    if relay:
        for half in range(2):
            for i in range(2):
                passed_on(half, i).wait_send()


def mend_kernel(heads, guard_ref, part_in, kva_ref, kvb_ref, qz_ref, part_ref, a_ref, b_ref, q_ref, acc_ref, out_ref, stat_ref, sem):
    del part_in
    limit = (SAFE_SCORE * HEAD ** 0.5) ** 2 / 1.05
    safe = (jnp.max(guard_ref[0]) <= limit) & (jnp.max(guard_ref[1]) <= SAFE_VALUE)

    def fetch(src, dst):
        copy = pltpu.make_async_copy(src, dst, sem)
        copy.start()
        copy.wait()

    @pl.when(jnp.logical_not(safe))
    def again():
        width = heads * HEAD
        lanes = q_ref.shape[-1]

        def query_block(b, _):
            at = pl.multiple_of(b * lanes, lanes)
            fetch(qz_ref.at[:, :, pl.ds(at, lanes)], q_ref)
            acc_ref[...] = jnp.zeros_like(acc_ref)
            for h in range(heads):
                stat_ref[h] = jnp.full((8, lanes), -jnp.inf, jnp.float32)
                stat_ref[heads + h] = jnp.zeros((8, lanes), jnp.float32)
            for kv_ref, keys_ref in ((kva_ref, a_ref), (kvb_ref, b_ref)):

                def keys_block(i, _, kv_ref=kv_ref, keys_ref=keys_ref):
                    fetch(kv_ref.at[i // ROW, lax.rem(i, ROW)], keys_ref)
                    for h in range(heads):
                        first = h // 2 * 128
                        scores = jnp.dot(keys_ref[:, first:first + 128], q_ref[h], preferred_element_type=jnp.float32) * HEAD ** -0.5
                        old = stat_ref[h, 0:1]
                        new = jnp.maximum(old, jnp.max(scores, axis=0, keepdims=True))
                        weights = jnp.exp(scores - new)
                        fade = jnp.exp(old - new)
                        stat_ref[h, 0:1] = new
                        stat_ref[heads + h, 0:1] = stat_ref[heads + h, 0:1] * fade + jnp.sum(weights, axis=0, keepdims=True)
                        values = keys_ref[:, width + h * HEAD:width + (h + 1) * HEAD]
                        summed = lax.dot_general(values, weights.astype(jnp.bfloat16), (((0,), (0,)), ((), ())), preferred_element_type=jnp.float32)
                        acc_ref[h * HEAD:(h + 1) * HEAD] = acc_ref[h * HEAD:(h + 1) * HEAD] * fade + summed
                    return 0

                lax.fori_loop(0, SIDE * ROW, keys_block, 0)
            sums = folded([acc_ref[h * HEAD:(h + 1) * HEAD] for h in range(heads)])
            tops, totals = (folded([jnp.broadcast_to(stat_ref[i + h, 0:1], stat_ref.shape[1:]) for h in range(heads)]) for i in (0, heads))
            for h in range(GROUP):
                out_ref[h * HEAD:(h + 1) * HEAD] = sums[h]
                row = GROUP * HEAD + h
                out_ref[row:row + 1] = tops[h][:1]
                out_ref[row + GROUP:row + GROUP + 1] = totals[h][:1]
            fetch(out_ref, part_ref.at[:, pl.ds(at, lanes)])
            return 0

        lax.fori_loop(0, part_ref.shape[-1] // lanes, query_block, 0)


def attend(a, b, q, heads, form, collective_id):
    lanes = a.shape[-1]
    sets = q.shape[-1] // (heads * HEAD)
    relay = sets == 2
    count = SIDE * (-(-2 * q.shape[1] * sets // 128) * 128)
    block = 512
    out_rows = -(-GROUP * (HEAD + 2) // 8) * 8
    keys = ROW if relay else ROW * SIDE
    v_rows = lanes - heads * HEAD // 128 * 128
    vmem = pl.BlockSpec(memory_space=pltpu.VMEM)
    anywhere = pl.BlockSpec(memory_space=pl.ANY)
    part, kva, kvb, qz, guard = pl.pallas_call(
        functools.partial(attend_kernel, heads, relay, form),
        out_shape=(
            jax.ShapeDtypeStruct((out_rows, count), jnp.float32),
            jax.ShapeDtypeStruct((SIDE, ROW) + a.shape[1:], a.dtype),
            jax.ShapeDtypeStruct((SIDE, ROW) + b.shape[1:], b.dtype),
            jax.ShapeDtypeStruct((heads, 128, count), q.dtype),
            jax.ShapeDtypeStruct((2, 8, 128), jnp.float32),
        ),
        in_specs=[vmem] * 3,
        out_specs=(vmem, anywhere, anywhere, vmem, vmem),
        scratch_shapes=[
            pltpu.VMEM((SIDE, ROW) + a.shape[1:], a.dtype),
            pltpu.VMEM((SIDE, ROW) + b.shape[1:], b.dtype),
            pltpu.VMEM((ROW,) + q.shape[1:], q.dtype),
            pltpu.VMEM((heads * HEAD, count) if heads > GROUP else (8, 128), jnp.float32),
            pltpu.VMEM((heads, 8, count), jnp.float32),
            pltpu.VMEM((v_rows, keys * a.shape[1]), jnp.bfloat16),
            pltpu.VMEM((v_rows, keys * b.shape[1]), jnp.bfloat16),
            pltpu.VMEM((2, 8, 128), jnp.float32),
            pltpu.SemaphoreType.DMA((64,)),
            pltpu.SemaphoreType.DMA((2, ROW)),
            pltpu.SemaphoreType.DMA((2, SIDE)),
            pltpu.SemaphoreType.DMA((ROW,)),
            pltpu.SemaphoreType.DMA((2,)),
        ],
        compiler_params=pltpu.CompilerParams(collective_id=collective_id, has_side_effects=True, vmem_limit_bytes=VMEM_LIMIT),
        name="attend",
    )(a, b, q)
    return pl.pallas_call(
        functools.partial(mend_kernel, heads),
        out_shape=jax.ShapeDtypeStruct(part.shape, part.dtype),
        in_specs=[vmem] + [anywhere] * 4,
        out_specs=anywhere,
        input_output_aliases={1: 0},
        scratch_shapes=[
            pltpu.VMEM(a.shape[1:], a.dtype),
            pltpu.VMEM(b.shape[1:], b.dtype),
            pltpu.VMEM((heads, 128, block), q.dtype),
            pltpu.VMEM((heads * HEAD, block), jnp.float32),
            pltpu.VMEM((out_rows, block), jnp.float32),
            pltpu.VMEM((2 * heads, 8, block), jnp.float32),
            pltpu.SemaphoreType.DMA,
        ],
        compiler_params=pltpu.CompilerParams(vmem_limit_bytes=VMEM_LIMIT),
        name="mend",
    )(guard, part, kva, kvb, qz)


def combine_kernel(part_ref, out_ref, got_ref, send_sem, recv_sem):
    t, z, y, x = position()
    partner = (1 - t, z, y, x)
    ring = NEAR + (2,)
    signal_all([partner] + [(t, z, y, turn(x, d)) for d in ring])
    send = Sender(send_sem, (t, z, y, x))
    lanes = got_ref.shape[-1]

    def chip(i):
        return part_ref.at[:, pl.ds(pl.multiple_of(i * lanes, 128), lanes)]

    for d in (2,) + NEAR:
        to = turn(x, d)
        send(chip(to), got_ref.at[x], recv_sem.at[x], (t, z, y, to))
    got_ref[x] = chip(x)[...]
    for d in ring:
        at = turn(x, d)
        send.arrived(got_ref.at[at], recv_sem.at[at])
    width = GROUP * HEAD
    for h in range(GROUP):
        tops = [got_ref[i, width + h:width + h + 1] for i in range(SIDE)]
        top = functools.reduce(jnp.maximum, tops)
        fades = [jnp.exp(m - top) for m in tops]
        total = sum(f * got_ref[i, width + GROUP + h:width + GROUP + h + 1] for i, f in enumerate(fades))
        merged = sum(f / total * got_ref[i, h * HEAD:(h + 1) * HEAD] for i, f in enumerate(fades))
        out_ref[t, h * HEAD:(h + 1) * HEAD] = merged.astype(jnp.bfloat16)
    send(out_ref.at[t], out_ref.at[t], recv_sem.at[SIDE], partner)
    send.arrived(out_ref.at[1 - t], recv_sem.at[SIDE])
    send.drain()


def combine(parts, collective_id):
    rows, queries = parts.shape
    vmem = pl.BlockSpec(memory_space=pltpu.VMEM)
    return pl.pallas_call(
        combine_kernel,
        out_shape=jax.ShapeDtypeStruct((2, GROUP * HEAD, queries // SIDE), jnp.bfloat16),
        in_specs=[vmem],
        out_specs=vmem,
        scratch_shapes=[
            pltpu.VMEM((SIDE, rows, queries // SIDE), jnp.float32),
            pltpu.SemaphoreType.DMA((SIDE,)),
            pltpu.SemaphoreType.DMA((SIDE + 1,)),
        ],
        compiler_params=pltpu.CompilerParams(collective_id=collective_id, has_side_effects=True, vmem_limit_bytes=VMEM_LIMIT),
        name="combine",
    )(parts)


def deal_kernel(mask_ref, patch_ref, pos_ref, w_ref, bias_ref, hidden_ref, deal_ref, pack_ref, count_ref, counts_ref, wide_ref, out_ref, in_ref, count_send, count_recv, row_send, row_recv):
    t, me = lax.axis_index("time"), lax.axis_index("region")
    barrier = pltpu.get_barrier_semaphore()

    def each(act):
        def step(d, _):
            act(lax.rem(me + d, REGIONS))
            return 0

        lax.fori_loop(1, REGIONS, step, 0)

    def to(peer):
        return {"time": t, "region": peer}

    def copy(src, dst, send_sem, recv_sem, peer):
        return pltpu.make_async_remote_copy(src_ref=src, dst_ref=dst, send_sem=send_sem, recv_sem=recv_sem, device_id=to(peer), device_id_type=MESH)

    def finish(ref, send_sem, recv_sem):
        rest = ref.at[pl.ds(0, REGIONS - 1)]
        everything = copy(rest, rest, send_sem, recv_sem, me)
        everything.wait_recv()
        everything.wait_send()

    mask = jnp.broadcast_to(mask_ref[...].astype(jnp.float32), (8, mask_ref.shape[1]))
    count_ref[...] = jnp.broadcast_to(jnp.sum(mask, axis=1, keepdims=True), count_ref.shape)
    each(lambda peer: pl.semaphore_signal(barrier, inc=1, device_id=to(peer), device_id_type=MESH))
    pl.semaphore_wait(barrier, REGIONS - 1)
    each(lambda peer: copy(count_ref, counts_ref.at[me], count_send, count_recv, peer).start())

    tokens, width = pos_ref.shape
    wide_ref[...] = jnp.zeros_like(wide_ref)
    embedded = jnp.dot(patch_ref[...], w_ref[...], preferred_element_type=jnp.float32) + bias_ref[...] + pos_ref[...].astype(jnp.float32)
    embedded = embedded.astype(jnp.bfloat16)
    before = lax.broadcasted_iota(jnp.int32, (tokens, tokens), 0) < lax.broadcasted_iota(jnp.int32, (tokens, tokens), 1)
    local_rank = jnp.dot(mask.astype(jnp.bfloat16), before.astype(jnp.bfloat16), preferred_element_type=jnp.float32).astype(jnp.int32)[:1]

    finish(counts_ref, count_send, count_recv)
    counts_ref[me] = count_ref[...]
    counts = counts_ref[:, 0, :]
    region = lax.broadcasted_iota(jnp.int32, (REGIONS, 128), 0)
    lane = lax.broadcasted_iota(jnp.int32, (REGIONS, 128), 1)
    lower = lax.broadcasted_iota(jnp.int32, (REGIONS, REGIONS), 1) < lax.broadcasted_iota(jnp.int32, (REGIONS, REGIONS), 0)
    starts = jnp.dot(lower.astype(jnp.bfloat16), counts.astype(jnp.bfloat16), preferred_element_type=jnp.float32)
    own_start = jnp.sum(jnp.where(region == me, starts, 0.0), axis=0, keepdims=True).astype(jnp.int32)[:, :1]
    on_lanes = [jnp.sum(jnp.where(region == lane, v, 0.0), axis=0, keepdims=True).astype(jnp.int32) for v in (counts, starts)]

    goes_to = jnp.where(mask[:1] > 0.5, ((own_start + local_rank) & (REGIONS - 1)) + REGIONS * (local_rank >> 6), -1)
    deal = (lax.broadcasted_iota(jnp.int32, (2 * REGIONS, tokens), 0) == goes_to).astype(jnp.bfloat16)
    deal_ref[...] = deal
    rows = jnp.dot(deal, embedded, preferred_element_type=jnp.float32)
    pieces = width // 128
    for i in range(2):
        for p in range(pieces):
            wide_ref[:, i * 8 + p, :] = rows[i * REGIONS:(i + 1) * REGIONS, p * 128:(p + 1) * 128]
    out_ref[...] = wide_ref[...].astype(jnp.bfloat16)

    source_counts, source_starts = on_lanes
    places = lax.broadcasted_iota(jnp.int32, (hidden_ref.shape[0], 128), 0)
    first = (me - source_starts) & (REGIONS - 1)
    packs = []
    for i in range(2):
        rank = first + i * REGIONS
        there = (rank < source_counts) & (lane[:1] < REGIONS)
        place = jnp.where(there, (source_starts + rank) >> 6, -1)
        packs.append((places == place).astype(jnp.bfloat16)[:, :REGIONS])
        pack_ref[i] = packs[i]

    each(lambda peer: copy(out_ref.at[peer], in_ref.at[me], row_send, row_recv, peer).start())
    finish(in_ref, row_send, row_recv)
    in_ref[me] = out_ref[me]
    wide_ref[...] = in_ref[...].astype(jnp.float32)
    for p in range(pieces):
        parts = [jnp.dot(packs[i], wide_ref[:, i * 8 + p, :].astype(jnp.bfloat16), preferred_element_type=jnp.float32) for i in range(2)]
        hidden_ref[:, p * 128:(p + 1) * 128] = (parts[0] + parts[1]).astype(jnp.bfloat16)


def deal_out(vis_mask, patches, enc_pos, w_embed, b_embed, collective_id):
    tokens, width = enc_pos.shape
    vmem = pl.BlockSpec(memory_space=pltpu.VMEM)
    return pl.pallas_call(
        deal_kernel,
        out_shape=(
            jax.ShapeDtypeStruct((tokens // 8, width), jnp.bfloat16),
            jax.ShapeDtypeStruct((2 * REGIONS, tokens), jnp.bfloat16),
            jax.ShapeDtypeStruct((2, tokens // 8, REGIONS), jnp.bfloat16),
        ),
        in_specs=[vmem] * 5,
        out_specs=(vmem,) * 3,
        scratch_shapes=[
            pltpu.VMEM((8, 128), jnp.float32),
            pltpu.VMEM((REGIONS, 8, 128), jnp.float32),
            pltpu.VMEM((REGIONS, 16, 128), jnp.float32),
            pltpu.VMEM((REGIONS, 16, 128), jnp.bfloat16),
            pltpu.VMEM((REGIONS, 16, 128), jnp.bfloat16),
        ] + [pltpu.SemaphoreType.DMA] * 4,
        compiler_params=pltpu.CompilerParams(collective_id=collective_id, has_side_effects=True, vmem_limit_bytes=VMEM_LIMIT),
        name="deal",
    )(vis_mask[None], patches, enc_pos, w_embed, b_embed[None])


def exchange_kernel(src_ref, dst_ref, send_sem, recv_sem):
    t, me = lax.axis_index("time"), lax.axis_index("region")
    barrier = pltpu.get_barrier_semaphore()

    def signal(d, _):
        pl.semaphore_signal(barrier, inc=1, device_id={"time": t, "region": lax.rem(me + d, REGIONS)}, device_id_type=MESH)
        return 0

    lax.fori_loop(1, REGIONS, signal, 0)
    pl.semaphore_wait(barrier, REGIONS - 1)

    def start(d, _):
        peer = lax.rem(me + d, REGIONS)
        pltpu.make_async_remote_copy(
            src_ref=src_ref.at[peer],
            dst_ref=dst_ref.at[me],
            send_sem=send_sem,
            recv_sem=recv_sem,
            device_id={"time": t, "region": peer},
            device_id_type=MESH,
        ).start()
        return 0

    lax.fori_loop(1, REGIONS, start, 0)
    rest = dst_ref.at[pl.ds(0, REGIONS - 1)]
    everything = pltpu.make_async_remote_copy(
        src_ref=rest, dst_ref=rest, send_sem=send_sem, recv_sem=recv_sem, device_id={"time": t, "region": me}, device_id_type=MESH
    )
    everything.wait_recv()
    everything.wait_send()
    dst_ref[me] = src_ref[me]


def exchange(rows, collective_id):
    vmem = pl.BlockSpec(memory_space=pltpu.VMEM)
    return pl.pallas_call(
        exchange_kernel,
        out_shape=jax.ShapeDtypeStruct(rows.shape, rows.dtype),
        in_specs=[vmem],
        out_specs=vmem,
        scratch_shapes=[pltpu.SemaphoreType.DMA, pltpu.SemaphoreType.DMA],
        compiler_params=pltpu.CompilerParams(collective_id=collective_id, has_side_effects=True, vmem_limit_bytes=VMEM_LIMIT),
        name="exchange",
    )(rows)


def layer_norm(hidden, ln_gain, ln_shift):
    hid_f32 = hidden.astype(jnp.float32)
    mean_val = jnp.mean(hid_f32, axis=-1, keepdims=True)
    centered = hid_f32 - mean_val
    variance = jnp.mean(centered * centered, axis=-1, keepdims=True)
    return centered * lax.rsqrt(variance + LN_EPS) * ln_gain + ln_shift


def run_block(hidden, vec_rows, w_qkv, w_o, w_one, w_two, form, collective_id):
    tokens, width = hidden.shape
    half = width // 2
    heads = half // HEAD
    normed = layer_norm(hidden, vec_rows[0], vec_rows[1]).astype(jnp.bfloat16)
    projected = lax.dot_general(normed, w_qkv, (((1,), (1,)), ((), ())), preferred_element_type=jnp.float32)
    bias = jnp.concatenate([vec_rows[4], jnp.zeros_like(vec_rows[4]), vec_rows[5]])
    projected = (projected + bias).astype(jnp.bfloat16)

    def halves(part):
        return jnp.stack([projected[:, part * width + c * half:part * width + (c + 1) * half] for c in range(2)])

    q, k, v = halves(0), halves(1), halves(2)
    both = jnp.concatenate([k, v], axis=-1)
    split = tokens // 2 if tokens % 32 == 0 else 16
    sets = 2 if half % 128 else 1
    rows = tokens // sets
    q = jnp.concatenate([q[:, i * rows:(i + 1) * rows] for i in range(sets)], axis=-1)
    parts = attend(both[:, :split], both[:, split:], q, heads, form, collective_id)
    attended = combine(parts, collective_id + 1)
    if heads > GROUP:
        attended = jnp.concatenate([attended[:, :, :HEAD], attended[:, :, HEAD:]], axis=1)
    mixed = lax.dot_general(attended.reshape(width, -1), w_o, (((0,), (0,)), ((), ())), preferred_element_type=jnp.float32)
    mixed = mixed[:2 * tokens].reshape(sets, 2, rows, width)
    mixed = lax.dynamic_index_in_dim(mixed, lax.axis_index("time"), axis=1, keepdims=False).reshape(tokens, width)
    residual = (hidden.astype(jnp.float32) + mixed + vec_rows[6]).astype(jnp.bfloat16)
    normed_mlp = layer_norm(residual, vec_rows[2], vec_rows[3]).astype(jnp.bfloat16)
    mlp_hidden = jax.nn.gelu(jnp.dot(normed_mlp, w_one, preferred_element_type=jnp.float32) + vec_rows[8:12].reshape(-1), approximate=False).astype(jnp.bfloat16)
    return (residual.astype(jnp.float32) + jnp.dot(mlp_hidden, w_two, preferred_element_type=jnp.float32) + vec_rows[7]).astype(jnp.bfloat16)


def solution(mesh):
    def local_step(patches, enc_pos, vis_mask, dec_pos, w_embed, b_embed, enc_vec, enc_wqkv, enc_wo, enc_w1, enc_w2, enc_final, w_dec_in, mask_token, dec_vec, dec_wqkv, dec_wo, dec_w1, dec_w2, dec_final, w_out):
        enc_rows, dec_rows = (w.transpose(0, 2, 3, 4, 1).reshape(w.shape[0], -1, w.shape[1]) for w in (enc_wqkv, dec_wqkv))
        enc_out, dec_out = (w.reshape(w.shape[0], -1, w.shape[3]) for w in (enc_wo, dec_wo))
        enc_rows, dec_rows, enc_out, dec_out = lax.optimization_barrier((enc_rows, dec_rows, enc_out, dec_out))
        hidden, deal, pack = deal_out(vis_mask, patches, enc_pos, w_embed, b_embed, 1)
        for layer in range(enc_vec.shape[0]):
            hidden = run_block(hidden, enc_vec[layer], enc_rows[layer], enc_out[layer], enc_w1[layer], enc_w2[layer], ENC_FORMS[layer], 4 + 2 * layer)
        latent = jnp.dot(layer_norm(hidden, enc_final[0], enc_final[1]).astype(jnp.bfloat16), w_dec_in, preferred_element_type=jnp.float32).astype(jnp.bfloat16)
        back = jnp.stack([lax.dot_general(pack[i], latent, (((0,), (0,)), ((), ())), preferred_element_type=jnp.float32).astype(jnp.bfloat16) for i in range(2)], axis=1)
        returned = exchange(back, 3)
        placed = sum(lax.dot_general(deal[i * REGIONS:(i + 1) * REGIONS], returned[:, i], (((0,), (0,)), ((), ())), preferred_element_type=jnp.float32) for i in range(2))
        hidden = (jnp.where(vis_mask[:, None] == 1, placed, mask_token.astype(jnp.float32)) + dec_pos.astype(jnp.float32)).astype(jnp.bfloat16)
        for layer in range(dec_vec.shape[0]):
            hidden = run_block(hidden, dec_vec[layer], dec_rows[layer], dec_out[layer], dec_w1[layer], dec_w2[layer], FORMS[layer], 8 + 2 * layer)
        return jnp.dot(layer_norm(hidden, dec_final[0], dec_final[1]).astype(jnp.bfloat16), w_out, preferred_element_type=jnp.float32)

    token_rows = P(TOKEN_AXES, None)
    token_flags = P(TOKEN_AXES)
    replicated = P()
    in_specs = (token_rows, token_rows, token_flags, token_rows) + (replicated,) * 17
    return jax.shard_map(local_step, mesh=mesh, in_specs=in_specs, out_specs=token_rows, check_vma=False)
```
